32 devices in a mesh: patch: 16 (over z, x, core), lev: 2 (over y).
Axes of the slice: x: 2, y: 2, z: 4, core: 2. Of those that a mesh axis runs over, the one named last changes fastest.
Arguments:
- fields: bfloat16 [8, 32, 32768], P(None, 'lev', 'patch'), may hold values from -6 to 6
- interp: bfloat16 [128, 128, 256], P('patch'), may hold values from -0.375 to 0.375
- conv_weight: bfloat16 [128, 8, 128, 128], P('patch'), may hold values from -0.1875 to 0.1875
- vert_weight: float32 [32, 5], replicated, may hold values from 0.1 to 0.5
- send_tiles: int32 [16, 4, 2], P('patch'), may hold values from 0 to 8, as said below
- tile_pattern: int32 [128, 8], P('patch'), may hold values from 0 to 15, as said below
Outputs:
- localized: float32 [8, 32, 32768], P(None, 'lev', 'patch')
The draws below stay inside these ranges and needn't reach their ends.
Inputs may be any that keep to these rules, and one draw needn't show every extreme that they name: `send_tiles`: in every draw some link carries 2 tiles; every link carries at least one tile; the tiles of one link are distinct. `tile_pattern`: each row names distinct entries, each an own tile or a filled received slot.
All inputs are finite; a program needn't handle non-finite values.
Results may differ from the reference program's by a relative error of at most 0.0048.
Values may be sent and summed in bfloat16 or wider, within the bound.
A program may use at most 64 MiB of HBM per device.

```python
import math
import jax
import jax.numpy as jnp
from jax import lax

MEMBERS = 8
TILES_DEV = 8
TILE = 128
FINE_TILE = 256
K = 8
REACH = 2
MOST = 2
VHALF = 2
LEVELS = 32
BLOCKS = 128
COLUMNS = 32768
N_PATCH = 16


def link_table():
    return jnp.array([position - REACH if position < REACH else position - REACH + 1 for position in range(2 * REACH)], jnp.int32)


def link_counts(key):
    base = jax.random.fold_in(key, 11)
    counts = jax.random.randint(jax.random.fold_in(base, 1), (N_PATCH * 2 * REACH,), 1, MOST + 1)
    picked = jax.random.randint(jax.random.fold_in(base, 2), (), 0, N_PATCH * 2 * REACH)
    counts = jnp.where(jnp.arange(N_PATCH * 2 * REACH) == picked, MOST, counts)
    return counts.reshape(N_PATCH, 2 * REACH).astype(jnp.int32)


def draw_send_tiles(key, part):
    counts = link_counts(key)
    keys = jax.random.split(jax.random.fold_in(key, 12), N_PATCH * 2 * REACH)
    chosen = jax.vmap(lambda single: jax.random.permutation(single, TILES_DEV))(keys)[:, :MOST]
    chosen = chosen.reshape(N_PATCH, 2 * REACH, MOST)
    slot_ids = jnp.arange(MOST)[None, None, :]
    return jnp.where(slot_ids < counts[:, :, None], chosen, TILES_DEV).astype(jnp.int32)


def draw_tile_pattern(key, part):
    counts = link_counts(key)
    links = link_table()
    source = (jnp.arange(N_PATCH)[:, None] - links[None, :]) % N_PATCH
    arrived = counts[source, jnp.arange(2 * REACH)[None, :]]
    filled = jnp.arange(MOST)[None, None, :] < arrived[:, :, None]
    valid = jnp.concatenate([jnp.ones((N_PATCH, TILES_DEV), bool), filled.reshape(N_PATCH, 2 * REACH * MOST)], axis=1)
    width = TILES_DEV + 2 * REACH * MOST
    scores = jax.random.randint(jax.random.fold_in(key, 13), (N_PATCH, TILES_DEV, width), 0, 1 << 20) * width + jnp.arange(width)[None, None, :]
    scores = jnp.where(valid[:, None, :], scores, scores + (1 << 20) * width)
    order = jnp.argsort(scores, axis=-1)[..., :K]
    return order.reshape(N_PATCH * TILES_DEV, K).astype(jnp.int32)


def block_levels(stream_key, dims, shards, low, high):
    def one(dim, shards_of):
        heights = jax.random.uniform(jax.random.fold_in(jax.random.fold_in(stream_key, 6), dim), (shards_of,), jnp.float32, low / len(shards), high / len(shards))
        return jnp.repeat(jnp.exp(heights), dims[dim] // shards_of).reshape((-1,) + (1,) * (len(dims) - dim - 1))

    gain = one(*shards[0])
    for cut in shards[1:]:
        gain = gain * one(*cut)
    return gain


def noise(stream_key, extent, deviation, reach, cuts=(), kind=jnp.bfloat16):
    values = jax.random.normal(stream_key, extent, jnp.float32) * deviation
    if len(cuts) > 0:
        values = block_levels(stream_key, extent, cuts, -0.22, 0.18) * values
    return jnp.clip(values, min=-reach, max=reach).astype(kind)


def setup_inputs(seed: int = 0) -> dict:
    key_list = jax.random.split(jax.random.key(seed), 7)
    return {
        "fields": noise(key_list[0], (MEMBERS, LEVELS, COLUMNS), 1.0, 6.0, ((1, 2), (2, 16))),
        "interp": noise(key_list[1], (BLOCKS, TILE, FINE_TILE), FINE_TILE ** -0.5, 0.375, ((0, 16),)),
        "conv_weight": noise(key_list[2], (BLOCKS, K, TILE, TILE), (K * TILE) ** -0.5, 0.1875, ((0, 16),)),
        "vert_weight": jnp.clip(jnp.exp(jax.random.uniform(key_list[3], (LEVELS, 2 * VHALF + 1), jnp.float32, math.log(0.1), math.log(0.5))), 0.1, 0.5),
        "send_tiles": draw_send_tiles(jax.random.fold_in(key_list[6], 71), 0),
        "tile_pattern": draw_tile_pattern(jax.random.fold_in(key_list[6], 71), 0),
    }


HIGHEST = lax.Precision.HIGHEST


def link_offsets(reach_len):
    return [position - reach_len if position < reach_len else position - reach_len + 1 for position in range(2 * reach_len)]


def vertical_adjoint(values, weights, length, half_width):
    summed = jnp.zeros(values.shape[:-2] + (length, values.shape[-1]), jnp.float32)
    for offset in range(-half_width, half_width + 1):
        factor = weights[half_width + offset: half_width + offset + length, half_width - offset]
        summed = summed + factor[:, None] * values[..., half_width + offset: half_width + offset + length, :].astype(jnp.float32)
    return summed


def vertical_forward(values, weights, length, half_width):
    summed = jnp.zeros(values.shape[:-2] + (length, values.shape[-1]), jnp.float32)
    for offset in range(2 * half_width + 1):
        factor = weights[half_width: half_width + length, offset]
        summed = summed + factor[:, None] * values[..., offset: offset + length, :].astype(jnp.float32)
    return summed


def reference(fields, interp, conv_weight, vert_weight, send_tiles, tile_pattern):
    members, level_total, column_total = fields.shape
    block_total, tile_len, fine_len = interp.shape
    patch_count = N_PATCH
    tile_count = block_total // patch_count
    reach_len = send_tiles.shape[1] // 2
    slot_most = send_tiles.shape[2]
    half_width = (vert_weight.shape[1] - 1) // 2
    row_count = members * level_total
    extended_len = tile_count + 2 * reach_len * slot_most
    offsets = link_offsets(reach_len)
    flat = fields.reshape(row_count, patch_count, tile_count, fine_len)
    interp_patch = interp.reshape(patch_count, tile_count, tile_len, fine_len)
    conv_patch = conv_weight.reshape(patch_count, tile_count, -1, tile_len, tile_len)
    pattern_patch = tile_pattern.reshape(patch_count, tile_count, -1)
    positions = jnp.arange(patch_count).astype(jnp.int32)

    def restrict(position):
        block = lax.dynamic_index_in_dim(flat, position, 1, keepdims=False)
        return jnp.einsum("rtf,tcf->trc", block.astype(jnp.float32), interp_patch[position].astype(jnp.float32), precision=HIGHEST).astype(jnp.bfloat16)

    coarse = lax.map(restrict, positions)

    def adjoint_patch(position):
        products = jnp.einsum("tro,tkio->tkri", coarse[position].astype(jnp.float32), conv_patch[position].astype(jnp.float32), precision=HIGHEST)
        chosen = (pattern_patch[position][:, :, None] == jnp.arange(extended_len).astype(jnp.int32)[None, None, :]).astype(jnp.float32)
        summed = jnp.einsum("tke,tkri->eri", chosen, products, precision=HIGHEST)
        returning = summed[tile_count:].reshape(2 * reach_len, slot_most, row_count, tile_len).astype(jnp.bfloat16)
        return summed[:tile_count], returning

    own_part, returning = lax.map(adjoint_patch, positions)
    arrived_back = jnp.stack([jnp.roll(returning[:, position], -offsets[position], axis=0) for position in range(2 * reach_len)], axis=1)

    def combine(position):
        sending = (send_tiles[position][:, :, None] == jnp.arange(tile_count).astype(jnp.int32)[None, None, :]).astype(jnp.float32)
        added = jnp.einsum("ost,osri->tri", sending, arrived_back[position].astype(jnp.float32), precision=HIGHEST)
        return (own_part[position] + added).astype(jnp.bfloat16)

    adjoint = lax.map(combine, positions).reshape(patch_count, tile_count, members, level_total, tile_len)
    level_pad = ((0, 0), (0, 0), (0, 0), (half_width, half_width), (0, 0))
    weight_pad = jnp.pad(vert_weight, ((half_width, half_width), (0, 0)))
    middle = vertical_adjoint(jnp.pad(adjoint, level_pad), weight_pad, level_total, half_width).astype(jnp.bfloat16)
    smooth = vertical_forward(jnp.pad(middle, level_pad), weight_pad, level_total, half_width).astype(jnp.bfloat16)
    smooth = smooth.reshape(patch_count, tile_count, row_count, tile_len)

    def pack(position):
        sending = (send_tiles[position][:, :, None] == jnp.arange(tile_count).astype(jnp.int32)[None, None, :]).astype(jnp.float32)
        return jnp.einsum("ost,tri->osri", sending, smooth[position].astype(jnp.float32), precision=HIGHEST).astype(jnp.bfloat16)

    slots = lax.map(pack, positions)
    arrived = jnp.stack([jnp.roll(slots[:, position], offsets[position], axis=0) for position in range(2 * reach_len)], axis=1)

    def forward_patch(position):
        extended = jnp.concatenate([smooth[position], arrived[position].reshape(-1, row_count, tile_len)], axis=0)
        chosen = (pattern_patch[position][:, :, None] == jnp.arange(extended_len).astype(jnp.int32)[None, None, :]).astype(jnp.float32)
        picked = jnp.einsum("tke,eri->tkri", chosen, extended.astype(jnp.float32), precision=HIGHEST)
        mixed = jnp.einsum("tkri,tkio->tro", picked, conv_patch[position].astype(jnp.float32), precision=HIGHEST).astype(jnp.bfloat16)
        return jnp.einsum("tro,tof->rtf", mixed.astype(jnp.float32), interp_patch[position].astype(jnp.float32), precision=HIGHEST)

    result = lax.map(forward_patch, positions)
    return jnp.transpose(result, (1, 0, 2, 3)).reshape(members, level_total, column_total)
```

```python
import functools

import jax
import jax.numpy as jnp
from jax import lax
from jax.experimental import pallas as pl
from jax.experimental.pallas import tpu as pltpu
from jax.sharding import PartitionSpec as P

MESH = pl.DeviceIdType.MESH
F32 = jnp.float32
BF16 = jnp.bfloat16


def link_offsets(reach_len):
    return [
        position - reach_len if position < reach_len else position - reach_len + 1
        for position in range(2 * reach_len)
    ]


def chunks_of(parts):
    chunks = []
    for low, count in parts:
        step = count // 2 if count % 32 == 0 else count
        chunks.append([(low + at, step) for at in range(0, count, step)])
    return chunks


def dot_t(left, right):
    return lax.dot_general(left, right, (((1,), (1,)), ((), ())), preferred_element_type=F32)


def kernel(
    n_patch,
    n_lev,
    fields_hbm,
    interp_hbm,
    conv_hbm,
    weight_hbm,
    send_hbm,
    pattern_hbm,
    out,
    weight,
    send,
    pattern,
    fields,
    interp,
    conv,
    coarse,
    levels,
    middle,
    halo_out,
    halo_in,
    own,
    mixed,
    smooth,
    ext,
    power,
    which,
    slot_of,
    load_sem,
    halo_sem,
    back_sem,
    forth_sem,
    enter_sem,
    enter_lev,
    *links,
):
    members, level_len, _ = fields.shape
    tiles, tile_len, fine = interp.shape
    k_len = conv_hbm.shape[1]
    most, link_len = send.shape[1], send.shape[2]
    half = (weight.shape[0] - 1) // 2
    wide = 2 * half
    rows = members * level_len
    total_levels = weight.shape[1]
    offsets = link_offsets(link_len // 2)
    returning, sending, arrived = (links[i * link_len : (i + 1) * link_len] for i in range(3))
    arrived_back = [links[i * link_len : (i + 1) * link_len] for i in range(3, len(links) // link_len)]
    edge = wide * members
    parts = [(0, rows - 2 * edge), (rows - 2 * edge, 2 * edge)]
    chunks = chunks_of(parts)
    numbered = [(low, count) for part in chunks for low, count in part]
    me_p, me_l = lax.axis_index("patch"), lax.axis_index("lev")
    partner = [lax.rem(me_p + d + n_patch, n_patch) for d in offsets]
    source = [lax.rem(me_p - d + n_patch, n_patch) for d in offsets]
    opposite = [offsets.index(-d) for d in offsets]
    upper = sorted((o for o in range(link_len) if offsets[o] < 0), key=lambda o: offsets[o])
    lower = sorted((o for o in range(link_len) if offsets[o] > 0), key=lambda o: -offsets[o])

    load_w = pltpu.make_async_copy(weight_hbm, weight, load_sem.at[3])
    load_s = pltpu.make_async_copy(send_hbm, send, load_sem.at[4])
    load_p = pltpu.make_async_copy(pattern_hbm, pattern, load_sem.at[5])
    load_f = pltpu.make_async_copy(fields_hbm, fields, load_sem.at[0])
    load_i = pltpu.make_async_copy(interp_hbm, interp, load_sem.at[1])
    load_c = pltpu.make_async_copy(conv_hbm, conv.at[:, pl.ds(0, k_len)], load_sem.at[2])
    load_p.start()
    load_s.start()
    load_w.start()
    load_f.start()
    load_i.start()
    load_c.start()

    barrier = pltpu.get_barrier_semaphore()
    for o in range(link_len):

        @pl.when(partner[o] > me_p)
        def _(o=o):
            pl.semaphore_signal(
                barrier, inc=1, device_id={"patch": partner[o]}, device_id_type=MESH
            )

    @pl.when(me_l < n_lev - 1)
    def _():
        pl.semaphore_signal(barrier, inc=1, device_id={"lev": me_l + 1}, device_id_type=MESH)

    bits = k_len.bit_length()
    per_word = 31 // bits
    entries = tiles + link_len * most
    words = -(-entries // per_word)
    for e in range(entries):
        for w in range(words):
            inside = w * per_word <= e < (w + 1) * per_word
            power[w, e] = jnp.int32(1 << (bits * (e - w * per_word)) if inside else 0)
    for t in range(tiles):
        conv[t, k_len] = jnp.zeros((tile_len, tile_len), BF16)
    for i, (_, count) in enumerate(numbered):
        for o in range(link_len):
            arrived_back[i][o][most] = jnp.zeros((count, tile_len), BF16)
    ext[tiles] = jnp.zeros((rows, tile_len), BF16)
    load_p.wait()
    load_s.wait()
    load_w.wait()
    empty = sum(k_len << (bits * i) for i in range(per_word))
    for t in range(tiles):
        packed = [jnp.int32(empty) for _ in range(words)]
        for k in range(k_len):
            named = pattern[t, k]
            for w in range(words):
                packed[w] = packed[w] + jnp.int32(k - k_len) * power[w, named]
        for e in range(entries):
            w, place = e // per_word, bits * (e % per_word)
            which[t, e] = (packed[w] >> place) & ((1 << bits) - 1)
        for o in range(link_len):
            index = jnp.int32(most)
            for s in range(most):
                index = jnp.where(send[0, s, o] == t, s, index)
            slot_of[t, o] = index

    load_f.wait()
    load_i.wait()
    for t in range(tiles):
        block = fields[:, :, t * fine : (t + 1) * fine].reshape(rows, fine)
        coarse[t] = dot_t(block, interp[t])
        for l in range(level_len):
            levels[wide + l, t] = coarse[t, pl.ds(l, members, stride=level_len), :]
    for i in range(wide // 2):
        low = jnp.concatenate([levels[wide + 2 * i], levels[wide + 2 * i + 1]], axis=1)
        top = level_len + 2 * i
        high = jnp.concatenate([levels[top], levels[top + 1]], axis=1)
        halo_out[0, i] = low.astype(BF16)
        halo_out[1, i] = high.astype(BF16)

    down = pltpu.make_async_remote_copy(
        halo_out.at[0],
        halo_in.at[1],
        halo_sem.at[0],
        halo_sem.at[1],
        device_id={"lev": lax.rem(me_l + n_lev - 1, n_lev)},
        device_id_type=MESH,
    )
    up = pltpu.make_async_remote_copy(
        halo_out.at[1],
        halo_in.at[0],
        halo_sem.at[2],
        halo_sem.at[3],
        device_id={"lev": lax.rem(me_l + 1, n_lev)},
        device_id_type=MESH,
    )

    before = jnp.where(me_l > 0, 1, 0)
    for o in range(link_len):
        before = before + jnp.where(partner[o] < me_p, 1, 0)

    @pl.when(before > 0)
    def _():
        pl.semaphore_wait(barrier, before)

    for o in range(link_len):

        @pl.when(partner[o] < me_p)
        def _(o=o):
            pl.semaphore_signal(
                enter_sem.at[opposite[o]],
                inc=1,
                device_id={"patch": partner[o]},
                device_id_type=MESH,
            )

    @pl.when(me_l > 0)
    def _():
        pl.semaphore_signal(enter_lev, inc=1, device_id={"lev": me_l - 1}, device_id_type=MESH)
        down.start()

    @pl.when(me_l < n_lev - 1)
    def _():
        pl.semaphore_wait(enter_lev, 1)
        up.start()

    start = me_l * level_len

    def coefficient(level, column):
        return weight[column, jnp.clip(start + level, 0, total_levels - 1)]

    def adjoint_level(level):
        value = coefficient(level - half, wide) * levels[wide + level - half]
        for e in range(1 - half, half + 1):
            value = value + coefficient(level + e, half - e) * levels[wide + level + e]
        if level < 0:
            value = jnp.where(start + level >= 0, value, 0.0)
        if level >= level_len:
            value = jnp.where(start + level < total_levels, value, 0.0)
        middle[half + level] = value

    def forward_pair(level):
        both = []
        for l in (level, level + 1):
            value = coefficient(l, 0) * middle[l]
            for j in range(1, wide + 1):
                value = value + coefficient(l, j) * middle[l + j]
            both.append(value)
        pair = jnp.concatenate(both, axis=1).astype(BF16)
        if wide <= level < level_len - wide:
            place = (level - wide) * members
        else:
            place = level if level < wide else level - level_len + 2 * wide
            place = parts[1][0] + place * members
        smooth[:, pl.ds(place, 2 * members), :] = pair

    for level in range(half, level_len - half):
        adjoint_level(level)
    for level in range(wide, level_len - wide, 2):
        forward_pair(level)

    load_c.wait()

    def gathered(left, first):
        right = jnp.concatenate(
            [
                jnp.concatenate([conv[t, which[t, first + s]] for t in range(tiles)], axis=1)
                for s in range(most)
            ],
            axis=0,
        )
        return dot_t(left, right)

    def side_by_side(ref, count, low, size):
        return jnp.concatenate([ref[i, pl.ds(low, size)] for i in range(count)], axis=1)

    def sum_back(c, o):
        low, count = parts[c]
        left = side_by_side(smooth, tiles, low, count)
        sums = gathered(left, tiles + o * most).astype(BF16)
        for s in range(most):
            returning[o][s, pl.ds(low, count)] = sums[:, s * tile_len : (s + 1) * tile_len]

    def copy_back(o, i):
        low, count = numbered[i]
        return pltpu.make_async_remote_copy(
            returning[o].at[:, pl.ds(low, count)],
            arrived_back[i][o].at[pl.ds(0, most)],
            back_sem.at[0, i, o],
            back_sem.at[1, i, o],
            device_id={"patch": source[o]},
            device_id_type=MESH,
        )

    def copy_forth(o, i):
        low, count = numbered[i]
        return pltpu.make_async_remote_copy(
            sending[o].at[:, pl.ds(low, count)],
            arrived[o].at[:, pl.ds(low, count)],
            forth_sem.at[0, i, o],
            forth_sem.at[1, i, o],
            device_id={"patch": partner[o]},
            device_id_type=MESH,
        )

    def indices(c):
        first = len(chunks[0]) if c else 0
        return range(first, first + len(chunks[c]))

    def sum_own(c):
        low, count = parts[c]
        left = side_by_side(smooth, tiles, low, count)
        for first in range(0, tiles, most):
            sums = gathered(left, first)
            for s in range(most):
                own[first + s, pl.ds(low, count)] = sums[:, s * tile_len : (s + 1) * tile_len]

    def send_back(c):
        for o in upper:
            sum_back(c, o)
        if c == 0:
            for o in upper:

                @pl.when(source[o] > me_p)
                def _(o=o):
                    pl.semaphore_wait(enter_sem.at[opposite[o]], 1)

        for i in indices(c):
            for o in upper:
                copy_back(o, i).start()
        for o in lower:
            sum_back(c, o)
        for o in lower:

            @pl.when(source[o] < me_p)
            def _(o=o):
                for i in indices(c):
                    copy_back(o, i).start()

    send_back(0)
    sum_own(0)

    def unpack(side, base):
        for i in range(wide // 2):
            pair = halo_in[side, i].astype(F32)
            levels[base + 2 * i] = pair[:, :members]
            levels[base + 2 * i + 1] = pair[:, members:]

    def clear(base):
        for i in range(wide):
            levels[base + i] = jnp.zeros(levels.shape[1:], F32)

    @pl.when(me_l > 0)
    def _():
        up.wait_recv()
        unpack(0, 0)

    @pl.when(me_l == 0)
    def _():
        clear(0)

    @pl.when(me_l < n_lev - 1)
    def _():
        down.wait_recv()
        unpack(1, wide + level_len)

    @pl.when(me_l == n_lev - 1)
    def _():
        clear(wide + level_len)

    for level in list(range(-half, half)) + list(range(level_len - half, level_len + half)):
        adjoint_level(level)
    for level in list(range(0, wide, 2)) + list(range(level_len - wide, level_len, 2)):
        forward_pair(level)

    send_back(1)
    for o in lower:

        @pl.when(source[o] > me_p)
        def _(o=o):
            pl.semaphore_wait(enter_sem.at[opposite[o]], 1)
            for i in range(len(numbered)):
                copy_back(o, i).start()

    sum_own(1)

    for i, (low, count) in enumerate(numbered):
        for o in upper + lower:
            copy_back(o, i).wait_recv()
        for t in range(tiles):
            value = own[t, pl.ds(low, count)]
            for o in range(link_len):
                value = value + arrived_back[i][o][slot_of[t, o]].astype(F32)
            ext[t, pl.ds(low, count)] = value.astype(BF16)
        for o in lower + upper:
            for s in range(most):
                sending[o][s, pl.ds(low, count)] = ext[send[0, s, o], pl.ds(low, count)]
            copy_forth(o, i).start()

    def spread(left, named, t):
        right = jnp.concatenate(
            [
                jnp.concatenate([conv[u, which[u, e]] for e in named], axis=0)
                for u in (t, t + 1)
            ],
            axis=1,
        )
        return jnp.dot(left, right, preferred_element_type=F32)

    def places():
        return [(0, parts[0][1], edge), (parts[1][0], edge, 0), (parts[1][0] + edge, edge, rows - edge)]

    def put(t, sums, fresh):
        for begin, count, place in places():
            for i in range(2):
                value = sums[begin : begin + count, i * tile_len : (i + 1) * tile_len]
                if not fresh:
                    value = value + mixed[t + i, pl.ds(place, count)]
                mixed[t + i, pl.ds(place, count)] = value

    left = side_by_side(ext, tiles, 0, rows)
    for t in range(0, tiles, 2):
        put(t, spread(left, range(tiles), t), True)
    for group in (upper, lower):
        for i in range(len(numbered)):
            for o in group:
                copy_forth(o, i).wait_recv()
        left = jnp.concatenate([side_by_side(arrived[o], most, 0, rows) for o in group], axis=1)
        named = [tiles + o * most + s for o in group for s in range(most)]
        for t in range(0, tiles, 2):
            put(t, spread(left, named, t), False)

    for t in range(tiles):
        part = jnp.concatenate(
            [mixed[t, pl.ds(m, level_len, stride=members), :] for m in range(members)], axis=0
        ).astype(BF16)
        result = jnp.dot(part, interp[t], preferred_element_type=F32)
        out[:, :, t * fine : (t + 1) * fine] = result.reshape(members, level_len, fine)
    for i in range(len(numbered)):
        for o in range(link_len):
            copy_back(o, i).wait_send()
            copy_forth(o, i).wait_send()

    @pl.when(me_l > 0)
    def _():
        down.wait_send()

    @pl.when(me_l < n_lev - 1)
    def _():
        up.wait_send()


def solution(mesh):
    n_patch, n_lev = mesh.shape["patch"], mesh.shape["lev"]

    def shards(fields, interp, conv_weight, vert_weight, send_tiles, tile_pattern):
        members, level_len, column_len = fields.shape
        tiles, tile_len, fine = interp.shape
        k_len = conv_weight.shape[1]
        link_len, most = send_tiles.shape[1:]
        wide = vert_weight.shape[1] - 1
        rows = members * level_len
        any_spec = pl.BlockSpec(memory_space=pl.ANY)
        entries = tiles + link_len * most
        words = -(-entries // (31 // k_len.bit_length()))
        weight, send = vert_weight.T, send_tiles.transpose(0, 2, 1)
        edge = 2 * wide * members
        sizes = [count for part in chunks_of([(0, rows - edge), (rows - edge, edge)]) for _, count in part]

        def per_link(count, size=rows):
            return [pltpu.VMEM((count, size, tile_len), BF16) for _ in range(link_len)]

        return pl.pallas_call(
            functools.partial(kernel, n_patch, n_lev),
            name="localize",
            out_shape=pltpu.VMEM(fields.shape, F32),
            in_specs=[any_spec] * 6,
            out_specs=pl.BlockSpec(memory_space=pltpu.VMEM),
            scratch_shapes=[
                pltpu.SMEM(weight.shape, F32),
                pltpu.SMEM(send.shape, jnp.int32),
                pltpu.SMEM(tile_pattern.shape, jnp.int32),
                pltpu.VMEM(fields.shape, BF16),
                pltpu.VMEM(interp.shape, BF16),
                pltpu.VMEM((tiles, k_len + 1, tile_len, tile_len), BF16),
                pltpu.VMEM((tiles, rows, tile_len), F32),
                pltpu.VMEM((level_len + 2 * wide, tiles, members, tile_len), F32),
                pltpu.VMEM((level_len + wide, tiles, members, tile_len), F32),
                pltpu.VMEM((2, wide // 2, tiles, 2 * members, tile_len), BF16),
                pltpu.VMEM((2, wide // 2, tiles, 2 * members, tile_len), BF16),
                pltpu.VMEM((tiles, rows, tile_len), F32),
                pltpu.VMEM((tiles, rows, tile_len), F32),
                pltpu.VMEM((tiles, rows, tile_len), BF16),
                pltpu.VMEM((tiles + 1, rows, tile_len), BF16),
                pltpu.SMEM((words, entries), jnp.int32),
                pltpu.SMEM((tiles, entries), jnp.int32),
                pltpu.SMEM((tiles, link_len), jnp.int32),
                pltpu.SemaphoreType.DMA((6,)),
                pltpu.SemaphoreType.DMA((4,)),
                pltpu.SemaphoreType.DMA((2, len(sizes), link_len)),
                pltpu.SemaphoreType.DMA((2, len(sizes), link_len)),
                pltpu.SemaphoreType.REGULAR((link_len,)),
                pltpu.SemaphoreType.REGULAR,
            ]
            + per_link(most)
            + per_link(most)
            + per_link(most)
            + [ref for size in sizes for ref in per_link(most + 1, size)],
            compiler_params=pltpu.CompilerParams(collective_id=0, has_side_effects=True),
        )(fields, interp, conv_weight, weight, send, tile_pattern)

    in_specs = (
        P(None, "lev", "patch"),
        P("patch", None, None),
        P("patch", None, None, None),
        P(),
        P("patch", None, None),
        P("patch", None),
    )
    out_specs = P(None, "lev", "patch")
    return jax.shard_map(shards, mesh=mesh, in_specs=in_specs, out_specs=out_specs, check_vma=False)
```

```python
import functools

import jax
import jax.numpy as jnp
from jax import lax
from jax.experimental import pallas as pl
from jax.experimental.pallas import tpu as pltpu
from jax.sharding import PartitionSpec as P

MESH = pl.DeviceIdType.MESH
F32 = jnp.float32
BF16 = jnp.bfloat16


def link_offsets(reach_len):
    return [
        position - reach_len if position < reach_len else position - reach_len + 1
        for position in range(2 * reach_len)
    ]


def chunks_of(parts):
    chunks = []
    for low, count in parts:
        step = count // 2 if count % 32 == 0 else count
        chunks.append([(low + at, step) for at in range(0, count, step)])
    return chunks


def dot_t(left, right):
    return lax.dot_general(left, right, (((1,), (1,)), ((), ())), preferred_element_type=F32)


def kernel(
    n_patch,
    n_lev,
    fields_hbm,
    interp_hbm,
    conv_hbm,
    weight_hbm,
    send_hbm,
    pattern_hbm,
    out,
    weight,
    send,
    pattern,
    fields,
    interp,
    conv,
    coarse,
    levels,
    middle,
    halo_out,
    halo_in,
    own,
    mixed,
    smooth,
    ext,
    power,
    which,
    slot_of,
    load_sem,
    halo_sem,
    send_sem,
    back_sem,
    forth_sem,
    enter_sem,
    enter_lev,
    returning,
    sending,
    arrived,
    *arrived_back,
):
    members, level_len, _ = fields.shape
    tiles, tile_len, fine = interp.shape
    k_len = conv_hbm.shape[1]
    most, link_len = send.shape[1], send.shape[2]
    half = (weight.shape[0] - 1) // 2
    wide = 2 * half
    rows = members * level_len
    total_levels = weight.shape[1]
    offsets = link_offsets(link_len // 2)
    edge = wide * members
    parts = [(0, rows - 2 * edge), (rows - 2 * edge, 2 * edge)]
    chunks = chunks_of(parts)
    numbered = [(low, count) for part in chunks for low, count in part]
    me_p, me_l = lax.axis_index("patch"), lax.axis_index("lev")
    partner = [lax.rem(me_p + d + n_patch, n_patch) for d in offsets]
    source = [lax.rem(me_p - d + n_patch, n_patch) for d in offsets]
    upper = sorted((o for o in range(link_len) if offsets[o] < 0), key=lambda o: offsets[o])
    lower = sorted((o for o in range(link_len) if offsets[o] > 0), key=lambda o: -offsets[o])

    load_w = pltpu.make_async_copy(weight_hbm, weight, load_sem.at[3])
    load_s = pltpu.make_async_copy(send_hbm, send, load_sem.at[4])
    load_p = pltpu.make_async_copy(pattern_hbm, pattern, load_sem.at[5])
    load_f = pltpu.make_async_copy(fields_hbm, fields, load_sem.at[0])
    load_i = pltpu.make_async_copy(interp_hbm, interp, load_sem.at[1])
    load_c = pltpu.make_async_copy(conv_hbm, conv.at[:, pl.ds(0, k_len)], load_sem.at[2])
    load_p.start()
    load_s.start()
    load_w.start()
    load_f.start()
    load_i.start()
    load_c.start()

    barrier = pltpu.get_barrier_semaphore()
    for o in range(link_len):

        @pl.when(partner[o] > me_p)
        def _(o=o):
            pl.semaphore_signal(
                barrier, inc=1, device_id={"patch": partner[o]}, device_id_type=MESH
            )

    @pl.when(me_l < n_lev - 1)
    def _():
        pl.semaphore_signal(barrier, inc=1, device_id={"lev": me_l + 1}, device_id_type=MESH)

    bits = k_len.bit_length()
    per_word = 31 // bits
    entries = tiles + link_len * most
    words = -(-entries // per_word)
    for e in range(entries):
        for w in range(words):
            inside = w * per_word <= e < (w + 1) * per_word
            power[w, e] = jnp.int32(1 << (bits * (e - w * per_word)) if inside else 0)
    for t in range(tiles):
        conv[t, k_len] = jnp.zeros((tile_len, tile_len), BF16)
    for i, (_, count) in enumerate(numbered):
        for o in range(link_len):
            arrived_back[i][o, most] = jnp.zeros((count, tile_len), BF16)
    ext[tiles] = jnp.zeros((rows, tile_len), BF16)
    before = jnp.where(me_l > 0, 1, 0)
    for o in range(link_len):
        before = before + jnp.where(partner[o] < me_p, 1, 0)

    @pl.when(before > 0)
    def _():
        pl.semaphore_wait(barrier, before)

    for o in range(link_len):

        @pl.when(partner[o] < me_p)
        def _(o=o):
            pl.semaphore_signal(
                enter_sem.at[0 if offsets[o] < 0 else 1],
                inc=1,
                device_id={"patch": partner[o]},
                device_id_type=MESH,
            )

    @pl.when(me_l > 0)
    def _():
        pl.semaphore_signal(enter_lev, inc=1, device_id={"lev": me_l - 1}, device_id_type=MESH)

    load_p.wait()
    load_s.wait()
    load_w.wait()
    load_f.wait()
    load_i.wait()
    empty = sum(k_len << (bits * i) for i in range(per_word))
    for t in range(tiles):
        packed = [jnp.int32(empty) for _ in range(words)]
        for k in range(k_len):
            named = pattern[t, k]
            for w in range(words):
                packed[w] = packed[w] + jnp.int32(k - k_len) * power[w, named]
        for e in range(entries):
            w, place = e // per_word, bits * (e % per_word)
            which[t, e] = (packed[w] >> place) & ((1 << bits) - 1)
        for o in range(link_len):
            index = jnp.int32(most)
            for s in range(most):
                index = jnp.where(send[0, s, o] == t, s, index)
            slot_of[t, o] = index
    for t in range(tiles):
        block = fields[:, :, t * fine : (t + 1) * fine].reshape(rows, fine)
        coarse[t] = dot_t(block, interp[t])
        for l in range(level_len):
            levels[wide + l, t] = coarse[t, pl.ds(l, members, stride=level_len), :]
    for i in range(wide // 2):
        low = jnp.concatenate([levels[wide + 2 * i], levels[wide + 2 * i + 1]], axis=1)
        top = level_len + 2 * i
        high = jnp.concatenate([levels[top], levels[top + 1]], axis=1)
        halo_out[0, i] = low.astype(BF16)
        halo_out[1, i] = high.astype(BF16)

    down = pltpu.make_async_remote_copy(
        halo_out.at[0],
        halo_in.at[1],
        halo_sem.at[0],
        halo_sem.at[1],
        device_id={"lev": lax.rem(me_l + n_lev - 1, n_lev)},
        device_id_type=MESH,
    )
    up = pltpu.make_async_remote_copy(
        halo_out.at[1],
        halo_in.at[0],
        halo_sem.at[2],
        halo_sem.at[3],
        device_id={"lev": lax.rem(me_l + 1, n_lev)},
        device_id_type=MESH,
    )

    @pl.when(me_l > 0)
    def _():
        down.start()

    @pl.when(me_l < n_lev - 1)
    def _():
        pl.semaphore_wait(enter_lev, 1)
        up.start()

    start = me_l * level_len

    def coefficient(level, column):
        return weight[column, jnp.clip(start + level, 0, total_levels - 1)]

    def adjoint_level(level):
        value = coefficient(level - half, wide) * levels[wide + level - half]
        for e in range(1 - half, half + 1):
            value = value + coefficient(level + e, half - e) * levels[wide + level + e]
        if level < 0:
            value = jnp.where(start + level >= 0, value, 0.0)
        if level >= level_len:
            value = jnp.where(start + level < total_levels, value, 0.0)
        middle[half + level] = value

    def forward_pair(level):
        both = []
        for l in (level, level + 1):
            value = coefficient(l, 0) * middle[l]
            for j in range(1, wide + 1):
                value = value + coefficient(l, j) * middle[l + j]
            both.append(value)
        pair = jnp.concatenate(both, axis=1).astype(BF16)
        if wide <= level < level_len - wide:
            place = (level - wide) * members
        else:
            place = level if level < wide else level - level_len + 2 * wide
            place = parts[1][0] + place * members
        smooth[:, pl.ds(place, 2 * members), :] = pair

    for level in range(half, level_len - half):
        adjoint_level(level)
    for level in range(wide, level_len - wide, 2):
        forward_pair(level)

    load_c.wait()

    def gathered(left, first):
        right = jnp.concatenate(
            [
                jnp.concatenate([conv[t, which[t, first + s]] for t in range(tiles)], axis=1)
                for s in range(most)
            ],
            axis=0,
        )
        return dot_t(left, right)

    def side_by_side(ref, count, low, size):
        return jnp.concatenate([ref[i, pl.ds(low, size)] for i in range(count)], axis=1)

    def sum_back(c, o):
        low, count = parts[c]
        left = side_by_side(smooth, tiles, low, count)
        sums = gathered(left, tiles + o * most).astype(BF16)
        for s in range(most):
            returning[o, s, pl.ds(low, count)] = sums[:, s * tile_len : (s + 1) * tile_len]

    def copy_back(o, i):
        low, count = numbered[i]
        return pltpu.make_async_remote_copy(
            returning.at[o, :, pl.ds(low, count)],
            arrived_back[i].at[o, pl.ds(0, most)],
            send_sem.at[0],
            back_sem.at[i],
            device_id={"patch": source[o]},
            device_id_type=MESH,
        )

    def copy_forth(o, i):
        low, count = numbered[i]
        return pltpu.make_async_remote_copy(
            sending.at[o, :, pl.ds(low, count)],
            arrived.at[o, :, pl.ds(low, count)],
            send_sem.at[1],
            forth_sem.at[0 if offsets[o] < 0 else 1],
            device_id={"patch": partner[o]},
            device_id_type=MESH,
        )

    def all_back(i):
        low, count = numbered[i]
        return pltpu.make_async_remote_copy(
            returning.at[:, :, pl.ds(low, count)],
            arrived_back[i].at[:, pl.ds(0, most)],
            send_sem.at[0],
            back_sem.at[i],
            device_id={"patch": source[0]},
            device_id_type=MESH,
        )

    def all_forth(first, count, sem):
        return pltpu.make_async_remote_copy(
            sending.at[pl.ds(first, count)],
            arrived.at[pl.ds(first, count)],
            send_sem.at[1],
            forth_sem.at[sem],
            device_id={"patch": partner[0]},
            device_id_type=MESH,
        )

    def indices(c):
        first = len(chunks[0]) if c else 0
        return range(first, first + len(chunks[c]))

    def sum_own():
        left = side_by_side(smooth, tiles, 0, rows)
        for first in range(0, tiles, most):
            sums = gathered(left, first)
            for s in range(most):
                own[first + s] = sums[:, s * tile_len : (s + 1) * tile_len]

    def await_entry(group, sem):
        later = jnp.int32(0)
        for o in group:
            later = later + jnp.where(source[o] > me_p, 1, 0)

        @pl.when(later > 0)
        def _():
            pl.semaphore_wait(enter_sem.at[sem], later)

    def send_back(c):
        for o in upper:
            sum_back(c, o)
        if c == 0:
            await_entry(upper, 0)
        for i in indices(c):
            for o in upper:
                copy_back(o, i).start()
        for o in lower:
            sum_back(c, o)
        for o in lower:

            @pl.when(source[o] < me_p)
            def _(o=o):
                for i in indices(c):
                    copy_back(o, i).start()

    send_back(0)

    def unpack(side, base):
        for i in range(wide // 2):
            pair = halo_in[side, i].astype(F32)
            levels[base + 2 * i] = pair[:, :members]
            levels[base + 2 * i + 1] = pair[:, members:]

    def clear(base):
        for i in range(wide):
            levels[base + i] = jnp.zeros(levels.shape[1:], F32)

    @pl.when(me_l > 0)
    def _():
        up.wait_recv()
        unpack(0, 0)

    @pl.when(me_l == 0)
    def _():
        clear(0)

    @pl.when(me_l < n_lev - 1)
    def _():
        down.wait_recv()
        unpack(1, wide + level_len)

    @pl.when(me_l == n_lev - 1)
    def _():
        clear(wide + level_len)

    for level in list(range(-half, half)) + list(range(level_len - half, level_len + half)):
        adjoint_level(level)
    for level in list(range(0, wide, 2)) + list(range(level_len - wide, level_len, 2)):
        forward_pair(level)

    send_back(1)
    await_entry(lower, 1)
    for o in lower:

        @pl.when(source[o] > me_p)
        def _(o=o):
            for i in range(len(numbered)):
                copy_back(o, i).start()

    sum_own()

    for i, (low, count) in enumerate(numbered):
        all_back(i).wait_recv()
        for t in range(tiles):
            value = own[t, pl.ds(low, count)]
            for o in range(link_len):
                value = value + arrived_back[i][o, slot_of[t, o]].astype(F32)
            ext[t, pl.ds(low, count)] = value.astype(BF16)
        for o in lower + upper:
            for s in range(most):
                sending[o, s, pl.ds(low, count)] = ext[send[0, s, o], pl.ds(low, count)]
            copy_forth(o, i).start()

    def spread(left, named, t):
        right = jnp.concatenate(
            [
                jnp.concatenate([conv[u, which[u, e]] for e in named], axis=0)
                for u in (t, t + 1)
            ],
            axis=1,
        )
        return jnp.dot(left, right, preferred_element_type=F32)

    def places():
        return [(0, parts[0][1], edge), (parts[1][0], edge, 0), (parts[1][0] + edge, edge, rows - edge)]

    def put(t, sums, fresh):
        for begin, count, place in places():
            for i in range(2):
                value = sums[begin : begin + count, i * tile_len : (i + 1) * tile_len]
                if not fresh:
                    value = value + mixed[t + i, pl.ds(place, count)]
                mixed[t + i, pl.ds(place, count)] = value

    left = side_by_side(ext, tiles, 0, rows)
    for t in range(0, tiles, 2):
        put(t, spread(left, range(tiles), t), True)
    for first, group in ((0, upper), (link_len // 2, lower)):
        all_forth(first, link_len // 2, first * 2 // link_len).wait_recv()
        left = jnp.concatenate(
            [side_by_side(arrived.at[o], most, 0, rows) for o in group], axis=1
        )
        named = [tiles + o * most + s for o in group for s in range(most)]
        for t in range(0, tiles, 2):
            put(t, spread(left, named, t), False)

    for t in range(tiles):
        part = jnp.concatenate(
            [mixed[t, pl.ds(m, level_len, stride=members), :] for m in range(members)], axis=0
        ).astype(BF16)
        result = jnp.dot(part, interp[t], preferred_element_type=F32)
        out[:, :, t * fine : (t + 1) * fine] = result.reshape(members, level_len, fine)
    for i in range(len(numbered)):
        all_back(i).wait_send()
    all_forth(0, link_len, 0).wait_send()

    @pl.when(me_l > 0)
    def _():
        down.wait_send()

    @pl.when(me_l < n_lev - 1)
    def _():
        up.wait_send()


def solution(mesh):
    n_patch, n_lev = mesh.shape["patch"], mesh.shape["lev"]

    def shards(fields, interp, conv_weight, vert_weight, send_tiles, tile_pattern):
        members, level_len, column_len = fields.shape
        tiles, tile_len, fine = interp.shape
        k_len = conv_weight.shape[1]
        link_len, most = send_tiles.shape[1:]
        wide = vert_weight.shape[1] - 1
        rows = members * level_len
        any_spec = pl.BlockSpec(memory_space=pl.ANY)
        entries = tiles + link_len * most
        words = -(-entries // (31 // k_len.bit_length()))
        weight, send = vert_weight.T, send_tiles.transpose(0, 2, 1)
        edge = 2 * wide * members
        sizes = [count for part in chunks_of([(0, rows - edge), (rows - edge, edge)]) for _, count in part]

        def per_link(count, size=rows):
            return pltpu.VMEM((link_len, count, size, tile_len), BF16)

        return pl.pallas_call(
            functools.partial(kernel, n_patch, n_lev),
            name="localize",
            out_shape=pltpu.VMEM(fields.shape, F32),
            in_specs=[any_spec] * 6,
            out_specs=pl.BlockSpec(memory_space=pltpu.VMEM),
            scratch_shapes=[
                pltpu.SMEM(weight.shape, F32),
                pltpu.SMEM(send.shape, jnp.int32),
                pltpu.SMEM(tile_pattern.shape, jnp.int32),
                pltpu.VMEM(fields.shape, BF16),
                pltpu.VMEM(interp.shape, BF16),
                pltpu.VMEM((tiles, k_len + 1, tile_len, tile_len), BF16),
                pltpu.VMEM((tiles, rows, tile_len), F32),
                pltpu.VMEM((level_len + 2 * wide, tiles, members, tile_len), F32),
                pltpu.VMEM((level_len + wide, tiles, members, tile_len), F32),
                pltpu.VMEM((2, wide // 2, tiles, 2 * members, tile_len), BF16),
                pltpu.VMEM((2, wide // 2, tiles, 2 * members, tile_len), BF16),
                pltpu.VMEM((tiles, rows, tile_len), F32),
                pltpu.VMEM((tiles, rows, tile_len), F32),
                pltpu.VMEM((tiles, rows, tile_len), BF16),
                pltpu.VMEM((tiles + 1, rows, tile_len), BF16),
                pltpu.SMEM((words, entries), jnp.int32),
                pltpu.SMEM((tiles, entries), jnp.int32),
                pltpu.SMEM((tiles, link_len), jnp.int32),
                pltpu.SemaphoreType.DMA((6,)),
                pltpu.SemaphoreType.DMA((4,)),
                pltpu.SemaphoreType.DMA((2,)),
                pltpu.SemaphoreType.DMA((len(sizes),)),
                pltpu.SemaphoreType.DMA((2,)),
                pltpu.SemaphoreType.REGULAR((2,)),
                pltpu.SemaphoreType.REGULAR,
            ]
            + [per_link(most)] * 3
            + [per_link(most + 1, size) for size in sizes],
            compiler_params=pltpu.CompilerParams(collective_id=0, has_side_effects=True),
        )(fields, interp, conv_weight, weight, send, tile_pattern)

    in_specs = (
        P(None, "lev", "patch"),
        P("patch", None, None),
        P("patch", None, None, None),
        P(),
        P("patch", None, None),
        P("patch", None),
    )
    out_specs = P(None, "lev", "patch")
    return jax.shard_map(shards, mesh=mesh, in_specs=in_specs, out_specs=out_specs, check_vma=False)
```

```python
import functools

import jax
import jax.numpy as jnp
from jax import lax
from jax.experimental import pallas as pl
from jax.experimental.pallas import tpu as pltpu
from jax.sharding import PartitionSpec as P

MESH = pl.DeviceIdType.MESH
F32 = jnp.float32
BF16 = jnp.bfloat16


def link_offsets(reach_len):
    return [
        position - reach_len if position < reach_len else position - reach_len + 1
        for position in range(2 * reach_len)
    ]


def chunks_of(parts):
    chunks = []
    for low, count in parts:
        step = count // 2 if count % 32 == 0 else count
        chunks.append([(low + at, step) for at in range(0, count, step)])
    return chunks


def dot_t(left, right):
    return lax.dot_general(left, right, (((1,), (1,)), ((), ())), preferred_element_type=F32)


def kernel(
    n_patch,
    n_lev,
    fields_hbm,
    interp_hbm,
    conv_hbm,
    weight_hbm,
    send_hbm,
    pattern_hbm,
    out,
    weight,
    send,
    pattern,
    fields,
    interp,
    conv,
    coarse,
    levels,
    middle,
    halo_out,
    halo_in,
    own,
    mixed,
    smooth,
    ext,
    power,
    which,
    slot_of,
    load_sem,
    halo_sem,
    send_sem,
    back_sem,
    forth_sem,
    enter_sem,
    enter_lev,
    returning,
    sending,
    arrived,
    *arrived_back,
):
    members, level_len, _ = fields.shape
    tiles, tile_len, fine = interp.shape
    k_len = conv_hbm.shape[1]
    most, link_len = send.shape[1], send.shape[2]
    half = (weight.shape[0] - 1) // 2
    wide = 2 * half
    rows = members * level_len
    total_levels = weight.shape[1]
    offsets = link_offsets(link_len // 2)
    edge = wide * members
    parts = [(0, rows - 2 * edge), (rows - 2 * edge, 2 * edge)]
    chunks = chunks_of(parts)
    numbered = [(low, count) for part in chunks for low, count in part]
    me_p, me_l = lax.axis_index("patch"), lax.axis_index("lev")
    partner = [lax.rem(me_p + d + n_patch, n_patch) for d in offsets]
    source = [lax.rem(me_p - d + n_patch, n_patch) for d in offsets]
    upper = sorted((o for o in range(link_len) if offsets[o] < 0), key=lambda o: offsets[o])
    lower = sorted((o for o in range(link_len) if offsets[o] > 0), key=lambda o: -offsets[o])

    load_w = pltpu.make_async_copy(weight_hbm, weight, load_sem.at[3])
    load_s = pltpu.make_async_copy(send_hbm, send, load_sem.at[4])
    load_p = pltpu.make_async_copy(pattern_hbm, pattern, load_sem.at[5])
    load_f = pltpu.make_async_copy(fields_hbm, fields, load_sem.at[0])
    load_i = pltpu.make_async_copy(interp_hbm, interp, load_sem.at[1])
    load_c = pltpu.make_async_copy(conv_hbm, conv.at[:, pl.ds(0, k_len)], load_sem.at[2])
    load_p.start()
    load_s.start()
    load_w.start()
    load_f.start()
    load_i.start()
    load_c.start()

    barrier = pltpu.get_barrier_semaphore()
    for o in range(link_len):

        @pl.when(partner[o] > me_p)
        def _(o=o):
            pl.semaphore_signal(
                barrier, inc=1, device_id={"patch": partner[o]}, device_id_type=MESH
            )

    @pl.when(me_l < n_lev - 1)
    def _():
        pl.semaphore_signal(barrier, inc=1, device_id={"lev": me_l + 1}, device_id_type=MESH)

    bits = k_len.bit_length()
    per_word = 31 // bits
    entries = tiles + link_len * most
    words = -(-entries // per_word)
    for e in range(entries):
        for w in range(words):
            inside = w * per_word <= e < (w + 1) * per_word
            power[w, e] = jnp.int32(1 << (bits * (e - w * per_word)) if inside else 0)
    for t in range(tiles):
        conv[t, k_len] = jnp.zeros((tile_len, tile_len), BF16)
    for i, (_, count) in enumerate(numbered):
        for o in range(link_len):
            arrived_back[i][o, most] = jnp.zeros((count, tile_len), BF16)
    ext[tiles] = jnp.zeros((rows, tile_len), BF16)
    before = jnp.where(me_l > 0, 1, 0)
    for o in range(link_len):
        before = before + jnp.where(partner[o] < me_p, 1, 0)

    @pl.when(before > 0)
    def _():
        pl.semaphore_wait(barrier, before)

    for o in range(link_len):

        @pl.when(partner[o] < me_p)
        def _(o=o):
            pl.semaphore_signal(
                enter_sem.at[0 if offsets[o] < 0 else 1],
                inc=1,
                device_id={"patch": partner[o]},
                device_id_type=MESH,
            )

    @pl.when(me_l > 0)
    def _():
        pl.semaphore_signal(enter_lev, inc=1, device_id={"lev": me_l - 1}, device_id_type=MESH)

    load_p.wait()
    load_s.wait()
    load_w.wait()
    load_f.wait()
    load_i.wait()
    empty = sum(k_len << (bits * i) for i in range(per_word))
    for t in range(tiles):
        packed = [jnp.int32(empty) for _ in range(words)]
        for k in range(k_len):
            named = pattern[t, k]
            for w in range(words):
                packed[w] = packed[w] + jnp.int32(k - k_len) * power[w, named]
        for e in range(entries):
            w, place = e // per_word, bits * (e % per_word)
            which[t, e] = (packed[w] >> place) & ((1 << bits) - 1)
        for o in range(link_len):
            index = jnp.int32(most)
            for s in range(most):
                index = jnp.where(send[0, s, o] == t, s, index)
            slot_of[t, o] = index
    for t in range(tiles):
        block = fields[:, :, t * fine : (t + 1) * fine].reshape(rows, fine)
        coarse[t] = dot_t(block, interp[t])
        for l in range(level_len):
            levels[wide + l, t] = coarse[t, pl.ds(l, members, stride=level_len), :]
    for i in range(wide // 2):
        low = jnp.concatenate([levels[wide + 2 * i], levels[wide + 2 * i + 1]], axis=1)
        top = level_len + 2 * i
        high = jnp.concatenate([levels[top], levels[top + 1]], axis=1)
        halo_out[0, i] = low.astype(BF16)
        halo_out[1, i] = high.astype(BF16)

    down = pltpu.make_async_remote_copy(
        halo_out.at[0],
        halo_in.at[1],
        halo_sem.at[0],
        halo_sem.at[1],
        device_id={"lev": lax.rem(me_l + n_lev - 1, n_lev)},
        device_id_type=MESH,
    )
    up = pltpu.make_async_remote_copy(
        halo_out.at[1],
        halo_in.at[0],
        halo_sem.at[2],
        halo_sem.at[3],
        device_id={"lev": lax.rem(me_l + 1, n_lev)},
        device_id_type=MESH,
    )

    @pl.when(me_l > 0)
    def _():
        down.start()

    @pl.when(me_l < n_lev - 1)
    def _():
        pl.semaphore_wait(enter_lev, 1)
        up.start()

    start = me_l * level_len

    def coefficient(level, column):
        return weight[column, jnp.clip(start + level, 0, total_levels - 1)]

    def adjoint_level(level):
        value = coefficient(level - half, wide) * levels[wide + level - half]
        for e in range(1 - half, half + 1):
            value = value + coefficient(level + e, half - e) * levels[wide + level + e]
        if level < 0:
            value = jnp.where(start + level >= 0, value, 0.0)
        if level >= level_len:
            value = jnp.where(start + level < total_levels, value, 0.0)
        middle[half + level] = value

    def forward_pair(level):
        both = []
        for l in (level, level + 1):
            value = coefficient(l, 0) * middle[l]
            for j in range(1, wide + 1):
                value = value + coefficient(l, j) * middle[l + j]
            both.append(value)
        pair = jnp.concatenate(both, axis=1).astype(BF16)
        if wide <= level < level_len - wide:
            place = (level - wide) * members
        else:
            place = level if level < wide else level - level_len + 2 * wide
            place = parts[1][0] + place * members
        smooth[:, pl.ds(place, 2 * members), :] = pair

    for level in range(half, level_len - half):
        adjoint_level(level)
    for level in range(wide, level_len - wide, 2):
        forward_pair(level)

    load_c.wait()

    def gathered(left, first):
        right = jnp.concatenate(
            [
                jnp.concatenate([conv[t, which[t, first + s]] for t in range(tiles)], axis=1)
                for s in range(most)
            ],
            axis=0,
        )
        return dot_t(left, right)

    def side_by_side(ref, count, low, size):
        return jnp.concatenate([ref[i, pl.ds(low, size)] for i in range(count)], axis=1)

    def sum_back(c, o):
        low, count = parts[c]
        left = side_by_side(smooth, tiles, low, count)
        sums = gathered(left, tiles + o * most).astype(BF16)
        for s in range(most):
            returning[o, s, pl.ds(low, count)] = sums[:, s * tile_len : (s + 1) * tile_len]

    def copy_back(o, i):
        low, count = numbered[i]
        return pltpu.make_async_remote_copy(
            returning.at[o, :, pl.ds(low, count)],
            arrived_back[i].at[o, pl.ds(0, most)],
            send_sem.at[0],
            back_sem.at[i],
            device_id={"patch": source[o]},
            device_id_type=MESH,
        )

    def copy_forth(o, i):
        low, count = numbered[i]
        return pltpu.make_async_remote_copy(
            sending.at[o, :, pl.ds(low, count)],
            arrived.at[o, :, pl.ds(low, count)],
            send_sem.at[1],
            forth_sem.at[0 if offsets[o] < 0 else 1],
            device_id={"patch": partner[o]},
            device_id_type=MESH,
        )

    def all_back(i):
        low, count = numbered[i]
        return pltpu.make_async_remote_copy(
            returning.at[:, :, pl.ds(low, count)],
            arrived_back[i].at[:, pl.ds(0, most)],
            send_sem.at[0],
            back_sem.at[i],
            device_id={"patch": source[0]},
            device_id_type=MESH,
        )

    def all_forth(first, count, sem):
        return pltpu.make_async_remote_copy(
            sending.at[pl.ds(first, count)],
            arrived.at[pl.ds(first, count)],
            send_sem.at[1],
            forth_sem.at[sem],
            device_id={"patch": partner[0]},
            device_id_type=MESH,
        )

    def indices(c):
        first = len(chunks[0]) if c else 0
        return range(first, first + len(chunks[c]))

    def sum_own():
        left = side_by_side(smooth, tiles, 0, rows)
        for first in range(0, tiles, most):
            sums = gathered(left, first)
            for s in range(most):
                own[first + s] = sums[:, s * tile_len : (s + 1) * tile_len]

    def await_entry(group, sem):
        later = jnp.int32(0)
        for o in group:
            later = later + jnp.where(source[o] > me_p, 1, 0)

        @pl.when(later > 0)
        def _():
            pl.semaphore_wait(enter_sem.at[sem], later)

    def send_back(c):
        for o in upper:
            sum_back(c, o)
        if c == 0:
            await_entry(upper, 0)
        for i in indices(c):
            for o in upper:
                copy_back(o, i).start()
        for o in lower:
            sum_back(c, o)
        for i in indices(c):
            for o in lower:
                if c == 0:

                    @pl.when(source[o] < me_p)
                    def _(o=o, i=i):
                        copy_back(o, i).start()

                else:
                    copy_back(o, i).start()

    send_back(0)

    def unpack(side, base):
        for i in range(wide // 2):
            pair = halo_in[side, i].astype(F32)
            levels[base + 2 * i] = pair[:, :members]
            levels[base + 2 * i + 1] = pair[:, members:]

    def clear(base):
        for i in range(wide):
            levels[base + i] = jnp.zeros(levels.shape[1:], F32)

    @pl.when(me_l > 0)
    def _():
        up.wait_recv()
        unpack(0, 0)

    @pl.when(me_l == 0)
    def _():
        clear(0)

    @pl.when(me_l < n_lev - 1)
    def _():
        down.wait_recv()
        unpack(1, wide + level_len)

    @pl.when(me_l == n_lev - 1)
    def _():
        clear(wide + level_len)

    for level in list(range(-half, half)) + list(range(level_len - half, level_len + half)):
        adjoint_level(level)
    for level in list(range(0, wide, 2)) + list(range(level_len - wide, level_len, 2)):
        forward_pair(level)

    await_entry(lower, 1)
    for i in indices(0):
        for o in lower:

            @pl.when(source[o] > me_p)
            def _(o=o, i=i):
                copy_back(o, i).start()

    send_back(1)
    sum_own()

    for i, (low, count) in enumerate(numbered):
        all_back(i).wait_recv()
        for t in range(tiles):
            value = own[t, pl.ds(low, count)]
            for o in range(link_len):
                value = value + arrived_back[i][o, slot_of[t, o]].astype(F32)
            ext[t, pl.ds(low, count)] = value.astype(BF16)
        for o in lower + upper:
            for s in range(most):
                sending[o, s, pl.ds(low, count)] = ext[send[0, s, o], pl.ds(low, count)]
            copy_forth(o, i).start()

    def spread(left, named, t):
        right = jnp.concatenate(
            [
                jnp.concatenate([conv[u, which[u, e]] for e in named], axis=0)
                for u in (t, t + 1)
            ],
            axis=1,
        )
        return jnp.dot(left, right, preferred_element_type=F32)

    def places():
        return [(0, parts[0][1], edge), (parts[1][0], edge, 0), (parts[1][0] + edge, edge, rows - edge)]

    def put(t, sums, fresh):
        for begin, count, place in places():
            for i in range(2):
                value = sums[begin : begin + count, i * tile_len : (i + 1) * tile_len]
                if not fresh:
                    value = value + mixed[t + i, pl.ds(place, count)]
                mixed[t + i, pl.ds(place, count)] = value

    def finish(first):
        for t in (first, first + 1):
            part = jnp.concatenate(
                [mixed[t, pl.ds(m, level_len, stride=members), :] for m in range(members)], axis=0
            ).astype(BF16)
            result = jnp.dot(part, interp[t], preferred_element_type=F32)
            out[:, :, t * fine : (t + 1) * fine] = result.reshape(members, level_len, fine)

    left = side_by_side(ext, tiles, 0, rows)
    for t in range(0, tiles, 2):
        put(t, spread(left, range(tiles), t), True)
    for first, group in ((0, upper), (link_len // 2, lower)):
        all_forth(first, link_len // 2, first * 2 // link_len).wait_recv()
        left = jnp.concatenate(
            [side_by_side(arrived.at[o], most, 0, rows) for o in group], axis=1
        )
        named = [tiles + o * most + s for o in group for s in range(most)]
        for t in range(0, tiles, 2):
            put(t, spread(left, named, t), False)
            if group is lower and t > 0:
                finish(t - 2)
    finish(tiles - 2)
    for i in range(len(numbered)):
        all_back(i).wait_send()
    all_forth(0, link_len, 0).wait_send()

    @pl.when(me_l > 0)
    def _():
        down.wait_send()

    @pl.when(me_l < n_lev - 1)
    def _():
        up.wait_send()


def solution(mesh):
    n_patch, n_lev = mesh.shape["patch"], mesh.shape["lev"]

    def shards(fields, interp, conv_weight, vert_weight, send_tiles, tile_pattern):
        members, level_len, column_len = fields.shape
        tiles, tile_len, fine = interp.shape
        k_len = conv_weight.shape[1]
        link_len, most = send_tiles.shape[1:]
        wide = vert_weight.shape[1] - 1
        rows = members * level_len
        any_spec = pl.BlockSpec(memory_space=pl.ANY)
        entries = tiles + link_len * most
        words = -(-entries // (31 // k_len.bit_length()))
        weight, send = vert_weight.T, send_tiles.transpose(0, 2, 1)
        edge = 2 * wide * members
        sizes = [count for part in chunks_of([(0, rows - edge), (rows - edge, edge)]) for _, count in part]

        def per_link(count, size=rows):
            return pltpu.VMEM((link_len, count, size, tile_len), BF16)

        return pl.pallas_call(
            functools.partial(kernel, n_patch, n_lev),
            name="localize",
            out_shape=pltpu.VMEM(fields.shape, F32),
            in_specs=[any_spec] * 6,
            out_specs=pl.BlockSpec(memory_space=pltpu.VMEM),
            scratch_shapes=[
                pltpu.SMEM(weight.shape, F32),
                pltpu.SMEM(send.shape, jnp.int32),
                pltpu.SMEM(tile_pattern.shape, jnp.int32),
                pltpu.VMEM(fields.shape, BF16),
                pltpu.VMEM(interp.shape, BF16),
                pltpu.VMEM((tiles, k_len + 1, tile_len, tile_len), BF16),
                pltpu.VMEM((tiles, rows, tile_len), F32),
                pltpu.VMEM((level_len + 2 * wide, tiles, members, tile_len), F32),
                pltpu.VMEM((level_len + wide, tiles, members, tile_len), F32),
                pltpu.VMEM((2, wide // 2, tiles, 2 * members, tile_len), BF16),
                pltpu.VMEM((2, wide // 2, tiles, 2 * members, tile_len), BF16),
                pltpu.VMEM((tiles, rows, tile_len), F32),
                pltpu.VMEM((tiles, rows, tile_len), F32),
                pltpu.VMEM((tiles, rows, tile_len), BF16),
                pltpu.VMEM((tiles + 1, rows, tile_len), BF16),
                pltpu.SMEM((words, entries), jnp.int32),
                pltpu.SMEM((tiles, entries), jnp.int32),
                pltpu.SMEM((tiles, link_len), jnp.int32),
                pltpu.SemaphoreType.DMA((6,)),
                pltpu.SemaphoreType.DMA((4,)),
                pltpu.SemaphoreType.DMA((2,)),
                pltpu.SemaphoreType.DMA((len(sizes),)),
                pltpu.SemaphoreType.DMA((2,)),
                pltpu.SemaphoreType.REGULAR((2,)),
                pltpu.SemaphoreType.REGULAR,
            ]
            + [per_link(most)] * 3
            + [per_link(most + 1, size) for size in sizes],
            compiler_params=pltpu.CompilerParams(collective_id=0, has_side_effects=True),
        )(fields, interp, conv_weight, weight, send, tile_pattern)

    in_specs = (
        P(None, "lev", "patch"),
        P("patch", None, None),
        P("patch", None, None, None),
        P(),
        P("patch", None, None),
        P("patch", None),
    )
    out_specs = P(None, "lev", "patch")
    return jax.shard_map(shards, mesh=mesh, in_specs=in_specs, out_specs=out_specs, check_vma=False)
```

```python
import functools

import jax
import jax.numpy as jnp
from jax import lax
from jax.experimental import pallas as pl
from jax.experimental.pallas import tpu as pltpu
from jax.sharding import PartitionSpec as P

MESH = pl.DeviceIdType.MESH
F32 = jnp.float32
BF16 = jnp.bfloat16


def link_offsets(reach_len):
    return [
        position - reach_len if position < reach_len else position - reach_len + 1
        for position in range(2 * reach_len)
    ]


def chunks_of(parts):
    chunks = []
    for low, count in parts:
        step = count // 2 if count % 32 == 0 else count
        chunks.append([(low + at, step) for at in range(0, count, step)])
    return chunks


def dot_t(left, right):
    return lax.dot_general(left, right, (((1,), (1,)), ((), ())), preferred_element_type=F32)


def kernel(
    n_patch,
    n_lev,
    fields_hbm,
    interp_hbm,
    conv_hbm,
    weight_hbm,
    send_hbm,
    pattern_hbm,
    out,
    weight,
    send,
    pattern,
    fields,
    interp,
    conv,
    turned,
    coarse,
    levels,
    middle,
    halo_out,
    halo_in,
    own,
    mixed,
    smooth,
    ext,
    power,
    which,
    slot_of,
    load_sem,
    halo_sem,
    send_sem,
    back_sem,
    forth_sem,
    enter_sem,
    enter_lev,
    returning,
    sending,
    arrived,
    *arrived_back,
):
    members, level_len, _ = fields.shape
    tiles, tile_len, fine = interp.shape
    k_len = conv_hbm.shape[1]
    most, link_len = send.shape[1], send.shape[2]
    half = (weight.shape[0] - 1) // 2
    wide = 2 * half
    rows = members * level_len
    total_levels = weight.shape[1]
    offsets = link_offsets(link_len // 2)
    edge = wide * members
    parts = [(0, rows - 2 * edge), (rows - 2 * edge, 2 * edge)]
    chunks = chunks_of(parts)
    numbered = [(low, count) for part in chunks for low, count in part]
    me_p, me_l = lax.axis_index("patch"), lax.axis_index("lev")
    partner = [lax.rem(me_p + d + n_patch, n_patch) for d in offsets]
    source = [lax.rem(me_p - d + n_patch, n_patch) for d in offsets]

    def rank(index):
        return jnp.where(index < n_patch - 4, index, 2 * n_patch - 5 - index)

    me_rank = rank(me_p)
    ahead = [rank(other) < me_rank for other in partner]
    behind = [rank(other) > me_rank for other in partner]
    answers = [rank(other) > me_rank for other in source]
    upper = sorted((o for o in range(link_len) if offsets[o] < 0), key=lambda o: offsets[o])
    lower = sorted((o for o in range(link_len) if offsets[o] > 0), key=lambda o: -offsets[o])

    load_w = pltpu.make_async_copy(weight_hbm, weight, load_sem.at[3])
    load_s = pltpu.make_async_copy(send_hbm, send, load_sem.at[4])
    load_p = pltpu.make_async_copy(pattern_hbm, pattern, load_sem.at[5])
    load_f = pltpu.make_async_copy(fields_hbm, fields, load_sem.at[0])
    load_i = pltpu.make_async_copy(interp_hbm, interp, load_sem.at[1])
    load_c = pltpu.make_async_copy(conv_hbm, conv.at[:, pl.ds(0, k_len)], load_sem.at[2])
    load_p.start()
    load_s.start()
    load_w.start()
    load_f.start()
    load_i.start()
    load_c.start()

    barrier = pltpu.get_barrier_semaphore()
    for o in range(link_len):

        @pl.when(behind[o])
        def _(o=o):
            pl.semaphore_signal(
                barrier, inc=1, device_id={"patch": partner[o]}, device_id_type=MESH
            )

    @pl.when(me_l < n_lev - 1)
    def _():
        pl.semaphore_signal(barrier, inc=1, device_id={"lev": me_l + 1}, device_id_type=MESH)

    bits = k_len.bit_length()
    per_word = 31 // bits
    entries = tiles + link_len * most
    words = -(-entries // per_word)
    for e in range(entries):
        for w in range(words):
            inside = w * per_word <= e < (w + 1) * per_word
            power[w, e] = jnp.int32(1 << (bits * (e - w * per_word)) if inside else 0)
    for t in range(tiles):
        conv[t, k_len] = jnp.zeros((tile_len, tile_len), BF16)
    for i, (_, count) in enumerate(numbered):
        for o in range(link_len):
            arrived_back[i][o, most] = jnp.zeros((count, tile_len), BF16)
    ext[tiles] = jnp.zeros((rows, tile_len), BF16)
    before = jnp.where(me_l > 0, 1, 0)
    for o in range(link_len):
        before = before + jnp.where(ahead[o], 1, 0)

    @pl.when(before > 0)
    def _():
        pl.semaphore_wait(barrier, before)

    for o in range(link_len):

        @pl.when(ahead[o])
        def _(o=o):
            wrapped = partner[o] < me_p if offsets[o] > 0 else partner[o] > me_p
            pl.semaphore_signal(
                enter_sem.at[jnp.where(wrapped, 1, 0)],
                inc=1,
                device_id={"patch": partner[o]},
                device_id_type=MESH,
            )

    @pl.when(me_l > 0)
    def _():
        pl.semaphore_signal(enter_lev, inc=1, device_id={"lev": me_l - 1}, device_id_type=MESH)

    load_f.wait()
    load_i.wait()
    down = []
    split = tiles // 2
    for h in range(2):
        for t in range(h * split, (h + 1) * split):
            block = fields[:, :, t * fine : (t + 1) * fine].reshape(rows, fine)
            coarse[t] = dot_t(block, interp[t])
            for l in range(level_len):
                levels[wide + l, t] = coarse[t, pl.ds(l, members, stride=level_len), :]
        some = pl.ds(h * split, split)
        for i in range(wide // 2):
            low = [levels[wide + 2 * i + n, some] for n in range(2)]
            high = [levels[level_len + 2 * i + n, some] for n in range(2)]
            halo_out[0, i, some] = jnp.concatenate(low, axis=1).astype(BF16)
            halo_out[1, i, some] = jnp.concatenate(high, axis=1).astype(BF16)
        down.append(
            pltpu.make_async_remote_copy(
                halo_out.at[0, :, some],
                halo_in.at[1, :, some],
                halo_sem.at[0],
                halo_sem.at[1],
                device_id={"lev": lax.rem(me_l + n_lev - 1, n_lev)},
                device_id_type=MESH,
            )
        )
        @pl.when(me_l > 0)
        def _(h=h):
            down[h].start()

    all_down = pltpu.make_async_remote_copy(
        halo_out.at[0],
        halo_in.at[1],
        halo_sem.at[0],
        halo_sem.at[1],
        device_id={"lev": lax.rem(me_l + n_lev - 1, n_lev)},
        device_id_type=MESH,
    )
    all_up = pltpu.make_async_remote_copy(
        halo_out.at[1],
        halo_in.at[0],
        halo_sem.at[2],
        halo_sem.at[3],
        device_id={"lev": lax.rem(me_l + 1, n_lev)},
        device_id_type=MESH,
    )

    @pl.when(me_l < n_lev - 1)
    def _():
        pl.semaphore_wait(enter_lev, 1)
        all_up.start()

    load_p.wait()
    load_s.wait()
    load_w.wait()
    empty = sum(k_len << (bits * i) for i in range(per_word))
    for t in range(tiles):
        packed = [jnp.int32(empty) for _ in range(words)]
        for k in range(k_len):
            named = pattern[t, k]
            for w in range(words):
                packed[w] = packed[w] + jnp.int32(k - k_len) * power[w, named]
        for e in range(entries):
            w, place = e // per_word, bits * (e % per_word)
            which[t, e] = (packed[w] >> place) & ((1 << bits) - 1)
        for o in range(link_len):
            index = jnp.int32(most)
            for s in range(most):
                index = jnp.where(send[0, s, o] == t, s, index)
            slot_of[t, o] = index
    start = me_l * level_len

    def coefficient(level, column):
        return weight[column, jnp.clip(start + level, 0, total_levels - 1)]

    def adjoint_level(level):
        value = coefficient(level - half, wide) * levels[wide + level - half]
        for e in range(1 - half, half + 1):
            value = value + coefficient(level + e, half - e) * levels[wide + level + e]
        if level < 0:
            value = jnp.where(start + level >= 0, value, 0.0)
        if level >= level_len:
            value = jnp.where(start + level < total_levels, value, 0.0)
        middle[half + level] = value

    def forward_pair(level):
        both = []
        for l in (level, level + 1):
            value = coefficient(l, 0) * middle[l]
            for j in range(1, wide + 1):
                value = value + coefficient(l, j) * middle[l + j]
            both.append(value)
        pair = jnp.concatenate(both, axis=1).astype(BF16)
        if wide <= level < level_len - wide:
            place = (level - wide) * members
        else:
            place = level if level < wide else level - level_len + 2 * wide
            place = parts[1][0] + place * members
        smooth[:, pl.ds(place, 2 * members), :] = pair

    for level in range(half, level_len - half):
        adjoint_level(level)
    for level in range(wide, level_len - wide, 2):
        forward_pair(level)

    load_c.wait()

    def gathered(left, first):
        right = jnp.concatenate(
            [
                jnp.concatenate([conv[t, which[t, first + s]] for t in range(tiles)], axis=1)
                for s in range(most)
            ],
            axis=0,
        )
        return dot_t(left, right)

    def gathered_turned(left, first):
        right = jnp.concatenate(
            [
                jnp.concatenate([turned[t, which[t, first + s]] for t in range(tiles)], axis=0)
                for s in range(most)
            ],
            axis=1,
        )
        return jnp.dot(left, right, preferred_element_type=F32)

    def side_by_side(ref, count, low, size):
        return jnp.concatenate([ref[i, pl.ds(low, size)] for i in range(count)], axis=1)

    def sum_back(c, o):
        low, count = parts[c]
        left = side_by_side(smooth, tiles, low, count)
        sums = (gathered_turned if c else gathered)(left, tiles + o * most).astype(BF16)
        for s in range(most):
            returning[o, s, pl.ds(low, count)] = sums[:, s * tile_len : (s + 1) * tile_len]

    def copy_back(o, i):
        low, count = numbered[i]
        return pltpu.make_async_remote_copy(
            returning.at[o, :, pl.ds(low, count)],
            arrived_back[i].at[o, pl.ds(0, most)],
            send_sem.at[0],
            back_sem.at[i],
            device_id={"patch": source[o]},
            device_id_type=MESH,
        )

    def copy_forth(o, i):
        low, count = numbered[i]
        return pltpu.make_async_remote_copy(
            sending.at[o, :, pl.ds(low, count)],
            arrived.at[o, :, pl.ds(low, count)],
            send_sem.at[1],
            forth_sem.at[0 if offsets[o] < 0 else 1],
            device_id={"patch": partner[o]},
            device_id_type=MESH,
        )

    def all_back(i):
        low, count = numbered[i]
        return pltpu.make_async_remote_copy(
            returning.at[:, :, pl.ds(low, count)],
            arrived_back[i].at[:, pl.ds(0, most)],
            send_sem.at[0],
            back_sem.at[i],
            device_id={"patch": source[0]},
            device_id_type=MESH,
        )

    def all_forth(first, count, sem):
        return pltpu.make_async_remote_copy(
            sending.at[pl.ds(first, count)],
            arrived.at[pl.ds(first, count)],
            send_sem.at[1],
            forth_sem.at[sem],
            device_id={"patch": partner[0]},
            device_id_type=MESH,
        )

    def indices(c):
        first = len(chunks[0]) if c else 0
        return range(first, first + len(chunks[c]))

    def sum_own():
        left = side_by_side(smooth, tiles, 0, rows)
        for first in range(0, tiles, most):
            sums = gathered_turned(left, first)
            for s in range(most):
                own[first + s] = sums[:, s * tile_len : (s + 1) * tile_len]

    def await_entry(group, wrapped):
        later = jnp.int32(0)
        for o in group:
            around = source[o] > me_p if offsets[o] > 0 else source[o] < me_p
            wanted = jnp.logical_and(answers[o], around == wrapped)
            later = later + jnp.where(wanted, 1, 0)

        @pl.when(later > 0)
        def _():
            pl.semaphore_wait(enter_sem.at[1 if wrapped else 0], later)

    def send_back(c):
        for o in upper:
            sum_back(c, o)
        if c == 0:
            await_entry(upper + lower, False)
        for i in indices(c):
            for o in upper:
                copy_back(o, i).start()
        for o in lower:
            sum_back(c, o)
        for i in indices(c):
            for o in lower:
                if c == 0:

                    @pl.when(source[o] < me_p)
                    def _(o=o, i=i):
                        copy_back(o, i).start()

                else:
                    copy_back(o, i).start()

    send_back(0)
    for t in range(tiles):
        for k in range(k_len + 1):
            turned[t, k] = conv[t, k].T

    def unpack(side, base):
        for i in range(wide // 2):
            pair = halo_in[side, i].astype(F32)
            levels[base + 2 * i] = pair[:, :members]
            levels[base + 2 * i + 1] = pair[:, members:]

    def clear(base):
        for i in range(wide):
            levels[base + i] = jnp.zeros(levels.shape[1:], F32)

    await_entry(upper + lower, True)
    for i in indices(0):
        for o in lower:

            @pl.when(source[o] > me_p)
            def _(o=o, i=i):
                copy_back(o, i).start()

    @pl.when(me_l > 0)
    def _():
        all_up.wait_recv()
        unpack(0, 0)

    @pl.when(me_l == 0)
    def _():
        clear(0)

    @pl.when(me_l < n_lev - 1)
    def _():
        all_down.wait_recv()
        unpack(1, wide + level_len)

    @pl.when(me_l == n_lev - 1)
    def _():
        clear(wide + level_len)

    for level in list(range(-half, half)) + list(range(level_len - half, level_len + half)):
        adjoint_level(level)
    for level in list(range(0, wide, 2)) + list(range(level_len - wide, level_len, 2)):
        forward_pair(level)

    send_back(1)
    sum_own()

    for i, (low, count) in enumerate(numbered):
        all_back(i).wait_recv()
        for t in range(tiles):
            value = own[t, pl.ds(low, count)]
            for o in range(link_len):
                value = value + arrived_back[i][o, slot_of[t, o]].astype(F32)
            ext[t, pl.ds(low, count)] = value.astype(BF16)
        for o in lower + upper:
            for s in range(most):
                sending[o, s, pl.ds(low, count)] = ext[send[0, s, o], pl.ds(low, count)]
        for o in lower:

            @pl.when(partner[o] < me_p)
            def _(o=o, i=i):
                copy_forth(o, i).start()

        for o in upper:
            copy_forth(o, i).start()
        for o in lower:

            @pl.when(partner[o] > me_p)
            def _(o=o, i=i):
                copy_forth(o, i).start()


    def spread(left, named, t):
        right = jnp.concatenate(
            [
                jnp.concatenate([conv[u, which[u, e]] for e in named], axis=0)
                for u in (t, t + 1)
            ],
            axis=1,
        )
        return jnp.dot(left, right, preferred_element_type=F32)

    def places():
        return [(0, parts[0][1], edge), (parts[1][0], edge, 0), (parts[1][0] + edge, edge, rows - edge)]

    def put(t, sums, fresh):
        for begin, count, place in places():
            for i in range(2):
                value = sums[begin : begin + count, i * tile_len : (i + 1) * tile_len]
                if not fresh:
                    value = value + mixed[t + i, pl.ds(place, count)]
                mixed[t + i, pl.ds(place, count)] = value

    def finish(first):
        for t in (first, first + 1):
            part = jnp.concatenate(
                [mixed[t, pl.ds(m, level_len, stride=members), :] for m in range(members)], axis=0
            ).astype(BF16)
            result = jnp.dot(part, interp[t], preferred_element_type=F32)
            out[:, :, t * fine : (t + 1) * fine] = result.reshape(members, level_len, fine)

    left = side_by_side(ext, tiles, 0, rows)
    for t in range(0, tiles, 2):
        put(t, spread(left, range(tiles), t), True)
    for first, group in ((0, upper), (link_len // 2, lower)):
        all_forth(first, link_len // 2, first * 2 // link_len).wait_recv()
        left = jnp.concatenate(
            [side_by_side(arrived.at[o], most, 0, rows) for o in group], axis=1
        )
        named = [tiles + o * most + s for o in group for s in range(most)]
        for t in range(0, tiles, 2):
            put(t, spread(left, named, t), False)
            if group is lower and t > 0:
                finish(t - 2)
    finish(tiles - 2)
    for i in range(len(numbered)):
        all_back(i).wait_send()
    all_forth(0, link_len, 0).wait_send()

    @pl.when(me_l > 0)
    def _():
        all_down.wait_send()

    @pl.when(me_l < n_lev - 1)
    def _():
        all_up.wait_send()


def solution(mesh):
    n_patch, n_lev = mesh.shape["patch"], mesh.shape["lev"]

    def shards(fields, interp, conv_weight, vert_weight, send_tiles, tile_pattern):
        members, level_len, column_len = fields.shape
        tiles, tile_len, fine = interp.shape
        k_len = conv_weight.shape[1]
        link_len, most = send_tiles.shape[1:]
        wide = vert_weight.shape[1] - 1
        rows = members * level_len
        any_spec = pl.BlockSpec(memory_space=pl.ANY)
        entries = tiles + link_len * most
        words = -(-entries // (31 // k_len.bit_length()))
        weight, send = vert_weight.T, send_tiles.transpose(0, 2, 1)
        edge = 2 * wide * members
        sizes = [count for part in chunks_of([(0, rows - edge), (rows - edge, edge)]) for _, count in part]

        def per_link(count, size=rows):
            return pltpu.VMEM((link_len, count, size, tile_len), BF16)

        return pl.pallas_call(
            functools.partial(kernel, n_patch, n_lev),
            name="localize",
            out_shape=pltpu.VMEM(fields.shape, F32),
            in_specs=[any_spec] * 6,
            out_specs=pl.BlockSpec(memory_space=pltpu.VMEM),
            scratch_shapes=[
                pltpu.SMEM(weight.shape, F32),
                pltpu.SMEM(send.shape, jnp.int32),
                pltpu.SMEM(tile_pattern.shape, jnp.int32),
                pltpu.VMEM(fields.shape, BF16),
                pltpu.VMEM(interp.shape, BF16),
                pltpu.VMEM((tiles, k_len + 1, tile_len, tile_len), BF16),
                pltpu.VMEM((tiles, k_len + 1, tile_len, tile_len), BF16),
                pltpu.VMEM((tiles, rows, tile_len), F32),
                pltpu.VMEM((level_len + 2 * wide, tiles, members, tile_len), F32),
                pltpu.VMEM((level_len + wide, tiles, members, tile_len), F32),
                pltpu.VMEM((2, wide // 2, tiles, 2 * members, tile_len), BF16),
                pltpu.VMEM((2, wide // 2, tiles, 2 * members, tile_len), BF16),
                pltpu.VMEM((tiles, rows, tile_len), F32),
                pltpu.VMEM((tiles, rows, tile_len), F32),
                pltpu.VMEM((tiles, rows, tile_len), BF16),
                pltpu.VMEM((tiles + 1, rows, tile_len), BF16),
                pltpu.SMEM((words, entries), jnp.int32),
                pltpu.SMEM((tiles, entries), jnp.int32),
                pltpu.SMEM((tiles, link_len), jnp.int32),
                pltpu.SemaphoreType.DMA((6,)),
                pltpu.SemaphoreType.DMA((4,)),
                pltpu.SemaphoreType.DMA((2,)),
                pltpu.SemaphoreType.DMA((len(sizes),)),
                pltpu.SemaphoreType.DMA((2,)),
                pltpu.SemaphoreType.REGULAR((2,)),
                pltpu.SemaphoreType.REGULAR,
            ]
            + [per_link(most)] * 3
            + [per_link(most + 1, size) for size in sizes],
            compiler_params=pltpu.CompilerParams(collective_id=0, has_side_effects=True),
        )(fields, interp, conv_weight, weight, send, tile_pattern)

    in_specs = (
        P(None, "lev", "patch"),
        P("patch", None, None),
        P("patch", None, None, None),
        P(),
        P("patch", None, None),
        P("patch", None),
    )
    out_specs = P(None, "lev", "patch")
    return jax.shard_map(shards, mesh=mesh, in_specs=in_specs, out_specs=out_specs, check_vma=False)
```

```python
import functools

import jax
import jax.numpy as jnp
from jax import lax
from jax.experimental import pallas as pl
from jax.experimental.pallas import tpu as pltpu
from jax.sharding import PartitionSpec as P

MESH = pl.DeviceIdType.MESH
F32 = jnp.float32
BF16 = jnp.bfloat16


def link_offsets(reach_len):
    return [
        position - reach_len if position < reach_len else position - reach_len + 1
        for position in range(2 * reach_len)
    ]


def chunks_of(parts):
    chunks = []
    for low, count in parts:
        step = count // 2 if count % 32 == 0 else count
        chunks.append([(low + at, step) for at in range(0, count, step)])
    return chunks


def dot_t(left, right):
    return lax.dot_general(left, right, (((1,), (1,)), ((), ())), preferred_element_type=F32)


def kernel(
    n_patch,
    n_lev,
    fields_hbm,
    interp_hbm,
    conv_hbm,
    weight_hbm,
    send_hbm,
    pattern_hbm,
    left_out,
    turn_out,
    base_out,
    weight,
    send,
    pattern,
    fields,
    interp,
    conv,
    turned,
    coarse,
    levels,
    middle,
    halo_out,
    halo_in,
    own,
    mixed,
    smooth,
    ext,
    power,
    which,
    slot_of,
    load_sem,
    halo_sem,
    send_sem,
    back_sem,
    forth_sem,
    enter_sem,
    enter_lev,
    returning,
    sending,
    arrived,
    *arrived_back,
):
    members, level_len, _ = fields.shape
    tiles, tile_len, fine = interp.shape
    k_len = conv_hbm.shape[1]
    most, link_len = send.shape[1], send.shape[2]
    half = (weight.shape[0] - 1) // 2
    wide = 2 * half
    rows = members * level_len
    total_levels = weight.shape[1]
    offsets = link_offsets(link_len // 2)
    edge = wide * members
    parts = [(0, rows - 2 * edge), (rows - 2 * edge, 2 * edge)]
    chunks = chunks_of(parts)
    numbered = [(low, count) for part in chunks for low, count in part]
    me_p, me_l = lax.axis_index("patch"), lax.axis_index("lev")
    partner = [lax.rem(me_p + d + n_patch, n_patch) for d in offsets]
    source = [lax.rem(me_p - d + n_patch, n_patch) for d in offsets]

    def rank(index):
        return jnp.where(index < n_patch - 4, index, 2 * n_patch - 5 - index)

    me_rank = rank(me_p)
    ahead = [rank(other) < me_rank for other in partner]
    behind = [rank(other) > me_rank for other in partner]
    answers = [rank(other) > me_rank for other in source]
    upper = sorted((o for o in range(link_len) if offsets[o] < 0), key=lambda o: offsets[o])
    lower = sorted((o for o in range(link_len) if offsets[o] > 0), key=lambda o: -offsets[o])

    load_w = pltpu.make_async_copy(weight_hbm, weight, load_sem.at[3])
    load_s = pltpu.make_async_copy(send_hbm, send, load_sem.at[4])
    load_p = pltpu.make_async_copy(pattern_hbm, pattern, load_sem.at[5])
    load_f = pltpu.make_async_copy(fields_hbm, fields, load_sem.at[0])
    load_i = pltpu.make_async_copy(interp_hbm, interp, load_sem.at[1])
    load_c = pltpu.make_async_copy(conv_hbm, conv.at[:, pl.ds(0, k_len)], load_sem.at[2])
    load_p.start()
    load_s.start()
    load_w.start()
    load_f.start()
    load_i.start()
    load_c.start()

    barrier = pltpu.get_barrier_semaphore()
    for o in range(link_len):

        @pl.when(behind[o])
        def _(o=o):
            pl.semaphore_signal(
                barrier, inc=1, device_id={"patch": partner[o]}, device_id_type=MESH
            )

    @pl.when(me_l < n_lev - 1)
    def _():
        pl.semaphore_signal(barrier, inc=1, device_id={"lev": me_l + 1}, device_id_type=MESH)

    bits = k_len.bit_length()
    per_word = 31 // bits
    entries = tiles + link_len * most
    words = -(-entries // per_word)
    for e in range(entries):
        for w in range(words):
            inside = w * per_word <= e < (w + 1) * per_word
            power[w, e] = jnp.int32(1 << (bits * (e - w * per_word)) if inside else 0)
    for t in range(tiles):
        conv[t, k_len] = jnp.zeros((tile_len, tile_len), BF16)
    for i, (_, count) in enumerate(numbered):
        for o in range(link_len):
            arrived_back[i][o, most] = jnp.zeros((count, tile_len), BF16)
    ext[tiles] = jnp.zeros((rows, tile_len), BF16)
    eager = jnp.logical_or(me_p < n_patch - 4, me_p >= n_patch - 2)

    def enter():
        before = jnp.where(me_l > 0, 1, 0)
        for o in range(link_len):
            before = before + jnp.where(ahead[o], 1, 0)

        @pl.when(before > 0)
        def _():
            pl.semaphore_wait(barrier, before)

        for o in range(link_len):

            @pl.when(ahead[o])
            def _(o=o):
                wrapped = partner[o] < me_p if offsets[o] > 0 else partner[o] > me_p
                pl.semaphore_signal(
                    enter_sem.at[jnp.where(wrapped, 1, 0)],
                    inc=1,
                    device_id={"patch": partner[o]},
                    device_id_type=MESH,
                )

        @pl.when(me_l > 0)
        def _():
            pl.semaphore_signal(enter_lev, inc=1, device_id={"lev": me_l - 1}, device_id_type=MESH)

    pl.when(eager)(enter)
    load_f.wait()
    load_i.wait()
    load_p.wait()
    load_s.wait()
    load_w.wait()
    empty = sum(k_len << (bits * i) for i in range(per_word))
    for t in range(tiles):
        packed = [jnp.int32(empty) for _ in range(words)]
        for k in range(k_len):
            named = pattern[t, k]
            for w in range(words):
                packed[w] = packed[w] + jnp.int32(k - k_len) * power[w, named]
        for e in range(entries):
            w, place = e // per_word, bits * (e % per_word)
            which[t, e] = (packed[w] >> place) & ((1 << bits) - 1)
        for o in range(link_len):
            index = jnp.int32(most)
            for s in range(most):
                index = jnp.where(send[0, s, o] == t, s, index)
            slot_of[t, o] = index
    down = []
    split = tiles // 2
    for h in range(2):
        for t in range(h * split, (h + 1) * split):
            block = fields[:, :, t * fine : (t + 1) * fine].reshape(rows, fine)
            coarse[t] = dot_t(block, interp[t])
            for l in range(level_len):
                levels[wide + l, t] = coarse[t, pl.ds(l, members, stride=level_len), :]
        some = pl.ds(h * split, split)
        for i in range(wide // 2):
            low = [levels[wide + 2 * i + n, some] for n in range(2)]
            high = [levels[level_len + 2 * i + n, some] for n in range(2)]
            halo_out[0, i, some] = jnp.concatenate(low, axis=1).astype(BF16)
            halo_out[1, i, some] = jnp.concatenate(high, axis=1).astype(BF16)
        down.append(
            pltpu.make_async_remote_copy(
                halo_out.at[0, :, some],
                halo_in.at[1, :, some],
                halo_sem.at[0],
                halo_sem.at[1],
                device_id={"lev": lax.rem(me_l + n_lev - 1, n_lev)},
                device_id_type=MESH,
            )
        )
        if h == 0:
            pl.when(jnp.logical_not(eager))(enter)

        @pl.when(me_l > 0)
        def _(h=h):
            down[h].start()

    all_down = pltpu.make_async_remote_copy(
        halo_out.at[0],
        halo_in.at[1],
        halo_sem.at[0],
        halo_sem.at[1],
        device_id={"lev": lax.rem(me_l + n_lev - 1, n_lev)},
        device_id_type=MESH,
    )
    all_up = pltpu.make_async_remote_copy(
        halo_out.at[1],
        halo_in.at[0],
        halo_sem.at[2],
        halo_sem.at[3],
        device_id={"lev": lax.rem(me_l + 1, n_lev)},
        device_id_type=MESH,
    )

    start = me_l * level_len

    def coefficient(level, column):
        return weight[column, jnp.clip(start + level, 0, total_levels - 1)]

    def adjoint_level(level):
        value = coefficient(level - half, wide) * levels[wide + level - half]
        for e in range(1 - half, half + 1):
            value = value + coefficient(level + e, half - e) * levels[wide + level + e]
        if level < 0:
            value = jnp.where(start + level >= 0, value, 0.0)
        if level >= level_len:
            value = jnp.where(start + level < total_levels, value, 0.0)
        middle[half + level] = value

    def forward_pair(level):
        both = []
        for l in (level, level + 1):
            value = coefficient(l, 0) * middle[l]
            for j in range(1, wide + 1):
                value = value + coefficient(l, j) * middle[l + j]
            both.append(value)
        pair = jnp.concatenate(both, axis=1).astype(BF16)
        if wide <= level < level_len - wide:
            place = (level - wide) * members
        else:
            place = level if level < wide else level - level_len + 2 * wide
            place = parts[1][0] + place * members
        smooth[:, pl.ds(place, 2 * members), :] = pair

    for level in range(half, level_len - half):
        adjoint_level(level)
    for level in range(wide, level_len - wide, 2):
        forward_pair(level)

    load_c.wait()

    def gathered(left, first):
        right = jnp.concatenate(
            [
                jnp.concatenate([conv[t, which[t, first + s]] for t in range(tiles)], axis=1)
                for s in range(most)
            ],
            axis=0,
        )
        return dot_t(left, right)

    def gathered_turned(left, first):
        right = jnp.concatenate(
            [
                jnp.concatenate([turned[t, which[t, first + s]] for t in range(tiles)], axis=0)
                for s in range(most)
            ],
            axis=1,
        )
        return jnp.dot(left, right, preferred_element_type=F32)

    def side_by_side(ref, count, low, size):
        return jnp.concatenate([ref[i, pl.ds(low, size)] for i in range(count)], axis=1)

    def sum_back(c, o):
        low, count = parts[c]
        left = side_by_side(smooth, tiles, low, count)
        sums = (gathered_turned if c else gathered)(left, tiles + o * most).astype(BF16)
        for s in range(most):
            returning[o, s, pl.ds(low, count)] = sums[:, s * tile_len : (s + 1) * tile_len]

    def copy_back(o, i):
        low, count = numbered[i]
        return pltpu.make_async_remote_copy(
            returning.at[o, :, pl.ds(low, count)],
            arrived_back[i].at[o, pl.ds(0, most)],
            send_sem.at[0],
            back_sem.at[i],
            device_id={"patch": source[o]},
            device_id_type=MESH,
        )

    def copy_forth(o, i):
        low, count = numbered[i]
        return pltpu.make_async_remote_copy(
            sending.at[o, :, pl.ds(low, count)],
            arrived.at[o, :, pl.ds(low, count)],
            send_sem.at[1],
            forth_sem.at[0 if offsets[o] < 0 else 1],
            device_id={"patch": partner[o]},
            device_id_type=MESH,
        )

    def all_back(i):
        low, count = numbered[i]
        return pltpu.make_async_remote_copy(
            returning.at[:, :, pl.ds(low, count)],
            arrived_back[i].at[:, pl.ds(0, most)],
            send_sem.at[0],
            back_sem.at[i],
            device_id={"patch": source[0]},
            device_id_type=MESH,
        )

    def all_forth(first, count, sem):
        return pltpu.make_async_remote_copy(
            sending.at[pl.ds(first, count)],
            arrived.at[pl.ds(first, count)],
            send_sem.at[1],
            forth_sem.at[sem],
            device_id={"patch": partner[0]},
            device_id_type=MESH,
        )

    def indices(c):
        first = len(chunks[0]) if c else 0
        return range(first, first + len(chunks[c]))

    def sum_own():
        left = side_by_side(smooth, tiles, 0, rows)
        for first in range(0, tiles, most):
            sums = gathered_turned(left, first)
            for s in range(most):
                own[first + s] = sums[:, s * tile_len : (s + 1) * tile_len]

    def await_entry(group, wrapped):
        later = jnp.int32(0)
        for o in group:
            around = source[o] > me_p if offsets[o] > 0 else source[o] < me_p
            wanted = jnp.logical_and(answers[o], around == wrapped)
            later = later + jnp.where(wanted, 1, 0)

        @pl.when(later > 0)
        def _():
            pl.semaphore_wait(enter_sem.at[1 if wrapped else 0], later)

    def send_back(c):
        for o in upper:
            sum_back(c, o)
        if c == 0:
            await_entry(upper + lower, False)
        for i in indices(c):
            for o in upper:
                copy_back(o, i).start()
        if c == 0:

            @pl.when(me_l < n_lev - 1)
            def _():
                pl.semaphore_wait(enter_lev, 1)
                all_up.start()

        for o in lower:
            sum_back(c, o)
        for i in indices(c):
            for o in lower:
                if c == 0:

                    @pl.when(source[o] < me_p)
                    def _(o=o, i=i):
                        copy_back(o, i).start()

                else:
                    copy_back(o, i).start()

    send_back(0)
    for t in range(tiles):
        for k in range(k_len + 1):
            turned[t, k] = conv[t, k].T

    def unpack(side, base):
        for i in range(wide // 2):
            pair = halo_in[side, i].astype(F32)
            levels[base + 2 * i] = pair[:, :members]
            levels[base + 2 * i + 1] = pair[:, members:]

    def clear(base):
        for i in range(wide):
            levels[base + i] = jnp.zeros(levels.shape[1:], F32)

    await_entry(upper + lower, True)
    for i in indices(0):
        for o in lower:

            @pl.when(source[o] > me_p)
            def _(o=o, i=i):
                copy_back(o, i).start()

    @pl.when(me_l > 0)
    def _():
        all_up.wait_recv()
        unpack(0, 0)

    @pl.when(me_l == 0)
    def _():
        clear(0)

    @pl.when(me_l < n_lev - 1)
    def _():
        all_down.wait_recv()
        unpack(1, wide + level_len)

    @pl.when(me_l == n_lev - 1)
    def _():
        clear(wide + level_len)

    for level in list(range(-half, half)) + list(range(level_len - half, level_len + half)):
        adjoint_level(level)
    for level in list(range(0, wide, 2)) + list(range(level_len - wide, level_len, 2)):
        forward_pair(level)

    send_back(1)
    sum_own()

    for i, (low, count) in enumerate(numbered):
        all_back(i).wait_recv()
        for t in range(tiles):
            value = own[t, pl.ds(low, count)]
            for o in range(link_len):
                value = value + arrived_back[i][o, slot_of[t, o]].astype(F32)
            ext[t, pl.ds(low, count)] = value.astype(BF16)
        for o in lower + upper:
            for s in range(most):
                sending[o, s, pl.ds(low, count)] = ext[send[0, s, o], pl.ds(low, count)]
        for o in lower:

            @pl.when(partner[o] < me_p)
            def _(o=o, i=i):
                copy_forth(o, i).start()

        for o in upper:
            copy_forth(o, i).start()
        for o in lower:

            @pl.when(partner[o] > me_p)
            def _(o=o, i=i):
                copy_forth(o, i).start()


    def spread(left, named, t):
        right = jnp.concatenate(
            [
                jnp.concatenate([conv[u, which[u, e]] for e in named], axis=0)
                for u in (t, t + 1)
            ],
            axis=1,
        )
        return jnp.dot(left, right, preferred_element_type=F32)

    def add(left, named, fresh):
        for t in range(0, tiles, 2):
            sums = spread(left, named, t)
            for i in range(2):
                value = sums[:, i * tile_len : (i + 1) * tile_len]
                mixed[t + i] = value if fresh else value + mixed[t + i]

    def received(group):
        return jnp.concatenate(
            [side_by_side(arrived.at[o], most, 0, rows) for o in group], axis=1
        )

    def entries_of(group):
        return [tiles + o * most + s for o in group for s in range(most)]

    add(side_by_side(ext, tiles, 0, rows), range(tiles), True)
    for t in range(tiles):
        stack = jnp.concatenate([conv[t, which[t, e]] for e in entries_of(lower)], axis=0)
        turn_out[t] = jnp.dot(stack, interp[t], preferred_element_type=F32).astype(BF16)
    all_forth(0, link_len // 2, 0).wait_recv()
    add(received(upper), entries_of(upper), False)
    for t in range(tiles):
        base_out[t] = jnp.dot(mixed[t].astype(BF16), interp[t], preferred_element_type=F32)
    all_forth(link_len // 2, link_len // 2, 1).wait_recv()
    left_out[...] = received(lower)
    for i in range(len(numbered)):
        all_back(i).wait_send()
    all_forth(0, link_len, 0).wait_send()

    @pl.when(me_l > 0)
    def _():
        all_down.wait_send()

    @pl.when(me_l < n_lev - 1)
    def _():
        all_up.wait_send()


def finish(places, left, turn, base, out_hbm, out, sem):
    tiles, _, fine = turn.shape
    level_len = out.shape[1]
    copies = []
    for t in range(tiles):
        sums = base[t] + jnp.dot(left[...], turn[t], preferred_element_type=F32)
        columns = pl.ds(t * fine, fine)
        for row, level in places:
            out[:, level, columns] = sums[row : row + out.shape[0]]
        copy = pltpu.make_async_copy(out.at[:, :, columns], out_hbm.at[:, :, columns], sem.at[t])
        copy.start()
        copies.append(copy)
    for copy in copies:
        copy.wait()


def solution(mesh):
    n_patch, n_lev = mesh.shape["patch"], mesh.shape["lev"]

    def shards(fields, interp, conv_weight, vert_weight, send_tiles, tile_pattern):
        members, level_len, column_len = fields.shape
        tiles, tile_len, fine = interp.shape
        k_len = conv_weight.shape[1]
        link_len, most = send_tiles.shape[1:]
        wide = vert_weight.shape[1] - 1
        rows = members * level_len
        any_spec = pl.BlockSpec(memory_space=pl.ANY)
        entries = tiles + link_len * most
        words = -(-entries // (31 // k_len.bit_length()))
        weight, send = vert_weight.T, send_tiles.transpose(0, 2, 1)
        edge = 2 * wide * members
        sizes = [count for part in chunks_of([(0, rows - edge), (rows - edge, edge)]) for _, count in part]

        def per_link(count, size=rows):
            return pltpu.VMEM((link_len, count, size, tile_len), BF16)

        vmem_spec = pl.BlockSpec(memory_space=pltpu.VMEM)
        half_len = link_len // 2 * most * tile_len
        order = list(range(wide, level_len - wide))
        order += list(range(wide)) + list(range(level_len - wide, level_len))
        places = [(i * members, level) for i, level in enumerate(order)]

        left, turn, base = pl.pallas_call(
            functools.partial(kernel, n_patch, n_lev),
            name="localize",
            out_shape=[
                pltpu.VMEM((rows, half_len), BF16),
                pltpu.VMEM((tiles, half_len, fine), BF16),
                pltpu.VMEM((tiles, rows, fine), F32),
            ],
            in_specs=[any_spec] * 6,
            out_specs=[vmem_spec] * 3,
            scratch_shapes=[
                pltpu.SMEM(weight.shape, F32),
                pltpu.SMEM(send.shape, jnp.int32),
                pltpu.SMEM(tile_pattern.shape, jnp.int32),
                pltpu.VMEM(fields.shape, BF16),
                pltpu.VMEM(interp.shape, BF16),
                pltpu.VMEM((tiles, k_len + 1, tile_len, tile_len), BF16),
                pltpu.VMEM((tiles, k_len + 1, tile_len, tile_len), BF16),
                pltpu.VMEM((tiles, rows, tile_len), F32),
                pltpu.VMEM((level_len + 2 * wide, tiles, members, tile_len), F32),
                pltpu.VMEM((level_len + wide, tiles, members, tile_len), F32),
                pltpu.VMEM((2, wide // 2, tiles, 2 * members, tile_len), BF16),
                pltpu.VMEM((2, wide // 2, tiles, 2 * members, tile_len), BF16),
                pltpu.VMEM((tiles, rows, tile_len), F32),
                pltpu.VMEM((tiles, rows, tile_len), F32),
                pltpu.VMEM((tiles, rows, tile_len), BF16),
                pltpu.VMEM((tiles + 1, rows, tile_len), BF16),
                pltpu.SMEM((words, entries), jnp.int32),
                pltpu.SMEM((tiles, entries), jnp.int32),
                pltpu.SMEM((tiles, link_len), jnp.int32),
                pltpu.SemaphoreType.DMA((6,)),
                pltpu.SemaphoreType.DMA((4,)),
                pltpu.SemaphoreType.DMA((2,)),
                pltpu.SemaphoreType.DMA((len(sizes),)),
                pltpu.SemaphoreType.DMA((2,)),
                pltpu.SemaphoreType.REGULAR((2,)),
                pltpu.SemaphoreType.REGULAR,
            ]
            + [per_link(most)] * 3
            + [per_link(most + 1, size) for size in sizes],
            compiler_params=pltpu.CompilerParams(collective_id=0, has_side_effects=True),
        )(fields, interp, conv_weight, weight, send, tile_pattern)
        return pl.pallas_call(
            functools.partial(finish, places),
            name="finish",
            out_shape=jax.ShapeDtypeStruct(fields.shape, F32),
            in_specs=[vmem_spec] * 3,
            out_specs=any_spec,
            scratch_shapes=[
                pltpu.VMEM(fields.shape, F32),
                pltpu.SemaphoreType.DMA((tiles,)),
            ],
            compiler_params=pltpu.CompilerParams(vmem_limit_bytes=8 << 20),
        )(left, turn, base)

    in_specs = (
        P(None, "lev", "patch"),
        P("patch", None, None),
        P("patch", None, None, None),
        P(),
        P("patch", None, None),
        P("patch", None),
    )
    out_specs = P(None, "lev", "patch")
    return jax.shard_map(shards, mesh=mesh, in_specs=in_specs, out_specs=out_specs, check_vma=False)
```

```python
import functools

import jax
import jax.numpy as jnp
from jax import lax
from jax.experimental import pallas as pl
from jax.experimental.pallas import tpu as pltpu
from jax.sharding import PartitionSpec as P

MESH = pl.DeviceIdType.MESH
F32 = jnp.float32
BF16 = jnp.bfloat16


def link_offsets(reach_len):
    return [
        position - reach_len if position < reach_len else position - reach_len + 1
        for position in range(2 * reach_len)
    ]


def chunks_of(parts):
    chunks = []
    for low, count in parts:
        step = 32 if count % 32 == 0 else count
        chunks.append([(low + at, step) for at in range(0, count, step)])
    return chunks


def split_rows(n_lev, level_len, members, wide):
    early = level_len - wide if n_lev == 2 else level_len - 2 * wide
    return [(0, early * members), (early * members, (level_len - early) * members)]


def dot_t(left, right):
    return lax.dot_general(left, right, (((1,), (1,)), ((), ())), preferred_element_type=F32)


def kernel(
    n_patch,
    n_lev,
    fields_hbm,
    interp_hbm,
    conv_hbm,
    weight_hbm,
    send_hbm,
    pattern_hbm,
    left_out,
    turn_out,
    base_out,
    weight,
    send,
    pattern,
    fields,
    interp,
    conv,
    turned,
    coarse,
    levels,
    middle,
    halo_out,
    halo_in,
    own,
    mixed,
    smooth,
    ext,
    power,
    which,
    slot_of,
    load_sem,
    halo_sem,
    send_sem,
    back_sem,
    forth_sem,
    enter_sem,
    enter_lev,
    returning,
    sending,
    arrived,
    *arrived_back,
):
    members, level_len, _ = fields.shape
    tiles, tile_len, fine = interp.shape
    k_len = conv_hbm.shape[1]
    most, link_len = send.shape[1], send.shape[2]
    half = (weight.shape[0] - 1) // 2
    wide = 2 * half
    rows = members * level_len
    total_levels = weight.shape[1]
    offsets = link_offsets(link_len // 2)
    two = n_lev == 2
    parts = split_rows(n_lev, level_len, members, wide)
    chunks = chunks_of(parts)
    numbered = [(low, count) for part in chunks for low, count in part]
    me_p, me_l = lax.axis_index("patch"), lax.axis_index("lev")
    partner = [lax.rem(me_p + d + n_patch, n_patch) for d in offsets]
    source = [lax.rem(me_p - d + n_patch, n_patch) for d in offsets]

    order = list(range(wide, level_len - wide))
    order += list(range(wide)) + list(range(level_len - wide, level_len))

    def turned_level(index):
        return jnp.where(me_l == 0, index, level_len - 1 - index) if two else index

    def level_of(group):
        return turned_level(group) if two else order[group]

    def rank(index):
        return jnp.where(index < n_patch - 4, index, 2 * n_patch - 5 - index)

    me_rank = rank(me_p)
    ahead = [rank(other) < me_rank for other in partner]
    behind = [rank(other) > me_rank for other in partner]
    answers = [rank(other) > me_rank for other in source]
    upper = sorted((o for o in range(link_len) if offsets[o] < 0), key=lambda o: offsets[o])
    lower = sorted((o for o in range(link_len) if offsets[o] > 0), key=lambda o: -offsets[o])

    load_w = pltpu.make_async_copy(weight_hbm, weight, load_sem.at[3])
    load_s = pltpu.make_async_copy(send_hbm, send, load_sem.at[4])
    load_p = pltpu.make_async_copy(pattern_hbm, pattern, load_sem.at[5])
    load_f = pltpu.make_async_copy(fields_hbm, fields, load_sem.at[0])
    load_i = pltpu.make_async_copy(interp_hbm, interp, load_sem.at[1])
    load_c = pltpu.make_async_copy(conv_hbm, conv.at[:, pl.ds(0, k_len)], load_sem.at[2])
    load_p.start()
    load_s.start()
    load_w.start()
    load_f.start()
    load_i.start()
    load_c.start()

    barrier = pltpu.get_barrier_semaphore()
    for o in range(link_len):

        @pl.when(behind[o])
        def _(o=o):
            pl.semaphore_signal(
                barrier, inc=1, device_id={"patch": partner[o]}, device_id_type=MESH
            )

    @pl.when(me_l < n_lev - 1)
    def _():
        pl.semaphore_signal(barrier, inc=1, device_id={"lev": me_l + 1}, device_id_type=MESH)

    bits = k_len.bit_length()
    per_word = 31 // bits
    entries = tiles + link_len * most
    words = -(-entries // per_word)
    for e in range(entries):
        for w in range(words):
            inside = w * per_word <= e < (w + 1) * per_word
            power[w, e] = jnp.int32(1 << (bits * (e - w * per_word)) if inside else 0)
    for t in range(tiles):
        conv[t, k_len] = jnp.zeros((tile_len, tile_len), BF16)
    for i, (_, count) in enumerate(numbered):
        for o in range(link_len):
            arrived_back[i][o, most] = jnp.zeros((count, tile_len), BF16)
    ext[tiles] = jnp.zeros((rows, tile_len), BF16)
    eager = jnp.logical_or(me_p < n_patch - 4, me_p >= n_patch - 2)

    def enter():
        before = jnp.where(me_l > 0, 1, 0)
        for o in range(link_len):
            before = before + jnp.where(ahead[o], 1, 0)

        @pl.when(before > 0)
        def _():
            pl.semaphore_wait(barrier, before)

        for o in range(link_len):

            @pl.when(ahead[o])
            def _(o=o):
                wrapped = partner[o] < me_p if offsets[o] > 0 else partner[o] > me_p
                pl.semaphore_signal(
                    enter_sem.at[jnp.where(wrapped, 1, 0)],
                    inc=1,
                    device_id={"patch": partner[o]},
                    device_id_type=MESH,
                )

        @pl.when(me_l > 0)
        def _():
            pl.semaphore_signal(enter_lev, inc=1, device_id={"lev": me_l - 1}, device_id_type=MESH)

    pl.when(eager)(enter)
    load_f.wait()
    load_i.wait()
    load_p.wait()
    load_s.wait()
    load_w.wait()
    empty = sum(k_len << (bits * i) for i in range(per_word))
    for t in range(tiles):
        packed = [jnp.int32(empty) for _ in range(words)]
        for k in range(k_len):
            named = pattern[t, k]
            for w in range(words):
                packed[w] = packed[w] + jnp.int32(k - k_len) * power[w, named]
        for e in range(entries):
            w, place = e // per_word, bits * (e % per_word)
            which[t, e] = (packed[w] >> place) & ((1 << bits) - 1)
        for o in range(link_len):
            index = jnp.int32(most)
            for s in range(most):
                index = jnp.where(send[0, s, o] == t, s, index)
            slot_of[t, o] = index
    split = tiles // 2
    below = {"lev": lax.rem(me_l + n_lev - 1, n_lev)}
    above = {"lev": lax.rem(me_l + 1, n_lev)}

    def exchange(side, place, to, some=slice(None)):
        return pltpu.make_async_remote_copy(
            halo_out.at[side, :, some],
            halo_in.at[place, :, some],
            halo_sem.at[2 * side],
            halo_sem.at[2 * side + 1],
            device_id=to,
            device_id_type=MESH,
        )

    down = exchange(0, 1, below)
    up = down if two else exchange(1, 0, above)
    for h in range(2):
        for t in range(h * split, (h + 1) * split):
            block = fields[:, :, t * fine : (t + 1) * fine].reshape(rows, fine)
            coarse[t] = dot_t(block, interp[t])
            for l in range(level_len):
                place = pl.ds(turned_level(l), members, stride=level_len)
                levels[wide + l, t] = coarse[t, place, :]
        some = pl.ds(h * split, split)
        for i in range(wide // 2):
            low = [level_len - 1 - 2 * i - n if two else 2 * i + n for n in range(2)]
            low = [levels[wide + l, some] for l in low]
            halo_out[0, i, some] = jnp.concatenate(low, axis=1).astype(BF16)
            if not two:
                high = [levels[level_len + 2 * i + n, some] for n in range(2)]
                halo_out[1, i, some] = jnp.concatenate(high, axis=1).astype(BF16)
        if h == 0:
            pl.when(jnp.logical_not(eager))(enter)

        @pl.when(me_l > 0)
        def _(some=some):
            exchange(0, 1, below, some).start()

    start = me_l * level_len

    sign = jnp.where(me_l == 0, 1, -1) if two else 1

    def coefficient(level, shift):
        return weight[half + sign * shift, jnp.clip(start + turned_level(level), 0, total_levels - 1)]

    def adjoint_level(level):
        value = coefficient(level - half, half) * levels[wide + level - half]
        for e in range(1 - half, half + 1):
            value = value + coefficient(level + e, -e) * levels[wide + level + e]
        if level < 0:
            value = jnp.where(start + level >= 0, value, 0.0)
        if level >= level_len:
            value = jnp.where(start + level < total_levels, value, 0.0) if not two else value
        middle[half + level] = value

    def forward_pair(level):
        both = []
        for l in (level, level + 1):
            value = coefficient(l, -half) * middle[l]
            for j in range(1, wide + 1):
                value = value + coefficient(l, j - half) * middle[l + j]
            both.append(value)
        pair = jnp.concatenate(both, axis=1).astype(BF16)
        place = (level if two else order.index(level)) * members
        smooth[:, pl.ds(place, 2 * members), :] = pair

    def clear(base):
        for i in range(wide):
            levels[base + i] = jnp.zeros(levels.shape[1:], F32)

    if two:
        clear(0)
        for i in range(half):
            middle[i] = jnp.zeros(middle.shape[1:], F32)
        early = [range(level_len - half), range(0, level_len - wide, 2)]
        late = [range(level_len - half, level_len + half), range(level_len - wide, level_len, 2)]
    else:
        early = [range(half, level_len - half), range(wide, level_len - wide, 2)]
        late = [list(range(-half, half)) + list(range(level_len - half, level_len + half))]
        late.append(list(range(0, wide, 2)) + list(range(level_len - wide, level_len, 2)))
    for level in early[0]:
        adjoint_level(level)
    for level in early[1]:
        forward_pair(level)

    load_c.wait()

    def gathered(left, first):
        right = jnp.concatenate(
            [
                jnp.concatenate([conv[t, which[t, first + s]] for t in range(tiles)], axis=1)
                for s in range(most)
            ],
            axis=0,
        )
        return dot_t(left, right)

    def gathered_turned(left, first):
        right = jnp.concatenate(
            [
                jnp.concatenate([turned[t, which[t, first + s]] for t in range(tiles)], axis=0)
                for s in range(most)
            ],
            axis=1,
        )
        return jnp.dot(left, right, preferred_element_type=F32)

    def side_by_side(ref, count, low, size):
        return jnp.concatenate([ref[i, pl.ds(low, size)] for i in range(count)], axis=1)

    def sum_back(c, o):
        low, count = parts[c]
        left = side_by_side(smooth, tiles, low, count)
        sums = (gathered_turned if c else gathered)(left, tiles + o * most).astype(BF16)
        for s in range(most):
            returning[o, s, pl.ds(low, count)] = sums[:, s * tile_len : (s + 1) * tile_len]

    def copy_back(o, i):
        low, count = numbered[i]
        return pltpu.make_async_remote_copy(
            returning.at[o, :, pl.ds(low, count)],
            arrived_back[i].at[o, pl.ds(0, most)],
            send_sem.at[0],
            back_sem.at[i],
            device_id={"patch": source[o]},
            device_id_type=MESH,
        )

    def copy_forth(o, i):
        low, count = numbered[i]
        return pltpu.make_async_remote_copy(
            sending.at[o, :, pl.ds(low, count)],
            arrived.at[o, :, pl.ds(low, count)],
            send_sem.at[1],
            forth_sem.at[0 if offsets[o] < 0 else 1],
            device_id={"patch": partner[o]},
            device_id_type=MESH,
        )

    def all_back(i):
        low, count = numbered[i]
        return pltpu.make_async_remote_copy(
            returning.at[:, :, pl.ds(low, count)],
            arrived_back[i].at[:, pl.ds(0, most)],
            send_sem.at[0],
            back_sem.at[i],
            device_id={"patch": source[0]},
            device_id_type=MESH,
        )

    def all_forth(first, count, sem):
        return pltpu.make_async_remote_copy(
            sending.at[pl.ds(first, count)],
            arrived.at[pl.ds(first, count)],
            send_sem.at[1],
            forth_sem.at[sem],
            device_id={"patch": partner[0]},
            device_id_type=MESH,
        )

    def indices(c):
        first = len(chunks[0]) if c else 0
        return range(first, first + len(chunks[c]))

    def sum_own():
        left = side_by_side(smooth, tiles, 0, rows)
        for first in range(0, tiles, most):
            sums = gathered_turned(left, first)
            for s in range(most):
                own[first + s] = sums[:, s * tile_len : (s + 1) * tile_len]

    def await_entry(group, wrapped):
        later = jnp.int32(0)
        for o in group:
            around = source[o] > me_p if offsets[o] > 0 else source[o] < me_p
            wanted = jnp.logical_and(answers[o], around == wrapped)
            later = later + jnp.where(wanted, 1, 0)

        @pl.when(later > 0)
        def _():
            pl.semaphore_wait(enter_sem.at[1 if wrapped else 0], later)

    def send_back(c):
        for o in upper:
            sum_back(c, o)
        if c == 0:
            await_entry(upper + lower, False)
        for i in indices(c):
            for o in upper:
                copy_back(o, i).start()
        if c == 0:

            @pl.when(me_l < n_lev - 1)
            def _():
                pl.semaphore_wait(enter_lev, 1)
                up.start()

        for o in lower:
            sum_back(c, o)
        for i in indices(c):
            for o in lower:
                if c == 0:

                    @pl.when(source[o] < me_p)
                    def _(o=o, i=i):
                        copy_back(o, i).start()

                else:
                    copy_back(o, i).start()

    send_back(0)
    for t in range(tiles):
        for k in range(k_len + 1):
            turned[t, k] = conv[t, k].T

    def unpack(side, base):
        for i in range(wide // 2):
            pair = halo_in[side, i].astype(F32)
            levels[base + 2 * i] = pair[:, :members]
            levels[base + 2 * i + 1] = pair[:, members:]

    await_entry(upper + lower, True)
    for i in indices(0):
        for o in lower:

            @pl.when(source[o] > me_p)
            def _(o=o, i=i):
                copy_back(o, i).start()

    if two:
        down.wait_recv()
        unpack(1, wide + level_len)
    else:

        @pl.when(me_l > 0)
        def _():
            up.wait_recv()
            unpack(0, 0)

        @pl.when(me_l == 0)
        def _():
            clear(0)

        @pl.when(me_l < n_lev - 1)
        def _():
            down.wait_recv()
            unpack(1, wide + level_len)

        @pl.when(me_l == n_lev - 1)
        def _():
            clear(wide + level_len)

    for level in late[0]:
        adjoint_level(level)
    for level in late[1]:
        forward_pair(level)

    send_back(1)
    sum_own()

    last = len(numbered) - 1
    around = me_p >= n_patch - max(offsets)

    def near_forth(i):
        for o in upper:
            copy_forth(o, i).start()
        for o in lower:

            @pl.when(partner[o] > me_p)
            def _(o=o):
                copy_forth(o, i).start()

    for i, (low, count) in enumerate(numbered):
        all_back(i).wait_recv()
        for t in range(tiles):
            value = own[t, pl.ds(low, count)]
            for o in range(link_len):
                value = value + arrived_back[i][o, slot_of[t, o]].astype(F32)
            ext[t, pl.ds(low, count)] = value.astype(BF16)
        for o in lower + upper:
            for s in range(most):
                sending[o, s, pl.ds(low, count)] = ext[send[0, s, o], pl.ds(low, count)]
        for o in lower:

            @pl.when(partner[o] < me_p)
            def _(o=o, i=i):
                copy_forth(o, i).start()

        if i == last:
            pl.when(around)(lambda: near_forth(last - 1))
        if i == last - 1:
            pl.when(jnp.logical_not(around))(lambda: near_forth(last - 1))
        else:
            near_forth(i)

    def spread(left, named, t):
        right = jnp.concatenate(
            [
                jnp.concatenate([conv[u, which[u, e]] for e in named], axis=0)
                for u in (t, t + 1)
            ],
            axis=1,
        )
        return jnp.dot(left, right, preferred_element_type=F32)

    def add(left, named, fresh):
        for t in range(0, tiles, 2):
            sums = spread(left, named, t)
            for i in range(2):
                value = sums[:, i * tile_len : (i + 1) * tile_len]
                mixed[t + i] = value if fresh else value + mixed[t + i]

    def by_member(value, n):
        for g in range(level_len):
            place = pl.ds(pl.multiple_of(level_of(g) * members, members), members)
            coarse[n, place] = value[g * members : (g + 1) * members]
        lines = [coarse[n, pl.ds(m, level_len, stride=members), :] for m in range(members)]
        return jnp.concatenate(lines, axis=0).astype(BF16)

    def received(group):
        return jnp.concatenate(
            [side_by_side(arrived.at[o], most, 0, rows) for o in group], axis=1
        )

    def entries_of(group):
        return [tiles + o * most + s for o in group for s in range(most)]

    add(side_by_side(ext, tiles, 0, rows), range(tiles), True)
    for t in range(tiles):
        stack = jnp.concatenate([conv[t, which[t, e]] for e in entries_of(lower)], axis=0)
        turn_out[t] = jnp.dot(stack, interp[t], preferred_element_type=F32).astype(BF16)
    all_forth(0, link_len // 2, 0).wait_recv()
    add(received(upper), entries_of(upper), False)
    for t in range(tiles):
        part = by_member(mixed[t], t)
        base_out[t] = jnp.dot(part, interp[t], preferred_element_type=F32)
    all_forth(link_len // 2, link_len // 2, 1).wait_recv()
    for n, (o, s) in enumerate((o, s) for o in lower for s in range(most)):
        value = by_member(arrived[o, s].astype(F32), n)
        left_out[:, n * tile_len : (n + 1) * tile_len] = value
    for i in range(len(numbered)):
        all_back(i).wait_send()
    all_forth(0, link_len, 0).wait_send()

    @pl.when(me_l > 0)
    def _():
        down.wait_send()

    @pl.when(me_l < n_lev - 1)
    def _():
        up.wait_send()


def finish(left, turn, base, out_hbm, out, sem):
    tiles, _, fine = turn.shape
    copies = []
    for t in range(tiles):
        sums = base[t] + jnp.dot(left[...], turn[t], preferred_element_type=F32)
        columns = pl.ds(t * fine, fine)
        out[:, :, columns] = sums.reshape(out.shape[0], out.shape[1], fine)
        copy = pltpu.make_async_copy(out.at[:, :, columns], out_hbm.at[:, :, columns], sem.at[t])
        copy.start()
        copies.append(copy)
    for copy in copies:
        copy.wait()


def solution(mesh):
    n_patch, n_lev = mesh.shape["patch"], mesh.shape["lev"]

    def shards(fields, interp, conv_weight, vert_weight, send_tiles, tile_pattern):
        members, level_len, column_len = fields.shape
        tiles, tile_len, fine = interp.shape
        k_len = conv_weight.shape[1]
        link_len, most = send_tiles.shape[1:]
        wide = vert_weight.shape[1] - 1
        rows = members * level_len
        any_spec = pl.BlockSpec(memory_space=pl.ANY)
        entries = tiles + link_len * most
        words = -(-entries // (31 // k_len.bit_length()))
        weight, send = vert_weight.T, send_tiles.transpose(0, 2, 1)
        parts = split_rows(n_lev, level_len, members, wide)
        sizes = [count for part in chunks_of(parts) for _, count in part]

        def per_link(count, size=rows):
            return pltpu.VMEM((link_len, count, size, tile_len), BF16)

        vmem_spec = pl.BlockSpec(memory_space=pltpu.VMEM)
        half_len = link_len // 2 * most * tile_len
        left, turn, base = pl.pallas_call(
            functools.partial(kernel, n_patch, n_lev),
            name="localize",
            out_shape=[
                pltpu.VMEM((rows, half_len), BF16),
                pltpu.VMEM((tiles, half_len, fine), BF16),
                pltpu.VMEM((tiles, rows, fine), F32),
            ],
            in_specs=[any_spec] * 6,
            out_specs=[vmem_spec] * 3,
            scratch_shapes=[
                pltpu.SMEM(weight.shape, F32),
                pltpu.SMEM(send.shape, jnp.int32),
                pltpu.SMEM(tile_pattern.shape, jnp.int32),
                pltpu.VMEM(fields.shape, BF16),
                pltpu.VMEM(interp.shape, BF16),
                pltpu.VMEM((tiles, k_len + 1, tile_len, tile_len), BF16),
                pltpu.VMEM((tiles, k_len + 1, tile_len, tile_len), BF16),
                pltpu.VMEM((tiles, rows, tile_len), F32),
                pltpu.VMEM((level_len + 2 * wide, tiles, members, tile_len), F32),
                pltpu.VMEM((level_len + wide, tiles, members, tile_len), F32),
                pltpu.VMEM((2, wide // 2, tiles, 2 * members, tile_len), BF16),
                pltpu.VMEM((2, wide // 2, tiles, 2 * members, tile_len), BF16),
                pltpu.VMEM((tiles, rows, tile_len), F32),
                pltpu.VMEM((tiles, rows, tile_len), F32),
                pltpu.VMEM((tiles, rows, tile_len), BF16),
                pltpu.VMEM((tiles + 1, rows, tile_len), BF16),
                pltpu.SMEM((words, entries), jnp.int32),
                pltpu.SMEM((tiles, entries), jnp.int32),
                pltpu.SMEM((tiles, link_len), jnp.int32),
                pltpu.SemaphoreType.DMA((6,)),
                pltpu.SemaphoreType.DMA((4,)),
                pltpu.SemaphoreType.DMA((2,)),
                pltpu.SemaphoreType.DMA((len(sizes),)),
                pltpu.SemaphoreType.DMA((2,)),
                pltpu.SemaphoreType.REGULAR((2,)),
                pltpu.SemaphoreType.REGULAR,
            ]
            + [per_link(most)] * 3
            + [per_link(most + 1, size) for size in sizes],
            compiler_params=pltpu.CompilerParams(collective_id=0, has_side_effects=True),
        )(fields, interp, conv_weight, weight, send, tile_pattern)
        return pl.pallas_call(
            finish,
            name="finish",
            out_shape=jax.ShapeDtypeStruct(fields.shape, F32),
            in_specs=[vmem_spec] * 3,
            out_specs=any_spec,
            scratch_shapes=[
                pltpu.VMEM(fields.shape, F32),
                pltpu.SemaphoreType.DMA((tiles,)),
            ],
            compiler_params=pltpu.CompilerParams(vmem_limit_bytes=8 << 20),
        )(left, turn, base)

    in_specs = (
        P(None, "lev", "patch"),
        P("patch", None, None),
        P("patch", None, None, None),
        P(),
        P("patch", None, None),
        P("patch", None),
    )
    out_specs = P(None, "lev", "patch")
    return jax.shard_map(shards, mesh=mesh, in_specs=in_specs, out_specs=out_specs, check_vma=False)
```

```python
import functools

import jax
import jax.numpy as jnp
from jax import lax
from jax.experimental import pallas as pl
from jax.experimental.pallas import tpu as pltpu
from jax.sharding import PartitionSpec as P

MESH = pl.DeviceIdType.MESH
F32 = jnp.float32
BF16 = jnp.bfloat16
VMEM_BYTES = 67043328


def link_offsets(reach_len):
    return [
        position - reach_len if position < reach_len else position - reach_len + 1
        for position in range(2 * reach_len)
    ]


def chunks_of(parts):
    chunks = []
    for low, count in parts:
        step = 32 if count % 32 == 0 else count
        chunks.append([(low + at, step) for at in range(0, count, step)])
    return chunks


def split_rows(n_lev, level_len, members, wide):
    early = level_len - wide if n_lev == 2 else level_len - 2 * wide
    return [(0, early * members), (early * members, (level_len - early) * members)]


def dot_t(left, right):
    return lax.dot_general(left, right, (((1,), (1,)), ((), ())), preferred_element_type=F32)


def kernel(
    n_patch,
    n_lev,
    fields_hbm,
    interp_hbm,
    conv_hbm,
    weight_hbm,
    send_hbm,
    pattern_hbm,
    left_out,
    turn_out,
    base_out,
    weight,
    send,
    pattern,
    fields,
    interp,
    conv,
    turned,
    coarse,
    levels,
    middle,
    halo_out,
    halo_in,
    own,
    smooth,
    ext,
    send_rows,
    which_made,
    slot_made,
    which,
    slot_of,
    load_sem,
    halo_sem,
    send_sem,
    back_sem,
    forth_sem,
    enter_sem,
    enter_lev,
    returning,
    sending,
    arrived,
    *arrived_back,
):
    members, level_len, _ = fields.shape
    tiles, tile_len, fine = interp.shape
    k_len = conv_hbm.shape[1]
    most, link_len = send.shape[1], send.shape[2]
    half = (weight.shape[0] - 1) // 2
    wide = 2 * half
    rows = members * level_len
    total_levels = weight.shape[1]
    offsets = link_offsets(link_len // 2)
    two = n_lev == 2
    parts = split_rows(n_lev, level_len, members, wide)
    chunks = chunks_of(parts)
    numbered = [(low, count) for part in chunks for low, count in part]
    me_p, me_l = lax.axis_index("patch"), lax.axis_index("lev")
    partner = [lax.rem(me_p + d + n_patch, n_patch) for d in offsets]
    source = [lax.rem(me_p - d + n_patch, n_patch) for d in offsets]

    order = list(range(wide, level_len - wide))
    order += list(range(wide)) + list(range(level_len - wide, level_len))

    def turned_level(index):
        return jnp.where(me_l == 0, index, level_len - 1 - index) if two else index

    def level_of(group):
        return turned_level(group) if two else order[group]

    def rank(index):
        return jnp.where(index < n_patch - 4, index, 2 * n_patch - 5 - index)

    me_rank = rank(me_p)
    ahead = [rank(other) < me_rank for other in partner]
    behind = [rank(other) > me_rank for other in partner]
    answers = [rank(other) > me_rank for other in source]
    upper = sorted((o for o in range(link_len) if offsets[o] < 0), key=lambda o: offsets[o])
    lower = sorted((o for o in range(link_len) if offsets[o] > 0), key=lambda o: -offsets[o])

    load_w = pltpu.make_async_copy(weight_hbm, weight, load_sem.at[3])
    load_s = pltpu.make_async_copy(send_hbm, send, load_sem.at[4])
    load_v = pltpu.make_async_copy(send_hbm, send_rows, load_sem.at[6])
    load_p = pltpu.make_async_copy(pattern_hbm, pattern, load_sem.at[5])
    load_f = pltpu.make_async_copy(fields_hbm, fields, load_sem.at[0])
    load_i = pltpu.make_async_copy(interp_hbm, interp, load_sem.at[1])
    load_c = pltpu.make_async_copy(conv_hbm, conv.at[:, pl.ds(0, k_len)], load_sem.at[2])
    load_p.start()
    load_v.start()
    load_s.start()
    load_w.start()
    load_f.start()
    load_i.start()
    load_c.start()

    barrier = pltpu.get_barrier_semaphore()
    for o in range(link_len):

        @pl.when(behind[o])
        def _(o=o):
            pl.semaphore_signal(
                barrier, inc=1, device_id={"patch": partner[o]}, device_id_type=MESH
            )

    @pl.when(me_l < n_lev - 1)
    def _():
        pl.semaphore_signal(barrier, inc=1, device_id={"lev": me_l + 1}, device_id_type=MESH)

    entries = tiles + link_len * most
    for t in range(tiles):
        conv[t, k_len] = jnp.zeros((tile_len, tile_len), BF16)
    for i, (_, count) in enumerate(numbered):
        for o in range(link_len):
            arrived_back[i][o, most] = jnp.zeros((count, tile_len), BF16)
    ext[tiles] = jnp.zeros((rows, tile_len), BF16)
    enter_first = jnp.logical_or(me_p < 4, me_p >= n_patch - 2)
    enter_last = jnp.logical_and(jnp.logical_not(enter_first), me_p >= n_patch - 4)
    enter_second = jnp.logical_not(jnp.logical_or(enter_first, enter_last))

    def enter():
        before = jnp.where(me_l > 0, 1, 0)
        for o in range(link_len):
            before = before + jnp.where(ahead[o], 1, 0)

        @pl.when(before > 0)
        def _():
            pl.semaphore_wait(barrier, before)

        for o in range(link_len):

            @pl.when(ahead[o])
            def _(o=o):
                wrapped = partner[o] < me_p if offsets[o] > 0 else partner[o] > me_p
                pl.semaphore_signal(
                    enter_sem.at[jnp.where(wrapped, 1, 0)],
                    inc=1,
                    device_id={"patch": partner[o]},
                    device_id_type=MESH,
                )

        @pl.when(me_l > 0)
        def _():
            pl.semaphore_signal(enter_lev, inc=1, device_id={"lev": me_l - 1}, device_id_type=MESH)

    pl.when(enter_first)(enter)
    load_p.wait()
    load_v.wait()
    lane = lax.broadcasted_iota(jnp.int32, (tiles, entries), 1)
    index = jnp.full((tiles, entries), k_len, jnp.int32)
    for k in range(k_len):
        index = jnp.where(pattern[:, k : k + 1] == lane, k, index)
    which_made[...] = index
    row = lax.broadcasted_iota(jnp.int32, (tiles, link_len), 0)
    index = jnp.full((tiles, link_len), most, jnp.int32)
    for s in range(most):
        index = jnp.where(send_rows[0, s : s + 1, :] == row, s, index)
    slot_made[...] = index
    pl.when(enter_second)(enter)
    load_f.wait()
    load_i.wait()
    make_which = pltpu.make_async_copy(which_made, which, load_sem.at[7])
    make_slot = pltpu.make_async_copy(slot_made, slot_of, load_sem.at[8])
    make_which.start()
    make_slot.start()
    split = tiles // 2
    below = {"lev": lax.rem(me_l + n_lev - 1, n_lev)}
    above = {"lev": lax.rem(me_l + 1, n_lev)}

    def exchange(side, place, to, some=slice(None)):
        return pltpu.make_async_remote_copy(
            halo_out.at[side, :, some],
            halo_in.at[place, :, some],
            halo_sem.at[2 * side],
            halo_sem.at[2 * side + 1],
            device_id=to,
            device_id_type=MESH,
        )

    down = exchange(0, 1, below)
    up = down if two else exchange(1, 0, above)
    for h in range(2):
        for t in range(h * split, (h + 1) * split):
            block = fields[:, :, t * fine : (t + 1) * fine].reshape(rows, fine)
            coarse[t] = dot_t(block, interp[t])
            for l in range(level_len):
                place = pl.ds(turned_level(l), members, stride=level_len)
                levels[wide + l, t] = coarse[t, place, :]
        some = pl.ds(h * split, split)
        for i in range(wide // 2):
            low = [level_len - 1 - 2 * i - n if two else 2 * i + n for n in range(2)]
            low = [levels[wide + l, some] for l in low]
            halo_out[0, i, some] = jnp.concatenate(low, axis=1).astype(BF16)
            if not two:
                high = [levels[level_len + 2 * i + n, some] for n in range(2)]
                halo_out[1, i, some] = jnp.concatenate(high, axis=1).astype(BF16)
        if h == 0:
            pl.when(enter_last)(enter)

        @pl.when(me_l > 0)
        def _(some=some):
            exchange(0, 1, below, some).start()

    start = me_l * level_len

    sign = jnp.where(me_l == 0, 1, -1) if two else 1
    load_w.wait()

    def coefficient(level, shift):
        return weight[half + sign * shift, jnp.clip(start + turned_level(level), 0, total_levels - 1)]

    def adjoint_level(level):
        value = coefficient(level - half, half) * levels[wide + level - half]
        for e in range(1 - half, half + 1):
            value = value + coefficient(level + e, -e) * levels[wide + level + e]
        if level < 0:
            value = jnp.where(start + level >= 0, value, 0.0)
        if level >= level_len:
            value = jnp.where(start + level < total_levels, value, 0.0) if not two else value
        middle[half + level] = value

    def forward_pair(level):
        both = []
        for l in (level, level + 1):
            value = coefficient(l, -half) * middle[l]
            for j in range(1, wide + 1):
                value = value + coefficient(l, j - half) * middle[l + j]
            both.append(value)
        pair = jnp.concatenate(both, axis=1).astype(BF16)
        place = (level if two else order.index(level)) * members
        smooth[:, pl.ds(place, 2 * members), :] = pair

    def clear(base):
        for i in range(wide):
            levels[base + i] = jnp.zeros(levels.shape[1:], F32)

    if two:
        clear(0)
        for i in range(half):
            middle[i] = jnp.zeros(middle.shape[1:], F32)
        early = [range(level_len - half), range(0, level_len - wide, 2)]
        late = [range(level_len - half, level_len + half), range(level_len - wide, level_len, 2)]
    else:
        early = [range(half, level_len - half), range(wide, level_len - wide, 2)]
        late = [list(range(-half, half)) + list(range(level_len - half, level_len + half))]
        late.append(list(range(0, wide, 2)) + list(range(level_len - wide, level_len, 2)))
    for level in early[0]:
        adjoint_level(level)
    for level in early[1]:
        forward_pair(level)

    load_c.wait()
    load_s.wait()
    make_which.wait()
    make_slot.wait()

    def gathered(left, first):
        right = jnp.concatenate(
            [
                jnp.concatenate([conv[t, which[t, first + s]] for t in range(tiles)], axis=1)
                for s in range(most)
            ],
            axis=0,
        )
        return dot_t(left, right)

    def gathered_turned(left, first):
        right = jnp.concatenate(
            [
                jnp.concatenate([turned[t, which[t, first + s]] for t in range(tiles)], axis=0)
                for s in range(most)
            ],
            axis=1,
        )
        return jnp.dot(left, right, preferred_element_type=F32)

    def side_by_side(ref, count, low, size):
        return jnp.concatenate([ref[i, pl.ds(low, size)] for i in range(count)], axis=1)

    def sum_back(c, o):
        low, count = parts[c]
        left = side_by_side(smooth, tiles, low, count)
        sums = (gathered_turned if c else gathered)(left, tiles + o * most).astype(BF16)
        for s in range(most):
            returning[o, s, pl.ds(low, count)] = sums[:, s * tile_len : (s + 1) * tile_len]

    def copy_back(o, i):
        low, count = numbered[i]
        return pltpu.make_async_remote_copy(
            returning.at[o, :, pl.ds(low, count)],
            arrived_back[i].at[o, pl.ds(0, most)],
            send_sem.at[0],
            back_sem.at[i],
            device_id={"patch": source[o]},
            device_id_type=MESH,
        )

    def copy_forth(o, i):
        low, count = numbered[i]
        return pltpu.make_async_remote_copy(
            sending.at[o, :, pl.ds(low, count)],
            arrived.at[o, :, pl.ds(low, count)],
            send_sem.at[1],
            forth_sem.at[0 if offsets[o] < 0 else 1],
            device_id={"patch": partner[o]},
            device_id_type=MESH,
        )

    def all_back(i):
        low, count = numbered[i]
        return pltpu.make_async_remote_copy(
            returning.at[:, :, pl.ds(low, count)],
            arrived_back[i].at[:, pl.ds(0, most)],
            send_sem.at[0],
            back_sem.at[i],
            device_id={"patch": source[0]},
            device_id_type=MESH,
        )

    def all_forth(first, count, sem):
        return pltpu.make_async_remote_copy(
            sending.at[pl.ds(first, count)],
            arrived.at[pl.ds(first, count)],
            send_sem.at[1],
            forth_sem.at[sem],
            device_id={"patch": partner[0]},
            device_id_type=MESH,
        )

    def indices(c):
        first = len(chunks[0]) if c else 0
        return range(first, first + len(chunks[c]))

    def sum_own():
        left = side_by_side(smooth, tiles, 0, rows)
        for first in range(0, tiles, most):
            sums = gathered_turned(left, first)
            for s in range(most):
                own[first + s] = sums[:, s * tile_len : (s + 1) * tile_len]

    def await_entry(group, wrapped):
        later = jnp.int32(0)
        for o in group:
            around = source[o] > me_p if offsets[o] > 0 else source[o] < me_p
            wanted = jnp.logical_and(answers[o], around == wrapped)
            later = later + jnp.where(wanted, 1, 0)

        @pl.when(later > 0)
        def _():
            pl.semaphore_wait(enter_sem.at[1 if wrapped else 0], later)

    def send_back(c):
        for o in upper:
            sum_back(c, o)
        if c == 0:
            await_entry(upper + lower, False)
        for i in indices(c):
            for o in upper:
                copy_back(o, i).start()
        if c == 0:

            @pl.when(me_l < n_lev - 1)
            def _():
                pl.semaphore_wait(enter_lev, 1)
                up.start()

        for o in lower:
            sum_back(c, o)
        for i in indices(c):
            for o in lower:
                if c == 0:

                    @pl.when(source[o] < me_p)
                    def _(o=o, i=i):
                        copy_back(o, i).start()

                else:
                    copy_back(o, i).start()

    send_back(0)
    for t in range(tiles):
        for k in range(k_len + 1):
            turned[t, k] = conv[t, k].T

    def unpack(side, base):
        for i in range(wide // 2):
            pair = halo_in[side, i].astype(F32)
            levels[base + 2 * i] = pair[:, :members]
            levels[base + 2 * i + 1] = pair[:, members:]

    await_entry(upper + lower, True)
    for i in indices(0):
        for o in lower:

            @pl.when(source[o] > me_p)
            def _(o=o, i=i):
                copy_back(o, i).start()

    if two:
        down.wait_recv()
        unpack(1, wide + level_len)
    else:

        @pl.when(me_l > 0)
        def _():
            up.wait_recv()
            unpack(0, 0)

        @pl.when(me_l == 0)
        def _():
            clear(0)

        @pl.when(me_l < n_lev - 1)
        def _():
            down.wait_recv()
            unpack(1, wide + level_len)

        @pl.when(me_l == n_lev - 1)
        def _():
            clear(wide + level_len)

    for level in late[0]:
        adjoint_level(level)
    for level in late[1]:
        forward_pair(level)

    send_back(1)
    sum_own()

    last = len(numbered) - 1
    around = me_p >= n_patch - max(offsets)

    def near_forth(i):
        for o in upper:
            copy_forth(o, i).start()
        for o in lower:

            @pl.when(partner[o] > me_p)
            def _(o=o):
                copy_forth(o, i).start()

    def places_of(group):
        return 0 if group is lower else len(lower) * most * tile_len

    def through_interp(group):
        named = [tiles + o * most + s for o in group for s in range(most)]
        rows_of = pl.ds(places_of(group), len(named) * tile_len)
        for t in range(tiles):
            stack = jnp.concatenate([conv[t, which[t, e]] for e in named], axis=0)
            product = jnp.dot(stack, interp[t], preferred_element_type=F32)
            turn_out[t, rows_of] = product.astype(BF16)

    for i, (low, count) in enumerate(numbered):
        if i == last:
            through_interp(lower)
        all_back(i).wait_recv()
        for t in range(tiles):
            value = own[t, pl.ds(low, count)]
            for o in range(link_len):
                value = value + arrived_back[i][o, slot_of[t, o]].astype(F32)
            ext[t, pl.ds(low, count)] = value.astype(BF16)
        for o in lower + upper:
            for s in range(most):
                sending[o, s, pl.ds(low, count)] = ext[send[0, s, o], pl.ds(low, count)]
        for o in lower:

            @pl.when(partner[o] < me_p)
            def _(o=o, i=i):
                copy_forth(o, i).start()

        if i == last:
            pl.when(around)(lambda: near_forth(last - 1))
        if i == last - 1:
            pl.when(jnp.logical_not(around))(lambda: near_forth(last - 1))
        else:
            near_forth(i)

    def spread(left, named, t):
        right = jnp.concatenate(
            [
                jnp.concatenate([conv[u, which[u, e]] for e in named], axis=0)
                for u in (t, t + 1)
            ],
            axis=1,
        )
        return jnp.dot(left, right, preferred_element_type=F32)

    def by_member(value, n):
        for g in range(level_len):
            place = pl.ds(pl.multiple_of(level_of(g) * members, members), members)
            coarse[n, place] = value[g * members : (g + 1) * members]
        lines = [coarse[n, pl.ds(m, level_len, stride=members), :] for m in range(members)]
        return jnp.concatenate(lines, axis=0).astype(BF16)

    def by_member(value, n):
        for g in range(level_len):
            place = pl.ds(pl.multiple_of(level_of(g) * members, members), members)
            coarse[n, place] = value[g * members : (g + 1) * members]
        lines = [coarse[n, pl.ds(m, level_len, stride=members), :] for m in range(members)]
        return jnp.concatenate(lines, axis=0).astype(BF16)

    def received(group):
        return jnp.concatenate(
            [side_by_side(arrived.at[o], most, 0, rows) for o in group], axis=1
        )

    def entries_of(group):
        return [tiles + o * most + s for o in group for s in range(most)]

    left = side_by_side(ext, tiles, 0, rows)
    for t in range(0, tiles, 2):
        sums = spread(left, range(tiles), t)
        for i in range(2):
            part = by_member(sums[:, i * tile_len : (i + 1) * tile_len], t + i)
            base_out[t + i] = jnp.dot(part, interp[t + i], preferred_element_type=F32)
    through_interp(upper)
    for group in (lower, upper):
        for n, (o, s) in enumerate((o, s) for o in group for s in range(most)):
            if n == 0:
                first = 0 if group is upper else link_len // 2
                all_forth(first, link_len // 2, 0 if group is upper else 1).wait_recv()
            place = places_of(group) + n * tile_len
            left_out[:, place : place + tile_len] = by_member(arrived[o, s].astype(F32), n)
    for i in range(len(numbered)):
        all_back(i).wait_send()
    all_forth(0, link_len, 0).wait_send()

    @pl.when(me_l > 0)
    def _():
        down.wait_send()

    @pl.when(me_l < n_lev - 1)
    def _():
        up.wait_send()


def finish(left, turn, base, out_hbm, out, sem):
    tiles, _, fine = turn.shape
    copies = []
    for t in range(tiles):
        sums = base[t] + jnp.dot(left[...], turn[t], preferred_element_type=F32)
        columns = pl.ds(t * fine, fine)
        out[:, :, columns] = sums.reshape(out.shape[0], out.shape[1], fine)
        copy = pltpu.make_async_copy(out.at[:, :, columns], out_hbm.at[:, :, columns], sem.at[t])
        copy.start()
        copies.append(copy)
    for copy in copies:
        copy.wait()


def solution(mesh):
    n_patch, n_lev = mesh.shape["patch"], mesh.shape["lev"]

    def shards(fields, interp, conv_weight, vert_weight, send_tiles, tile_pattern):
        members, level_len, column_len = fields.shape
        tiles, tile_len, fine = interp.shape
        k_len = conv_weight.shape[1]
        link_len, most = send_tiles.shape[1:]
        wide = vert_weight.shape[1] - 1
        rows = members * level_len
        any_spec = pl.BlockSpec(memory_space=pl.ANY)
        entries = tiles + link_len * most
        weight, send = vert_weight.T, send_tiles.transpose(0, 2, 1)
        parts = split_rows(n_lev, level_len, members, wide)
        sizes = [count for part in chunks_of(parts) for _, count in part]

        def per_link(count, size=rows):
            return pltpu.VMEM((link_len, count, size, tile_len), BF16)

        vmem_spec = pl.BlockSpec(memory_space=pltpu.VMEM)
        wide_len = link_len * most * tile_len
        spare = VMEM_BYTES - 2 * (rows + tiles * fine) * wide_len - 4 * tiles * rows * fine
        spare -= 1 << 18
        left, turn, base = pl.pallas_call(
            functools.partial(kernel, n_patch, n_lev),
            name="localize",
            out_shape=[
                pltpu.VMEM((rows, wide_len), BF16),
                pltpu.VMEM((tiles, wide_len, fine), BF16),
                pltpu.VMEM((tiles, rows, fine), F32),
            ],
            in_specs=[any_spec] * 6,
            out_specs=[vmem_spec] * 3,
            scratch_shapes=[
                pltpu.SMEM(weight.shape, F32),
                pltpu.SMEM(send.shape, jnp.int32),
                pltpu.VMEM(tile_pattern.shape, jnp.int32),
                pltpu.VMEM(fields.shape, BF16),
                pltpu.VMEM(interp.shape, BF16),
                pltpu.VMEM((tiles, k_len + 1, tile_len, tile_len), BF16),
                pltpu.VMEM((tiles, k_len + 1, tile_len, tile_len), BF16),
                pltpu.VMEM((tiles, rows, tile_len), F32),
                pltpu.VMEM((level_len + 2 * wide, tiles, members, tile_len), F32),
                pltpu.VMEM((level_len + wide, tiles, members, tile_len), F32),
                pltpu.VMEM((2, wide // 2, tiles, 2 * members, tile_len), BF16),
                pltpu.VMEM((2, wide // 2, tiles, 2 * members, tile_len), BF16),
                pltpu.VMEM((tiles, rows, tile_len), F32),
                pltpu.VMEM((tiles, rows, tile_len), BF16),
                pltpu.VMEM((tiles + 1, rows, tile_len), BF16),
                pltpu.VMEM(send.shape, jnp.int32),
                pltpu.VMEM((tiles, entries), jnp.int32),
                pltpu.VMEM((tiles, link_len), jnp.int32),
                pltpu.SMEM((tiles, entries), jnp.int32),
                pltpu.SMEM((tiles, link_len), jnp.int32),
                pltpu.SemaphoreType.DMA((9,)),
                pltpu.SemaphoreType.DMA((4,)),
                pltpu.SemaphoreType.DMA((2,)),
                pltpu.SemaphoreType.DMA((len(sizes),)),
                pltpu.SemaphoreType.DMA((2,)),
                pltpu.SemaphoreType.REGULAR((2,)),
                pltpu.SemaphoreType.REGULAR,
            ]
            + [per_link(most)] * 3
            + [per_link(most + 1, size) for size in sizes],
            compiler_params=pltpu.CompilerParams(
                collective_id=0, has_side_effects=True, vmem_limit_bytes=spare
            ),
        )(fields, interp, conv_weight, weight, send, tile_pattern)
        return pl.pallas_call(
            finish,
            name="finish",
            out_shape=jax.ShapeDtypeStruct(fields.shape, F32),
            in_specs=[vmem_spec] * 3,
            out_specs=any_spec,
            scratch_shapes=[
                pltpu.VMEM(fields.shape, F32),
                pltpu.SemaphoreType.DMA((tiles,)),
            ],
            compiler_params=pltpu.CompilerParams(vmem_limit_bytes=8 << 20),
        )(left, turn, base)

    in_specs = (
        P(None, "lev", "patch"),
        P("patch", None, None),
        P("patch", None, None, None),
        P(),
        P("patch", None, None),
        P("patch", None),
    )
    out_specs = P(None, "lev", "patch")
    return jax.shard_map(shards, mesh=mesh, in_specs=in_specs, out_specs=out_specs, check_vma=False)
```

```python
import functools

import jax
import jax.numpy as jnp
from jax import lax
from jax.experimental import pallas as pl
from jax.experimental.pallas import tpu as pltpu
from jax.sharding import PartitionSpec as P

MESH = pl.DeviceIdType.MESH
F32 = jnp.float32
BF16 = jnp.bfloat16
VMEM_BYTES = 67043328


def link_offsets(reach_len):
    return [
        position - reach_len if position < reach_len else position - reach_len + 1
        for position in range(2 * reach_len)
    ]


def chunks_of(parts):
    chunks = []
    for low, count in parts:
        step = 32 if count % 32 == 0 else count
        chunks.append([(low + at, step) for at in range(0, count, step)])
    return chunks


def split_rows(n_lev, level_len, members, wide):
    early = level_len - wide if n_lev == 2 else level_len - 2 * wide
    return [(0, early * members), (early * members, (level_len - early) * members)]


def dot_t(left, right):
    return lax.dot_general(left, right, (((1,), (1,)), ((), ())), preferred_element_type=F32)


def kernel(
    n_patch,
    n_lev,
    fields_hbm,
    interp_hbm,
    conv_hbm,
    weight_hbm,
    send_hbm,
    pattern_hbm,
    left_out,
    turn_out,
    base_out,
    weight,
    send,
    pattern,
    fields,
    interp,
    conv,
    turned,
    coarse,
    levels,
    middle,
    halo_out,
    halo_in,
    own,
    smooth,
    ext,
    send_rows,
    which_made,
    slot_made,
    which,
    slot_of,
    load_sem,
    halo_sem,
    send_sem,
    back_sem,
    forth_sem,
    enter_sem,
    enter_lev,
    returning,
    sending,
    arrived,
    *arrived_back,
):
    members, level_len, _ = fields.shape
    tiles, tile_len, fine = interp.shape
    k_len = conv_hbm.shape[1]
    most, link_len = send.shape[1], send.shape[2]
    half = (weight.shape[0] - 1) // 2
    wide = 2 * half
    rows = members * level_len
    total_levels = weight.shape[1]
    offsets = link_offsets(link_len // 2)
    two = n_lev == 2
    parts = split_rows(n_lev, level_len, members, wide)
    chunks = chunks_of(parts)
    numbered = [(low, count) for part in chunks for low, count in part]
    me_p, me_l = lax.axis_index("patch"), lax.axis_index("lev")
    partner = [lax.rem(me_p + d + n_patch, n_patch) for d in offsets]
    source = [lax.rem(me_p - d + n_patch, n_patch) for d in offsets]

    order = list(range(wide, level_len - wide))
    order += list(range(wide)) + list(range(level_len - wide, level_len))

    def turned_level(index):
        return jnp.where(me_l == 0, index, level_len - 1 - index) if two else index

    def level_of(group):
        return turned_level(group) if two else order[group]

    def rank(index):
        return jnp.where(index < n_patch - 4, index, 2 * n_patch - 5 - index)

    me_rank = rank(me_p)
    ahead = [rank(other) < me_rank for other in partner]
    behind = [rank(other) > me_rank for other in partner]
    answers = [rank(other) > me_rank for other in source]
    upper = sorted((o for o in range(link_len) if offsets[o] < 0), key=lambda o: offsets[o])
    lower = sorted((o for o in range(link_len) if offsets[o] > 0), key=lambda o: -offsets[o])

    load_w = pltpu.make_async_copy(weight_hbm, weight, load_sem.at[3])
    load_s = pltpu.make_async_copy(send_hbm, send, load_sem.at[4])
    load_v = pltpu.make_async_copy(send_hbm, send_rows, load_sem.at[6])
    load_p = pltpu.make_async_copy(pattern_hbm, pattern, load_sem.at[5])
    load_f = pltpu.make_async_copy(fields_hbm, fields, load_sem.at[0])
    load_i = pltpu.make_async_copy(interp_hbm, interp, load_sem.at[1])
    load_c = pltpu.make_async_copy(conv_hbm, conv.at[:, pl.ds(0, k_len)], load_sem.at[2])
    load_p.start()
    load_v.start()
    load_s.start()
    load_w.start()
    load_f.start()
    load_i.start()
    load_c.start()

    barrier = pltpu.get_barrier_semaphore()
    for o in range(link_len):

        @pl.when(behind[o])
        def _(o=o):
            pl.semaphore_signal(
                barrier, inc=1, device_id={"patch": partner[o]}, device_id_type=MESH
            )

    @pl.when(me_l < n_lev - 1)
    def _():
        pl.semaphore_signal(barrier, inc=1, device_id={"lev": me_l + 1}, device_id_type=MESH)

    entries = tiles + link_len * most
    enter_first = jnp.logical_or(me_p < 4, me_p >= n_patch - 2)
    enter_last = jnp.logical_and(jnp.logical_not(enter_first), me_p >= n_patch - 4)
    enter_second = jnp.logical_not(jnp.logical_or(enter_first, enter_last))

    def enter():
        before = jnp.where(me_l > 0, 1, 0)
        for o in range(link_len):
            before = before + jnp.where(ahead[o], 1, 0)

        @pl.when(before > 0)
        def _():
            pl.semaphore_wait(barrier, before)

        for o in range(link_len):

            @pl.when(ahead[o])
            def _(o=o):
                wrapped = partner[o] < me_p if offsets[o] > 0 else partner[o] > me_p
                pl.semaphore_signal(
                    enter_sem.at[jnp.where(wrapped, 1, 0)],
                    inc=1,
                    device_id={"patch": partner[o]},
                    device_id_type=MESH,
                )

        @pl.when(me_l > 0)
        def _():
            pl.semaphore_signal(enter_lev, inc=1, device_id={"lev": me_l - 1}, device_id_type=MESH)

    pl.when(enter_first)(enter)
    for t in range(tiles):
        conv[t, k_len] = jnp.zeros((tile_len, tile_len), BF16)
    for i, (_, count) in enumerate(numbered):
        for o in range(link_len):
            arrived_back[i][o, most] = jnp.zeros((count, tile_len), BF16)
    ext[tiles] = jnp.zeros((rows, tile_len), BF16)
    load_p.wait()
    load_v.wait()
    lane = lax.broadcasted_iota(jnp.int32, (tiles, entries), 1)
    index = jnp.full((tiles, entries), k_len, jnp.int32)
    for k in range(k_len):
        index = jnp.where(pattern[:, k : k + 1] == lane, k, index)
    which_made[...] = index
    row = lax.broadcasted_iota(jnp.int32, (tiles, link_len), 0)
    index = jnp.full((tiles, link_len), most, jnp.int32)
    for s in range(most):
        index = jnp.where(send_rows[0, s : s + 1, :] == row, s, index)
    slot_made[...] = index
    pl.when(enter_second)(enter)
    load_f.wait()
    load_i.wait()
    make_which = pltpu.make_async_copy(which_made, which, load_sem.at[7])
    make_slot = pltpu.make_async_copy(slot_made, slot_of, load_sem.at[8])
    make_which.start()
    make_slot.start()
    split = tiles // 2
    below = {"lev": lax.rem(me_l + n_lev - 1, n_lev)}
    above = {"lev": lax.rem(me_l + 1, n_lev)}

    def exchange(side, place, to, some=slice(None)):
        return pltpu.make_async_remote_copy(
            halo_out.at[side, :, some],
            halo_in.at[place, :, some],
            halo_sem.at[2 * side],
            halo_sem.at[2 * side + 1],
            device_id=to,
            device_id_type=MESH,
        )

    down = exchange(0, 1, below)
    up = down if two else exchange(1, 0, above)
    for h in range(2):
        for t in range(h * split, (h + 1) * split):
            block = fields[:, :, t * fine : (t + 1) * fine].reshape(rows, fine)
            coarse[t] = dot_t(block, interp[t])
            for l in range(level_len):
                place = pl.ds(turned_level(l), members, stride=level_len)
                levels[wide + l, t] = coarse[t, place, :]
        some = pl.ds(h * split, split)
        for i in range(wide // 2):
            low = [level_len - 1 - 2 * i - n if two else 2 * i + n for n in range(2)]
            low = [levels[wide + l, some] for l in low]
            halo_out[0, i, some] = jnp.concatenate(low, axis=1).astype(BF16)
            if not two:
                high = [levels[level_len + 2 * i + n, some] for n in range(2)]
                halo_out[1, i, some] = jnp.concatenate(high, axis=1).astype(BF16)
        if h == 0:
            pl.when(enter_last)(enter)

        @pl.when(me_l > 0)
        def _(some=some):
            exchange(0, 1, below, some).start()

    start = me_l * level_len

    sign = jnp.where(me_l == 0, 1, -1) if two else 1
    load_w.wait()

    def coefficient(level, shift):
        return weight[half + sign * shift, jnp.clip(start + turned_level(level), 0, total_levels - 1)]

    def adjoint_level(level):
        value = coefficient(level - half, half) * levels[wide + level - half]
        for e in range(1 - half, half + 1):
            value = value + coefficient(level + e, -e) * levels[wide + level + e]
        if level < 0:
            value = jnp.where(start + level >= 0, value, 0.0)
        if level >= level_len:
            value = jnp.where(start + level < total_levels, value, 0.0) if not two else value
        middle[half + level] = value

    def forward_pair(level):
        both = []
        for l in (level, level + 1):
            value = coefficient(l, -half) * middle[l]
            for j in range(1, wide + 1):
                value = value + coefficient(l, j - half) * middle[l + j]
            both.append(value)
        pair = jnp.concatenate(both, axis=1).astype(BF16)
        place = (level if two else order.index(level)) * members
        smooth[:, pl.ds(place, 2 * members), :] = pair

    def clear(base):
        for i in range(wide):
            levels[base + i] = jnp.zeros(levels.shape[1:], F32)

    if two:
        clear(0)
        for i in range(half):
            middle[i] = jnp.zeros(middle.shape[1:], F32)
        early = [range(level_len - half), range(0, level_len - wide, 2)]
        late = [range(level_len - half, level_len + half), range(level_len - wide, level_len, 2)]
    else:
        early = [range(half, level_len - half), range(wide, level_len - wide, 2)]
        late = [list(range(-half, half)) + list(range(level_len - half, level_len + half))]
        late.append(list(range(0, wide, 2)) + list(range(level_len - wide, level_len, 2)))
    for level in early[0]:
        adjoint_level(level)
    for level in early[1]:
        forward_pair(level)

    load_c.wait()
    load_s.wait()
    make_which.wait()
    make_slot.wait()

    def gathered(left, first):
        right = jnp.concatenate(
            [
                jnp.concatenate([conv[t, which[t, first + s]] for t in range(tiles)], axis=1)
                for s in range(most)
            ],
            axis=0,
        )
        return dot_t(left, right)

    def gathered_turned(left, first):
        right = jnp.concatenate(
            [
                jnp.concatenate([turned[t, which[t, first + s]] for t in range(tiles)], axis=0)
                for s in range(most)
            ],
            axis=1,
        )
        return jnp.dot(left, right, preferred_element_type=F32)

    def side_by_side(ref, count, low, size):
        return jnp.concatenate([ref[i, pl.ds(low, size)] for i in range(count)], axis=1)

    def sum_back(c, o):
        low, count = parts[c]
        left = side_by_side(smooth, tiles, low, count)
        sums = (gathered_turned if c else gathered)(left, tiles + o * most).astype(BF16)
        for s in range(most):
            returning[o, s, pl.ds(low, count)] = sums[:, s * tile_len : (s + 1) * tile_len]

    def copy_back(o, i):
        low, count = numbered[i]
        return pltpu.make_async_remote_copy(
            returning.at[o, :, pl.ds(low, count)],
            arrived_back[i].at[o, pl.ds(0, most)],
            send_sem.at[0],
            back_sem.at[i],
            device_id={"patch": source[o]},
            device_id_type=MESH,
        )

    def copy_forth(o, i):
        low, count = numbered[i]
        return pltpu.make_async_remote_copy(
            sending.at[o, :, pl.ds(low, count)],
            arrived.at[o, :, pl.ds(low, count)],
            send_sem.at[1],
            forth_sem.at[0 if offsets[o] < 0 else 1],
            device_id={"patch": partner[o]},
            device_id_type=MESH,
        )

    def all_back(i):
        low, count = numbered[i]
        return pltpu.make_async_remote_copy(
            returning.at[:, :, pl.ds(low, count)],
            arrived_back[i].at[:, pl.ds(0, most)],
            send_sem.at[0],
            back_sem.at[i],
            device_id={"patch": source[0]},
            device_id_type=MESH,
        )

    def all_forth(first, count, sem):
        return pltpu.make_async_remote_copy(
            sending.at[pl.ds(first, count)],
            arrived.at[pl.ds(first, count)],
            send_sem.at[1],
            forth_sem.at[sem],
            device_id={"patch": partner[0]},
            device_id_type=MESH,
        )

    def indices(c):
        first = len(chunks[0]) if c else 0
        return range(first, first + len(chunks[c]))

    def sum_own():
        left = side_by_side(smooth, tiles, 0, rows)
        for first in range(0, tiles, most):
            sums = gathered_turned(left, first)
            for s in range(most):
                own[first + s] = sums[:, s * tile_len : (s + 1) * tile_len]

    def await_entry(group, wrapped):
        later = jnp.int32(0)
        for o in group:
            around = source[o] > me_p if offsets[o] > 0 else source[o] < me_p
            wanted = jnp.logical_and(answers[o], around == wrapped)
            later = later + jnp.where(wanted, 1, 0)

        @pl.when(later > 0)
        def _():
            pl.semaphore_wait(enter_sem.at[1 if wrapped else 0], later)

    def send_back(c, group):
        for o in group:
            sum_back(c, o)
        if c == 0:
            await_entry(group, False)
        for i in indices(c):
            for o in group:
                if c == 0 and group is lower:

                    @pl.when(source[o] < me_p)
                    def _(o=o, i=i):
                        copy_back(o, i).start()

                else:
                    copy_back(o, i).start()

    send_back(0, lower)

    @pl.when(me_l < n_lev - 1)
    def _():
        pl.semaphore_wait(enter_lev, 1)
        up.start()

    send_back(0, upper)
    for t in range(tiles):
        for k in range(k_len + 1):
            turned[t, k] = conv[t, k].T

    def unpack(side, base):
        for i in range(wide // 2):
            pair = halo_in[side, i].astype(F32)
            levels[base + 2 * i] = pair[:, :members]
            levels[base + 2 * i + 1] = pair[:, members:]

    await_entry(upper + lower, True)
    for i in indices(0):
        for o in lower:

            @pl.when(source[o] > me_p)
            def _(o=o, i=i):
                copy_back(o, i).start()

    if two:
        down.wait_recv()
        unpack(1, wide + level_len)
    else:

        @pl.when(me_l > 0)
        def _():
            up.wait_recv()
            unpack(0, 0)

        @pl.when(me_l == 0)
        def _():
            clear(0)

        @pl.when(me_l < n_lev - 1)
        def _():
            down.wait_recv()
            unpack(1, wide + level_len)

        @pl.when(me_l == n_lev - 1)
        def _():
            clear(wide + level_len)

    for level in late[0]:
        adjoint_level(level)
    for level in late[1]:
        forward_pair(level)

    around = me_p >= n_patch - max(offsets)

    @pl.when(around)
    def _():
        send_back(1, upper)
        send_back(1, lower)

    @pl.when(jnp.logical_not(around))
    def _():
        send_back(1, lower)
        send_back(1, upper)

    sum_own()

    last = len(numbered) - 1

    def near_forth(i):
        for o in upper:
            copy_forth(o, i).start()
        for o in lower:

            @pl.when(partner[o] > me_p)
            def _(o=o):
                copy_forth(o, i).start()

    def places_of(group):
        return 0 if group is lower else len(lower) * most * tile_len

    def through_interp(group):
        named = [tiles + o * most + s for o in group for s in range(most)]
        rows_of = pl.ds(places_of(group), len(named) * tile_len)
        for t in range(tiles):
            stack = jnp.concatenate([conv[t, which[t, e]] for e in named], axis=0)
            product = jnp.dot(stack, interp[t], preferred_element_type=F32)
            turn_out[t, rows_of] = product.astype(BF16)

    def both_through_interp():
        through_interp(lower)
        through_interp(upper)

    for i, (low, count) in enumerate(numbered):
        if i == last:
            pl.when(me_p < 2)(both_through_interp)
        all_back(i).wait_recv()
        for t in range(tiles):
            value = own[t, pl.ds(low, count)]
            for o in range(link_len):
                value = value + arrived_back[i][o, slot_of[t, o]].astype(F32)
            ext[t, pl.ds(low, count)] = value.astype(BF16)
        for o in lower + upper:
            for s in range(most):
                sending[o, s, pl.ds(low, count)] = ext[send[0, s, o], pl.ds(low, count)]
        for o in lower:

            @pl.when(partner[o] < me_p)
            def _(o=o, i=i):
                copy_forth(o, i).start()

        if i == last:
            pl.when(around)(lambda: near_forth(last - 1))
        if i == last - 1:
            pl.when(jnp.logical_not(around))(lambda: near_forth(last - 1))
        else:
            near_forth(i)

    def spread(left, named, t):
        right = jnp.concatenate(
            [
                jnp.concatenate([conv[u, which[u, e]] for e in named], axis=0)
                for u in (t, t + 1)
            ],
            axis=1,
        )
        return jnp.dot(left, right, preferred_element_type=F32)

    def by_member(value, n):
        for g in range(level_len):
            place = pl.ds(pl.multiple_of(level_of(g) * members, members), members)
            coarse[n, place] = value[g * members : (g + 1) * members]
        lines = [coarse[n, pl.ds(m, level_len, stride=members), :] for m in range(members)]
        return jnp.concatenate(lines, axis=0).astype(BF16)

    def by_member(value, n):
        for g in range(level_len):
            place = pl.ds(pl.multiple_of(level_of(g) * members, members), members)
            coarse[n, place] = value[g * members : (g + 1) * members]
        lines = [coarse[n, pl.ds(m, level_len, stride=members), :] for m in range(members)]
        return jnp.concatenate(lines, axis=0).astype(BF16)

    def received(group):
        return jnp.concatenate(
            [side_by_side(arrived.at[o], most, 0, rows) for o in group], axis=1
        )

    def entries_of(group):
        return [tiles + o * most + s for o in group for s in range(most)]

    left = side_by_side(ext, tiles, 0, rows)
    for t in range(0, tiles, 2):
        sums = spread(left, range(tiles), t)
        for i in range(2):
            part = by_member(sums[:, i * tile_len : (i + 1) * tile_len], t + i)
            base_out[t + i] = jnp.dot(part, interp[t + i], preferred_element_type=F32)
    pl.when(me_p >= 2)(both_through_interp)
    for group in (lower, upper):
        for n, (o, s) in enumerate((o, s) for o in group for s in range(most)):
            if n == 0:
                first = 0 if group is upper else link_len // 2
                all_forth(first, link_len // 2, 0 if group is upper else 1).wait_recv()
            place = places_of(group) + n * tile_len
            left_out[:, place : place + tile_len] = by_member(arrived[o, s].astype(F32), n)
    for i in range(len(numbered)):
        all_back(i).wait_send()
    all_forth(0, link_len, 0).wait_send()

    @pl.when(me_l > 0)
    def _():
        down.wait_send()

    @pl.when(me_l < n_lev - 1)
    def _():
        up.wait_send()


def finish(left, turn, base, out_hbm, out, sem):
    tiles, _, fine = turn.shape
    copies = []
    for t in range(tiles):
        sums = base[t] + jnp.dot(left[...], turn[t], preferred_element_type=F32)
        columns = pl.ds(t * fine, fine)
        out[:, :, columns] = sums.reshape(out.shape[0], out.shape[1], fine)
        copy = pltpu.make_async_copy(out.at[:, :, columns], out_hbm.at[:, :, columns], sem.at[t])
        copy.start()
        copies.append(copy)
    for copy in copies:
        copy.wait()


def solution(mesh):
    n_patch, n_lev = mesh.shape["patch"], mesh.shape["lev"]

    def shards(fields, interp, conv_weight, vert_weight, send_tiles, tile_pattern):
        members, level_len, column_len = fields.shape
        tiles, tile_len, fine = interp.shape
        k_len = conv_weight.shape[1]
        link_len, most = send_tiles.shape[1:]
        wide = vert_weight.shape[1] - 1
        rows = members * level_len
        any_spec = pl.BlockSpec(memory_space=pl.ANY)
        entries = tiles + link_len * most
        weight, send = vert_weight.T, send_tiles.transpose(0, 2, 1)
        parts = split_rows(n_lev, level_len, members, wide)
        sizes = [count for part in chunks_of(parts) for _, count in part]

        def per_link(count, size=rows):
            return pltpu.VMEM((link_len, count, size, tile_len), BF16)

        vmem_spec = pl.BlockSpec(memory_space=pltpu.VMEM)
        wide_len = link_len * most * tile_len
        spare = VMEM_BYTES - 2 * (rows + tiles * fine) * wide_len - 4 * tiles * rows * fine
        spare -= 1 << 18
        left, turn, base = pl.pallas_call(
            functools.partial(kernel, n_patch, n_lev),
            name="localize",
            out_shape=[
                pltpu.VMEM((rows, wide_len), BF16),
                pltpu.VMEM((tiles, wide_len, fine), BF16),
                pltpu.VMEM((tiles, rows, fine), F32),
            ],
            in_specs=[any_spec] * 6,
            out_specs=[vmem_spec] * 3,
            scratch_shapes=[
                pltpu.SMEM(weight.shape, F32),
                pltpu.SMEM(send.shape, jnp.int32),
                pltpu.VMEM(tile_pattern.shape, jnp.int32),
                pltpu.VMEM(fields.shape, BF16),
                pltpu.VMEM(interp.shape, BF16),
                pltpu.VMEM((tiles, k_len + 1, tile_len, tile_len), BF16),
                pltpu.VMEM((tiles, k_len + 1, tile_len, tile_len), BF16),
                pltpu.VMEM((tiles, rows, tile_len), F32),
                pltpu.VMEM((level_len + 2 * wide, tiles, members, tile_len), F32),
                pltpu.VMEM((level_len + wide, tiles, members, tile_len), F32),
                pltpu.VMEM((2, wide // 2, tiles, 2 * members, tile_len), BF16),
                pltpu.VMEM((2, wide // 2, tiles, 2 * members, tile_len), BF16),
                pltpu.VMEM((tiles, rows, tile_len), F32),
                pltpu.VMEM((tiles, rows, tile_len), BF16),
                pltpu.VMEM((tiles + 1, rows, tile_len), BF16),
                pltpu.VMEM(send.shape, jnp.int32),
                pltpu.VMEM((tiles, entries), jnp.int32),
                pltpu.VMEM((tiles, link_len), jnp.int32),
                pltpu.SMEM((tiles, entries), jnp.int32),
                pltpu.SMEM((tiles, link_len), jnp.int32),
                pltpu.SemaphoreType.DMA((9,)),
                pltpu.SemaphoreType.DMA((4,)),
                pltpu.SemaphoreType.DMA((2,)),
                pltpu.SemaphoreType.DMA((len(sizes),)),
                pltpu.SemaphoreType.DMA((2,)),
                pltpu.SemaphoreType.REGULAR((2,)),
                pltpu.SemaphoreType.REGULAR,
            ]
            + [per_link(most)] * 3
            + [per_link(most + 1, size) for size in sizes],
            compiler_params=pltpu.CompilerParams(
                collective_id=0, has_side_effects=True, vmem_limit_bytes=spare
            ),
        )(fields, interp, conv_weight, weight, send, tile_pattern)
        return pl.pallas_call(
            finish,
            name="finish",
            out_shape=jax.ShapeDtypeStruct(fields.shape, F32),
            in_specs=[vmem_spec] * 3,
            out_specs=any_spec,
            scratch_shapes=[
                pltpu.VMEM(fields.shape, F32),
                pltpu.SemaphoreType.DMA((tiles,)),
            ],
            compiler_params=pltpu.CompilerParams(vmem_limit_bytes=8 << 20),
        )(left, turn, base)

    in_specs = (
        P(None, "lev", "patch"),
        P("patch", None, None),
        P("patch", None, None, None),
        P(),
        P("patch", None, None),
        P("patch", None),
    )
    out_specs = P(None, "lev", "patch")
    return jax.shard_map(shards, mesh=mesh, in_specs=in_specs, out_specs=out_specs, check_vma=False)
```

```python
import functools

import jax
import jax.numpy as jnp
from jax import lax
from jax.experimental import pallas as pl
from jax.experimental.pallas import tpu as pltpu
from jax.sharding import PartitionSpec as P

MESH = pl.DeviceIdType.MESH
F32 = jnp.float32
BF16 = jnp.bfloat16
VMEM_BYTES = 67043328


def link_offsets(reach_len):
    return [
        position - reach_len if position < reach_len else position - reach_len + 1
        for position in range(2 * reach_len)
    ]


def chunks_of(parts):
    chunks = []
    for low, count in parts:
        step = 32 if count % 32 == 0 else count
        chunks.append([(low + at, step) for at in range(0, count, step)])
    return chunks


def split_rows(n_lev, level_len, members, wide):
    early = level_len - wide if n_lev == 2 else level_len - 2 * wide
    return [(0, early * members), (early * members, (level_len - early) * members)]


def dot_t(left, right):
    return lax.dot_general(left, right, (((1,), (1,)), ((), ())), preferred_element_type=F32)


def kernel(
    n_patch,
    n_lev,
    fields_hbm,
    interp_hbm,
    conv_hbm,
    weight_hbm,
    send_hbm,
    pattern_hbm,
    left_out,
    turn_out,
    base_out,
    weight,
    send,
    pattern,
    fields,
    interp,
    conv,
    turned,
    coarse,
    levels,
    middle,
    halo_out,
    halo_in,
    own,
    smooth,
    ext,
    send_rows,
    which_made,
    slot_made,
    which,
    slot_of,
    load_sem,
    halo_sem,
    send_sem,
    back_sem,
    forth_sem,
    enter_sem,
    enter_lev,
    returning,
    sending,
    arrived,
    *arrived_back,
):
    members, level_len, _ = fields.shape
    tiles, tile_len, fine = interp.shape
    k_len = conv_hbm.shape[1]
    most, link_len = send.shape[1], send.shape[2]
    half = (weight.shape[0] - 1) // 2
    wide = 2 * half
    rows = members * level_len
    total_levels = weight.shape[1]
    offsets = link_offsets(link_len // 2)
    two = n_lev == 2
    parts = split_rows(n_lev, level_len, members, wide)
    chunks = chunks_of(parts)
    numbered = [(low, count) for part in chunks for low, count in part]
    me_p, me_l = lax.axis_index("patch"), lax.axis_index("lev")
    partner = [lax.rem(me_p + d + n_patch, n_patch) for d in offsets]
    source = [lax.rem(me_p - d + n_patch, n_patch) for d in offsets]

    order = list(range(wide, level_len - wide))
    order += list(range(wide)) + list(range(level_len - wide, level_len))

    def turned_level(index):
        return jnp.where(me_l == 0, index, level_len - 1 - index) if two else index

    def level_of(group):
        return turned_level(group) if two else order[group]

    def rank(index):
        return jnp.where(index < n_patch - 4, index, 2 * n_patch - 5 - index)

    me_rank = rank(me_p)
    ahead = [rank(other) < me_rank for other in partner]
    behind = [rank(other) > me_rank for other in partner]
    answers = [rank(other) > me_rank for other in source]
    upper = sorted((o for o in range(link_len) if offsets[o] < 0), key=lambda o: offsets[o])
    lower = sorted((o for o in range(link_len) if offsets[o] > 0), key=lambda o: -offsets[o])

    load_w = pltpu.make_async_copy(weight_hbm, weight, load_sem.at[3])
    load_s = pltpu.make_async_copy(send_hbm, send, load_sem.at[4])
    load_v = pltpu.make_async_copy(send_hbm, send_rows, load_sem.at[6])
    load_p = pltpu.make_async_copy(pattern_hbm, pattern, load_sem.at[5])
    load_f = pltpu.make_async_copy(fields_hbm, fields, load_sem.at[0])
    load_i = pltpu.make_async_copy(interp_hbm, interp, load_sem.at[1])
    load_c = pltpu.make_async_copy(conv_hbm, conv.at[:, pl.ds(0, k_len)], load_sem.at[2])
    load_p.start()
    load_v.start()
    load_s.start()
    load_w.start()
    load_f.start()
    load_i.start()
    load_c.start()

    barrier = pltpu.get_barrier_semaphore()
    for o in range(link_len):

        @pl.when(behind[o])
        def _(o=o):
            pl.semaphore_signal(
                barrier, inc=1, device_id={"patch": partner[o]}, device_id_type=MESH
            )

    @pl.when(me_l < n_lev - 1)
    def _():
        pl.semaphore_signal(barrier, inc=1, device_id={"lev": me_l + 1}, device_id_type=MESH)

    entries = tiles + link_len * most
    enter_first = jnp.logical_or(me_p < 4, me_p >= n_patch - 2)
    enter_last = jnp.logical_and(jnp.logical_not(enter_first), me_p >= n_patch - 4)
    enter_second = jnp.logical_not(jnp.logical_or(enter_first, enter_last))

    def enter():
        before = jnp.where(me_l > 0, 1, 0)
        for o in range(link_len):
            before = before + jnp.where(ahead[o], 1, 0)

        @pl.when(before > 0)
        def _():
            pl.semaphore_wait(barrier, before)

        for o in range(link_len):

            @pl.when(ahead[o])
            def _(o=o):
                wrapped = partner[o] < me_p if offsets[o] > 0 else partner[o] > me_p
                pl.semaphore_signal(
                    enter_sem.at[jnp.where(wrapped, 1, 0)],
                    inc=1,
                    device_id={"patch": partner[o]},
                    device_id_type=MESH,
                )

        @pl.when(me_l > 0)
        def _():
            pl.semaphore_signal(enter_lev, inc=1, device_id={"lev": me_l - 1}, device_id_type=MESH)

    pl.when(enter_first)(enter)
    for t in range(tiles):
        conv[t, k_len] = jnp.zeros((tile_len, tile_len), BF16)
    for i, (_, count) in enumerate(numbered):
        for o in range(link_len):
            arrived_back[i][o, most] = jnp.zeros((count, tile_len), BF16)
    ext[tiles] = jnp.zeros((rows, tile_len), BF16)
    load_p.wait()
    load_v.wait()
    lane = lax.broadcasted_iota(jnp.int32, (tiles, entries), 1)
    index = jnp.full((tiles, entries), k_len, jnp.int32)
    for k in range(k_len):
        index = jnp.where(pattern[:, k : k + 1] == lane, k, index)
    which_made[...] = index
    row = lax.broadcasted_iota(jnp.int32, (tiles, link_len), 0)
    index = jnp.full((tiles, link_len), most, jnp.int32)
    for s in range(most):
        index = jnp.where(send_rows[0, s : s + 1, :] == row, s, index)
    slot_made[...] = index
    pl.when(enter_second)(enter)
    load_f.wait()
    load_i.wait()
    make_which = pltpu.make_async_copy(which_made, which, load_sem.at[7])
    make_slot = pltpu.make_async_copy(slot_made, slot_of, load_sem.at[8])
    make_which.start()
    make_slot.start()
    split = tiles // 2
    below = {"lev": lax.rem(me_l + n_lev - 1, n_lev)}
    above = {"lev": lax.rem(me_l + 1, n_lev)}

    def exchange(side, place, to, some=slice(None)):
        return pltpu.make_async_remote_copy(
            halo_out.at[side, :, some],
            halo_in.at[place, :, some],
            halo_sem.at[2 * side],
            halo_sem.at[2 * side + 1],
            device_id=to,
            device_id_type=MESH,
        )

    down = exchange(0, 1, below)
    up = down if two else exchange(1, 0, above)
    for h in range(2):
        for t in range(h * split, (h + 1) * split):
            block = fields[:, :, t * fine : (t + 1) * fine].reshape(rows, fine)
            coarse[t] = dot_t(block, interp[t])
            for l in range(level_len):
                place = pl.ds(turned_level(l), members, stride=level_len)
                levels[wide + l, t] = coarse[t, place, :]
        some = pl.ds(h * split, split)
        for i in range(wide // 2):
            low = [level_len - 1 - 2 * i - n if two else 2 * i + n for n in range(2)]
            low = [levels[wide + l, some] for l in low]
            halo_out[0, i, some] = jnp.concatenate(low, axis=1).astype(BF16)
            if not two:
                high = [levels[level_len + 2 * i + n, some] for n in range(2)]
                halo_out[1, i, some] = jnp.concatenate(high, axis=1).astype(BF16)
        if h == 0:
            pl.when(enter_last)(enter)

        @pl.when(me_l > 0)
        def _(some=some):
            exchange(0, 1, below, some).start()

    start = me_l * level_len

    sign = jnp.where(me_l == 0, 1, -1) if two else 1
    load_w.wait()

    def coefficient(level, shift):
        return weight[half + sign * shift, jnp.clip(start + turned_level(level), 0, total_levels - 1)]

    def adjoint_level(level):
        value = coefficient(level - half, half) * levels[wide + level - half]
        for e in range(1 - half, half + 1):
            value = value + coefficient(level + e, -e) * levels[wide + level + e]
        if level < 0:
            value = jnp.where(start + level >= 0, value, 0.0)
        if level >= level_len:
            value = jnp.where(start + level < total_levels, value, 0.0) if not two else value
        middle[half + level] = value

    def forward_pair(level):
        both = []
        for l in (level, level + 1):
            value = coefficient(l, -half) * middle[l]
            for j in range(1, wide + 1):
                value = value + coefficient(l, j - half) * middle[l + j]
            both.append(value)
        pair = jnp.concatenate(both, axis=1).astype(BF16)
        place = (level if two else order.index(level)) * members
        smooth[:, pl.ds(place, 2 * members), :] = pair

    def clear(base):
        for i in range(wide):
            levels[base + i] = jnp.zeros(levels.shape[1:], F32)

    if two:
        clear(0)
        for i in range(half):
            middle[i] = jnp.zeros(middle.shape[1:], F32)
        early = [range(level_len - half), range(0, level_len - wide, 2)]
        late = [range(level_len - half, level_len + half), range(level_len - wide, level_len, 2)]
    else:
        early = [range(half, level_len - half), range(wide, level_len - wide, 2)]
        late = [list(range(-half, half)) + list(range(level_len - half, level_len + half))]
        late.append(list(range(0, wide, 2)) + list(range(level_len - wide, level_len, 2)))
    for level in early[0]:
        adjoint_level(level)
    for level in early[1]:
        forward_pair(level)

    load_c.wait()
    load_s.wait()
    make_which.wait()
    make_slot.wait()

    def gathered(left, first):
        right = jnp.concatenate(
            [
                jnp.concatenate([conv[t, which[t, first + s]] for t in range(tiles)], axis=1)
                for s in range(most)
            ],
            axis=0,
        )
        return dot_t(left, right)

    def gathered_turned(left, first):
        right = jnp.concatenate(
            [
                jnp.concatenate([turned[t, which[t, first + s]] for t in range(tiles)], axis=0)
                for s in range(most)
            ],
            axis=1,
        )
        return jnp.dot(left, right, preferred_element_type=F32)

    def side_by_side(ref, count, low, size):
        return jnp.concatenate([ref[i, pl.ds(low, size)] for i in range(count)], axis=1)

    def sum_back(c, o):
        low, count = parts[c]
        left = side_by_side(smooth, tiles, low, count)
        sums = (gathered_turned if c else gathered)(left, tiles + o * most).astype(BF16)
        for s in range(most):
            returning[o, s, pl.ds(low, count)] = sums[:, s * tile_len : (s + 1) * tile_len]

    def copy_back(o, i):
        low, count = numbered[i]
        return pltpu.make_async_remote_copy(
            returning.at[o, :, pl.ds(low, count)],
            arrived_back[i].at[o, pl.ds(0, most)],
            send_sem.at[0],
            back_sem.at[i],
            device_id={"patch": source[o]},
            device_id_type=MESH,
        )

    def copy_forth(o, i):
        low, count = numbered[i]
        return pltpu.make_async_remote_copy(
            sending.at[o, :, pl.ds(low, count)],
            arrived.at[o, :, pl.ds(low, count)],
            send_sem.at[1],
            forth_sem.at[0 if offsets[o] < 0 else 1],
            device_id={"patch": partner[o]},
            device_id_type=MESH,
        )

    def all_back(i):
        low, count = numbered[i]
        return pltpu.make_async_remote_copy(
            returning.at[:, :, pl.ds(low, count)],
            arrived_back[i].at[:, pl.ds(0, most)],
            send_sem.at[0],
            back_sem.at[i],
            device_id={"patch": source[0]},
            device_id_type=MESH,
        )

    def all_forth(first, count, sem):
        return pltpu.make_async_remote_copy(
            sending.at[pl.ds(first, count)],
            arrived.at[pl.ds(first, count)],
            send_sem.at[1],
            forth_sem.at[sem],
            device_id={"patch": partner[0]},
            device_id_type=MESH,
        )

    def indices(c):
        first = len(chunks[0]) if c else 0
        return range(first, first + len(chunks[c]))

    def sum_own():
        left = side_by_side(smooth, tiles, 0, rows)
        for first in range(0, tiles, most):
            sums = gathered_turned(left, first)
            for s in range(most):
                own[first + s] = sums[:, s * tile_len : (s + 1) * tile_len]

    def await_entry(group, wrapped):
        later = jnp.int32(0)
        for o in group:
            around = source[o] > me_p if offsets[o] > 0 else source[o] < me_p
            wanted = jnp.logical_and(answers[o], around == wrapped)
            later = later + jnp.where(wanted, 1, 0)

        @pl.when(later > 0)
        def _():
            pl.semaphore_wait(enter_sem.at[1 if wrapped else 0], later)

    def send_back(c, group):
        for o in group:
            sum_back(c, o)
        if c == 0:
            await_entry(group, False)
        for i in indices(c):
            for o in group:
                if c == 0 and group is lower:

                    @pl.when(source[o] < me_p)
                    def _(o=o, i=i):
                        copy_back(o, i).start()

                else:
                    copy_back(o, i).start()

    send_back(0, lower)

    @pl.when(me_l < n_lev - 1)
    def _():
        pl.semaphore_wait(enter_lev, 1)
        up.start()

    send_back(0, upper)
    for t in range(tiles):
        for k in range(k_len + 1):
            turned[t, k] = conv[t, k].T

    def unpack(side, base):
        for i in range(wide // 2):
            pair = halo_in[side, i].astype(F32)
            levels[base + 2 * i] = pair[:, :members]
            levels[base + 2 * i + 1] = pair[:, members:]

    await_entry(upper + lower, True)
    for i in indices(0):
        for o in lower:

            @pl.when(source[o] > me_p)
            def _(o=o, i=i):
                copy_back(o, i).start()

    if two:
        down.wait_recv()
        unpack(1, wide + level_len)
    else:

        @pl.when(me_l > 0)
        def _():
            up.wait_recv()
            unpack(0, 0)

        @pl.when(me_l == 0)
        def _():
            clear(0)

        @pl.when(me_l < n_lev - 1)
        def _():
            down.wait_recv()
            unpack(1, wide + level_len)

        @pl.when(me_l == n_lev - 1)
        def _():
            clear(wide + level_len)

    for level in late[0]:
        adjoint_level(level)
    for level in late[1]:
        forward_pair(level)

    around = me_p >= n_patch - max(offsets)

    @pl.when(around)
    def _():
        send_back(1, upper)
        send_back(1, lower)

    @pl.when(jnp.logical_not(around))
    def _():
        send_back(1, lower)
        send_back(1, upper)

    sum_own()

    last = len(numbered) - 1

    def near_forth(i):
        for o in upper:
            copy_forth(o, i).start()
        for o in lower:

            @pl.when(partner[o] > me_p)
            def _(o=o):
                copy_forth(o, i).start()

    def places_of(group):
        return 0 if group is lower else len(lower) * most * tile_len

    def through_interp(group):
        named = [tiles + o * most + s for o in group for s in range(most)]
        rows_of = pl.ds(places_of(group), len(named) * tile_len)
        for t in range(tiles):
            stack = jnp.concatenate([conv[t, which[t, e]] for e in named], axis=0)
            product = jnp.dot(stack, interp[t], preferred_element_type=F32)
            turn_out[t, rows_of] = product.astype(BF16)

    def both_through_interp():
        through_interp(lower)
        through_interp(upper)

    for i, (low, count) in enumerate(numbered):
        if i == last:
            pl.when(me_p < 2)(both_through_interp)
        all_back(i).wait_recv()
        for t in range(tiles):
            value = own[t, pl.ds(low, count)]
            for o in range(link_len):
                value = value + arrived_back[i][o, slot_of[t, o]].astype(F32)
            ext[t, pl.ds(low, count)] = value.astype(BF16)
        for o in lower + upper:
            for s in range(most):
                sending[o, s, pl.ds(low, count)] = ext[send[0, s, o], pl.ds(low, count)]
        for o in lower:

            @pl.when(partner[o] < me_p)
            def _(o=o, i=i):
                copy_forth(o, i).start()

        if i < last:
            pl.when(jnp.logical_not(around))(functools.partial(near_forth, i))
        else:
            for earlier in range(last):
                pl.when(around)(functools.partial(near_forth, earlier))
            near_forth(last)

    def spread(left, named, t):
        right = jnp.concatenate(
            [
                jnp.concatenate([conv[u, which[u, e]] for e in named], axis=0)
                for u in (t, t + 1)
            ],
            axis=1,
        )
        return jnp.dot(left, right, preferred_element_type=F32)

    def by_member(value, n):
        for g in range(level_len):
            place = pl.ds(pl.multiple_of(level_of(g) * members, members), members)
            coarse[n, place] = value[g * members : (g + 1) * members]
        lines = [coarse[n, pl.ds(m, level_len, stride=members), :] for m in range(members)]
        return jnp.concatenate(lines, axis=0).astype(BF16)

    def by_member(value, n):
        for g in range(level_len):
            place = pl.ds(pl.multiple_of(level_of(g) * members, members), members)
            coarse[n, place] = value[g * members : (g + 1) * members]
        lines = [coarse[n, pl.ds(m, level_len, stride=members), :] for m in range(members)]
        return jnp.concatenate(lines, axis=0).astype(BF16)

    def received(group):
        return jnp.concatenate(
            [side_by_side(arrived.at[o], most, 0, rows) for o in group], axis=1
        )

    def entries_of(group):
        return [tiles + o * most + s for o in group for s in range(most)]

    left = side_by_side(ext, tiles, 0, rows)
    for t in range(0, tiles, 2):
        sums = spread(left, range(tiles), t)
        for i in range(2):
            part = by_member(sums[:, i * tile_len : (i + 1) * tile_len], t + i)
            base_out[t + i] = jnp.dot(part, interp[t + i], preferred_element_type=F32)
    pl.when(me_p >= 2)(both_through_interp)
    for group in (lower, upper):
        for n, (o, s) in enumerate((o, s) for o in group for s in range(most)):
            if n == 0:
                first = 0 if group is upper else link_len // 2
                all_forth(first, link_len // 2, 0 if group is upper else 1).wait_recv()
            place = places_of(group) + n * tile_len
            left_out[:, place : place + tile_len] = by_member(arrived[o, s].astype(F32), n)
    for i in range(len(numbered)):
        all_back(i).wait_send()
    all_forth(0, link_len, 0).wait_send()

    @pl.when(me_l > 0)
    def _():
        down.wait_send()

    @pl.when(me_l < n_lev - 1)
    def _():
        up.wait_send()


def finish(left, turn, base, out_hbm, out, sem):
    tiles, _, fine = turn.shape
    copies = []
    for t in range(tiles):
        sums = base[t] + jnp.dot(left[...], turn[t], preferred_element_type=F32)
        columns = pl.ds(t * fine, fine)
        out[:, :, columns] = sums.reshape(out.shape[0], out.shape[1], fine)
        copy = pltpu.make_async_copy(out.at[:, :, columns], out_hbm.at[:, :, columns], sem.at[t])
        copy.start()
        copies.append(copy)
    for copy in copies:
        copy.wait()


def solution(mesh):
    n_patch, n_lev = mesh.shape["patch"], mesh.shape["lev"]

    def shards(fields, interp, conv_weight, vert_weight, send_tiles, tile_pattern):
        members, level_len, column_len = fields.shape
        tiles, tile_len, fine = interp.shape
        k_len = conv_weight.shape[1]
        link_len, most = send_tiles.shape[1:]
        wide = vert_weight.shape[1] - 1
        rows = members * level_len
        any_spec = pl.BlockSpec(memory_space=pl.ANY)
        entries = tiles + link_len * most
        weight, send = vert_weight.T, send_tiles.transpose(0, 2, 1)
        parts = split_rows(n_lev, level_len, members, wide)
        sizes = [count for part in chunks_of(parts) for _, count in part]

        def per_link(count, size=rows):
            return pltpu.VMEM((link_len, count, size, tile_len), BF16)

        vmem_spec = pl.BlockSpec(memory_space=pltpu.VMEM)
        wide_len = link_len * most * tile_len
        spare = VMEM_BYTES - 2 * (rows + tiles * fine) * wide_len - 4 * tiles * rows * fine
        spare -= 1 << 18
        left, turn, base = pl.pallas_call(
            functools.partial(kernel, n_patch, n_lev),
            name="localize",
            out_shape=[
                pltpu.VMEM((rows, wide_len), BF16),
                pltpu.VMEM((tiles, wide_len, fine), BF16),
                pltpu.VMEM((tiles, rows, fine), F32),
            ],
            in_specs=[any_spec] * 6,
            out_specs=[vmem_spec] * 3,
            scratch_shapes=[
                pltpu.SMEM(weight.shape, F32),
                pltpu.SMEM(send.shape, jnp.int32),
                pltpu.VMEM(tile_pattern.shape, jnp.int32),
                pltpu.VMEM(fields.shape, BF16),
                pltpu.VMEM(interp.shape, BF16),
                pltpu.VMEM((tiles, k_len + 1, tile_len, tile_len), BF16),
                pltpu.VMEM((tiles, k_len + 1, tile_len, tile_len), BF16),
                pltpu.VMEM((tiles, rows, tile_len), F32),
                pltpu.VMEM((level_len + 2 * wide, tiles, members, tile_len), F32),
                pltpu.VMEM((level_len + wide, tiles, members, tile_len), F32),
                pltpu.VMEM((2, wide // 2, tiles, 2 * members, tile_len), BF16),
                pltpu.VMEM((2, wide // 2, tiles, 2 * members, tile_len), BF16),
                pltpu.VMEM((tiles, rows, tile_len), F32),
                pltpu.VMEM((tiles, rows, tile_len), BF16),
                pltpu.VMEM((tiles + 1, rows, tile_len), BF16),
                pltpu.VMEM(send.shape, jnp.int32),
                pltpu.VMEM((tiles, entries), jnp.int32),
                pltpu.VMEM((tiles, link_len), jnp.int32),
                pltpu.SMEM((tiles, entries), jnp.int32),
                pltpu.SMEM((tiles, link_len), jnp.int32),
                pltpu.SemaphoreType.DMA((9,)),
                pltpu.SemaphoreType.DMA((4,)),
                pltpu.SemaphoreType.DMA((2,)),
                pltpu.SemaphoreType.DMA((len(sizes),)),
                pltpu.SemaphoreType.DMA((2,)),
                pltpu.SemaphoreType.REGULAR((2,)),
                pltpu.SemaphoreType.REGULAR,
            ]
            + [per_link(most)] * 3
            + [per_link(most + 1, size) for size in sizes],
            compiler_params=pltpu.CompilerParams(
                collective_id=0, has_side_effects=True, vmem_limit_bytes=spare
            ),
        )(fields, interp, conv_weight, weight, send, tile_pattern)
        return pl.pallas_call(
            finish,
            name="finish",
            out_shape=jax.ShapeDtypeStruct(fields.shape, F32),
            in_specs=[vmem_spec] * 3,
            out_specs=any_spec,
            scratch_shapes=[
                pltpu.VMEM(fields.shape, F32),
                pltpu.SemaphoreType.DMA((tiles,)),
            ],
            compiler_params=pltpu.CompilerParams(vmem_limit_bytes=8 << 20),
        )(left, turn, base)

    in_specs = (
        P(None, "lev", "patch"),
        P("patch", None, None),
        P("patch", None, None, None),
        P(),
        P("patch", None, None),
        P("patch", None),
    )
    out_specs = P(None, "lev", "patch")
    return jax.shard_map(shards, mesh=mesh, in_specs=in_specs, out_specs=out_specs, check_vma=False)
```

```python
import functools

import jax
import jax.numpy as jnp
from jax import lax
from jax.experimental import pallas as pl
from jax.experimental.pallas import tpu as pltpu
from jax.sharding import PartitionSpec as P

MESH = pl.DeviceIdType.MESH
F32 = jnp.float32
BF16 = jnp.bfloat16
VMEM_BYTES = 67043328


def link_offsets(reach_len):
    return [
        position - reach_len if position < reach_len else position - reach_len + 1
        for position in range(2 * reach_len)
    ]


def chunks_of(parts):
    chunks = []
    for low, count in parts:
        step = 32 if count % 32 == 0 else count
        chunks.append([(low + at, step) for at in range(0, count, step)])
    return chunks


def split_rows(n_lev, level_len, members, wide):
    early = level_len - wide if n_lev == 2 else level_len - 2 * wide
    return [(0, early * members), (early * members, (level_len - early) * members)]


def dot_t(left, right):
    return lax.dot_general(left, right, (((1,), (1,)), ((), ())), preferred_element_type=F32)


def kernel(
    n_patch,
    n_lev,
    fields_hbm,
    interp_hbm,
    conv_hbm,
    weight_hbm,
    send_hbm,
    pattern_hbm,
    left_out,
    turn_out,
    base_out,
    weight,
    send,
    pattern,
    fields,
    interp,
    conv,
    turned,
    coarse,
    levels,
    middle,
    halo_out,
    halo_in,
    own,
    smooth,
    ext,
    send_rows,
    which_made,
    slot_made,
    which,
    slot_of,
    load_sem,
    halo_sem,
    send_sem,
    back_sem,
    forth_sem,
    enter_sem,
    enter_lev,
    returning,
    sending,
    arrived,
    *arrived_back,
):
    members, level_len, _ = fields.shape
    tiles, tile_len, fine = interp.shape
    k_len = conv_hbm.shape[1]
    most, link_len = send.shape[1], send.shape[2]
    half = (weight.shape[0] - 1) // 2
    wide = 2 * half
    rows = members * level_len
    total_levels = weight.shape[1]
    offsets = link_offsets(link_len // 2)
    two = n_lev == 2
    parts = split_rows(n_lev, level_len, members, wide)
    chunks = chunks_of(parts)
    numbered = [(low, count) for part in chunks for low, count in part]
    me_p, me_l = lax.axis_index("patch"), lax.axis_index("lev")
    partner = [lax.rem(me_p + d + n_patch, n_patch) for d in offsets]
    source = [lax.rem(me_p - d + n_patch, n_patch) for d in offsets]

    order = list(range(wide, level_len - wide))
    order += list(range(wide)) + list(range(level_len - wide, level_len))

    def turned_level(index):
        return jnp.where(me_l == 0, index, level_len - 1 - index) if two else index

    def level_of(group):
        return turned_level(group) if two else order[group]

    def rank(index):
        return jnp.where(index < n_patch - 4, index, 2 * n_patch - 5 - index)

    me_rank = rank(me_p)
    ahead = [rank(other) < me_rank for other in partner]
    behind = [rank(other) > me_rank for other in partner]
    answers = [rank(other) > me_rank for other in source]
    upper = sorted((o for o in range(link_len) if offsets[o] < 0), key=lambda o: offsets[o])
    lower = sorted((o for o in range(link_len) if offsets[o] > 0), key=lambda o: -offsets[o])

    load_w = pltpu.make_async_copy(weight_hbm, weight, load_sem.at[3])
    load_s = pltpu.make_async_copy(send_hbm, send, load_sem.at[4])
    load_v = pltpu.make_async_copy(send_hbm, send_rows, load_sem.at[6])
    load_p = pltpu.make_async_copy(pattern_hbm, pattern, load_sem.at[5])
    load_f = pltpu.make_async_copy(fields_hbm, fields, load_sem.at[0])
    load_i = pltpu.make_async_copy(interp_hbm, interp, load_sem.at[1])
    load_c = pltpu.make_async_copy(conv_hbm, conv.at[:, pl.ds(0, k_len)], load_sem.at[2])
    load_p.start()
    load_v.start()
    load_s.start()
    load_w.start()
    load_f.start()
    load_i.start()
    load_c.start()

    barrier = pltpu.get_barrier_semaphore()
    for o in range(link_len):

        @pl.when(behind[o])
        def _(o=o):
            pl.semaphore_signal(
                barrier, inc=1, device_id={"patch": partner[o]}, device_id_type=MESH
            )

    @pl.when(me_l < n_lev - 1)
    def _():
        pl.semaphore_signal(barrier, inc=1, device_id={"lev": me_l + 1}, device_id_type=MESH)

    entries = tiles + link_len * most
    enter_first = jnp.logical_or(me_p < 4, me_p >= n_patch - 2)
    enter_last = jnp.logical_and(jnp.logical_not(enter_first), me_p >= n_patch - 4)
    enter_second = jnp.logical_not(jnp.logical_or(enter_first, enter_last))

    def enter():
        before = jnp.where(me_l > 0, 1, 0)
        for o in range(link_len):
            before = before + jnp.where(ahead[o], 1, 0)

        @pl.when(before > 0)
        def _():
            pl.semaphore_wait(barrier, before)

        for o in range(link_len):

            @pl.when(ahead[o])
            def _(o=o):
                wrapped = partner[o] < me_p if offsets[o] > 0 else partner[o] > me_p
                pl.semaphore_signal(
                    enter_sem.at[jnp.where(wrapped, 1, 0)],
                    inc=1,
                    device_id={"patch": partner[o]},
                    device_id_type=MESH,
                )

        @pl.when(me_l > 0)
        def _():
            pl.semaphore_signal(enter_lev, inc=1, device_id={"lev": me_l - 1}, device_id_type=MESH)

    pl.when(enter_first)(enter)
    for t in range(tiles):
        conv[t, k_len] = jnp.zeros((tile_len, tile_len), BF16)
    for i, (_, count) in enumerate(numbered):
        for o in range(link_len):
            arrived_back[i][o, most] = jnp.zeros((count, tile_len), BF16)
    ext[tiles] = jnp.zeros((rows, tile_len), BF16)
    load_p.wait()
    load_v.wait()
    lane = lax.broadcasted_iota(jnp.int32, (tiles, entries), 1)
    index = jnp.full((tiles, entries), k_len, jnp.int32)
    for k in range(k_len):
        index = jnp.where(pattern[:, k : k + 1] == lane, k, index)
    which_made[...] = index
    row = lax.broadcasted_iota(jnp.int32, (tiles, link_len), 0)
    index = jnp.full((tiles, link_len), most, jnp.int32)
    for s in range(most):
        index = jnp.where(send_rows[0, s : s + 1, :] == row, s, index)
    slot_made[...] = index
    pl.when(enter_second)(enter)
    load_f.wait()
    load_i.wait()
    make_which = pltpu.make_async_copy(which_made, which, load_sem.at[7])
    make_slot = pltpu.make_async_copy(slot_made, slot_of, load_sem.at[8])
    make_which.start()
    make_slot.start()
    split = tiles // 2
    below = {"lev": lax.rem(me_l + n_lev - 1, n_lev)}
    above = {"lev": lax.rem(me_l + 1, n_lev)}

    def exchange(side, place, to, some=slice(None)):
        return pltpu.make_async_remote_copy(
            halo_out.at[side, :, some],
            halo_in.at[place, :, some],
            halo_sem.at[2 * side],
            halo_sem.at[2 * side + 1],
            device_id=to,
            device_id_type=MESH,
        )

    down = exchange(0, 1, below)
    up = down if two else exchange(1, 0, above)
    for h in range(2):
        for t in range(h * split, (h + 1) * split):
            block = fields[:, :, t * fine : (t + 1) * fine].reshape(rows, fine)
            coarse[t] = dot_t(block, interp[t])
            for l in range(level_len):
                place = pl.ds(turned_level(l), members, stride=level_len)
                levels[wide + l, t] = coarse[t, place, :]
        some = pl.ds(h * split, split)
        for i in range(wide // 2):
            low = [level_len - 1 - 2 * i - n if two else 2 * i + n for n in range(2)]
            low = [levels[wide + l, some] for l in low]
            halo_out[0, i, some] = jnp.concatenate(low, axis=1).astype(BF16)
            if not two:
                high = [levels[level_len + 2 * i + n, some] for n in range(2)]
                halo_out[1, i, some] = jnp.concatenate(high, axis=1).astype(BF16)
        if h == 0:
            pl.when(enter_last)(enter)

        @pl.when(me_l > 0)
        def _(some=some):
            exchange(0, 1, below, some).start()

    start = me_l * level_len

    sign = jnp.where(me_l == 0, 1, -1) if two else 1
    load_w.wait()

    def coefficient(level, shift):
        return weight[half + sign * shift, jnp.clip(start + turned_level(level), 0, total_levels - 1)]

    def adjoint_level(level):
        value = coefficient(level - half, half) * levels[wide + level - half]
        for e in range(1 - half, half + 1):
            value = value + coefficient(level + e, -e) * levels[wide + level + e]
        if level < 0:
            value = jnp.where(start + level >= 0, value, 0.0)
        if level >= level_len:
            value = jnp.where(start + level < total_levels, value, 0.0) if not two else value
        middle[half + level] = value

    def forward_pair(level):
        both = []
        for l in (level, level + 1):
            value = coefficient(l, -half) * middle[l]
            for j in range(1, wide + 1):
                value = value + coefficient(l, j - half) * middle[l + j]
            both.append(value)
        pair = jnp.concatenate(both, axis=1).astype(BF16)
        place = (level if two else order.index(level)) * members
        smooth[:, pl.ds(place, 2 * members), :] = pair

    def clear(base):
        for i in range(wide):
            levels[base + i] = jnp.zeros(levels.shape[1:], F32)

    if two:
        clear(0)
        for i in range(half):
            middle[i] = jnp.zeros(middle.shape[1:], F32)
        early = [range(level_len - half), range(0, level_len - wide, 2)]
        late = [range(level_len - half, level_len + half), range(level_len - wide, level_len, 2)]
    else:
        early = [range(half, level_len - half), range(wide, level_len - wide, 2)]
        late = [list(range(-half, half)) + list(range(level_len - half, level_len + half))]
        late.append(list(range(0, wide, 2)) + list(range(level_len - wide, level_len, 2)))
    for level in early[0]:
        adjoint_level(level)
    for level in early[1]:
        forward_pair(level)

    load_c.wait()
    load_s.wait()
    make_which.wait()
    make_slot.wait()

    def gathered(left, first):
        right = jnp.concatenate(
            [
                jnp.concatenate([conv[t, which[t, first + s]] for t in range(tiles)], axis=1)
                for s in range(most)
            ],
            axis=0,
        )
        return dot_t(left, right)

    def gathered_turned(left, first):
        right = jnp.concatenate(
            [
                jnp.concatenate([turned[t, which[t, first + s]] for t in range(tiles)], axis=0)
                for s in range(most)
            ],
            axis=1,
        )
        return jnp.dot(left, right, preferred_element_type=F32)

    def side_by_side(ref, count, low, size):
        return jnp.concatenate([ref[i, pl.ds(low, size)] for i in range(count)], axis=1)

    def sum_back(c, o):
        low, count = parts[c]
        left = side_by_side(smooth, tiles, low, count)
        sums = (gathered_turned if c else gathered)(left, tiles + o * most).astype(BF16)
        for s in range(most):
            returning[o, s, pl.ds(low, count)] = sums[:, s * tile_len : (s + 1) * tile_len]

    def copy_back(o, i):
        low, count = numbered[i]
        return pltpu.make_async_remote_copy(
            returning.at[o, :, pl.ds(low, count)],
            arrived_back[i].at[o, pl.ds(0, most)],
            send_sem.at[0],
            back_sem.at[i],
            device_id={"patch": source[o]},
            device_id_type=MESH,
        )

    def copy_forth(o, i):
        low, count = numbered[i]
        return pltpu.make_async_remote_copy(
            sending.at[o, :, pl.ds(low, count)],
            arrived.at[o, :, pl.ds(low, count)],
            send_sem.at[1],
            forth_sem.at[0 if offsets[o] < 0 else 1],
            device_id={"patch": partner[o]},
            device_id_type=MESH,
        )

    def all_back(i):
        low, count = numbered[i]
        return pltpu.make_async_remote_copy(
            returning.at[:, :, pl.ds(low, count)],
            arrived_back[i].at[:, pl.ds(0, most)],
            send_sem.at[0],
            back_sem.at[i],
            device_id={"patch": source[0]},
            device_id_type=MESH,
        )

    def all_forth(first, count, sem):
        return pltpu.make_async_remote_copy(
            sending.at[pl.ds(first, count)],
            arrived.at[pl.ds(first, count)],
            send_sem.at[1],
            forth_sem.at[sem],
            device_id={"patch": partner[0]},
            device_id_type=MESH,
        )

    def indices(c):
        first = len(chunks[0]) if c else 0
        return range(first, first + len(chunks[c]))

    def sum_own():
        left = side_by_side(smooth, tiles, 0, rows)
        for first in range(0, tiles, most):
            sums = gathered_turned(left, first)
            for s in range(most):
                own[first + s] = sums[:, s * tile_len : (s + 1) * tile_len]

    def await_entry(group, wrapped):
        later = jnp.int32(0)
        for o in group:
            around = source[o] > me_p if offsets[o] > 0 else source[o] < me_p
            wanted = jnp.logical_and(answers[o], around == wrapped)
            later = later + jnp.where(wanted, 1, 0)

        @pl.when(later > 0)
        def _():
            pl.semaphore_wait(enter_sem.at[1 if wrapped else 0], later)

    def send_back(c, group):
        for o in group:
            sum_back(c, o)
        if c == 0:
            await_entry(group, False)
        for i in indices(c):
            for o in group:
                if c == 0 and group is lower:

                    @pl.when(source[o] < me_p)
                    def _(o=o, i=i):
                        copy_back(o, i).start()

                else:
                    copy_back(o, i).start()

    send_back(0, upper)

    @pl.when(me_l < n_lev - 1)
    def _():
        pl.semaphore_wait(enter_lev, 1)
        up.start()

    send_back(0, lower)
    for t in range(tiles):
        for k in range(k_len + 1):
            turned[t, k] = conv[t, k].T

    def unpack(side, base):
        for i in range(wide // 2):
            pair = halo_in[side, i].astype(F32)
            levels[base + 2 * i] = pair[:, :members]
            levels[base + 2 * i + 1] = pair[:, members:]

    await_entry(upper + lower, True)
    for i in indices(0):
        for o in lower:

            @pl.when(source[o] > me_p)
            def _(o=o, i=i):
                copy_back(o, i).start()

    if two:
        down.wait_recv()
        unpack(1, wide + level_len)
    else:

        @pl.when(me_l > 0)
        def _():
            up.wait_recv()
            unpack(0, 0)

        @pl.when(me_l == 0)
        def _():
            clear(0)

        @pl.when(me_l < n_lev - 1)
        def _():
            down.wait_recv()
            unpack(1, wide + level_len)

        @pl.when(me_l == n_lev - 1)
        def _():
            clear(wide + level_len)

    for level in late[0]:
        adjoint_level(level)
    for level in late[1]:
        forward_pair(level)

    @pl.when(me_p < 2)
    def _():
        send_back(1, lower)
        send_back(1, upper)

    @pl.when(me_p >= 2)
    def _():
        send_back(1, upper)
        send_back(1, lower)

    sum_own()

    last = len(numbered) - 1

    def places_of(group):
        return 0 if group is lower else len(lower) * most * tile_len

    def through_interp(group):
        named = [tiles + o * most + s for o in group for s in range(most)]
        rows_of = pl.ds(places_of(group), len(named) * tile_len)
        for t in range(tiles):
            stack = jnp.concatenate([conv[t, which[t, e]] for e in named], axis=0)
            product = jnp.dot(stack, interp[t], preferred_element_type=F32)
            turn_out[t, rows_of] = product.astype(BF16)

    def both_through_interp():
        through_interp(lower)
        through_interp(upper)

    for i, (low, count) in enumerate(numbered):
        if i == last:
            pl.when(me_p < 2)(both_through_interp)
        all_back(i).wait_recv()
        for t in range(tiles):
            value = own[t, pl.ds(low, count)]
            for o in range(link_len):
                value = value + arrived_back[i][o, slot_of[t, o]].astype(F32)
            ext[t, pl.ds(low, count)] = value.astype(BF16)
        for o in lower + upper:
            for s in range(most):
                sending[o, s, pl.ds(low, count)] = ext[send[0, s, o], pl.ds(low, count)]
        for o in lower:

            @pl.when(partner[o] < me_p)
            def _(o=o, i=i):
                copy_forth(o, i).start()

        for o in upper:
            copy_forth(o, i).start()
        for o in lower:

            @pl.when(partner[o] > me_p)
            def _(o=o, i=i):
                copy_forth(o, i).start()

    def spread(left, named, t):
        right = jnp.concatenate(
            [
                jnp.concatenate([conv[u, which[u, e]] for e in named], axis=0)
                for u in (t, t + 1)
            ],
            axis=1,
        )
        return jnp.dot(left, right, preferred_element_type=F32)

    def by_member(value, n):
        for g in range(level_len):
            place = pl.ds(pl.multiple_of(level_of(g) * members, members), members)
            coarse[n, place] = value[g * members : (g + 1) * members]
        lines = [coarse[n, pl.ds(m, level_len, stride=members), :] for m in range(members)]
        return jnp.concatenate(lines, axis=0).astype(BF16)

    def by_member(value, n):
        for g in range(level_len):
            place = pl.ds(pl.multiple_of(level_of(g) * members, members), members)
            coarse[n, place] = value[g * members : (g + 1) * members]
        lines = [coarse[n, pl.ds(m, level_len, stride=members), :] for m in range(members)]
        return jnp.concatenate(lines, axis=0).astype(BF16)

    def received(group):
        return jnp.concatenate(
            [side_by_side(arrived.at[o], most, 0, rows) for o in group], axis=1
        )

    def entries_of(group):
        return [tiles + o * most + s for o in group for s in range(most)]

    left = side_by_side(ext, tiles, 0, rows)
    for t in range(0, tiles, 2):
        sums = spread(left, range(tiles), t)
        for i in range(2):
            part = by_member(sums[:, i * tile_len : (i + 1) * tile_len], t + i)
            base_out[t + i] = jnp.dot(part, interp[t + i], preferred_element_type=F32)
    pl.when(me_p >= 2)(both_through_interp)
    for group in (lower, upper):
        for n, (o, s) in enumerate((o, s) for o in group for s in range(most)):
            if n == 0:
                first = 0 if group is upper else link_len // 2
                all_forth(first, link_len // 2, 0 if group is upper else 1).wait_recv()
            place = places_of(group) + n * tile_len
            left_out[:, place : place + tile_len] = by_member(arrived[o, s].astype(F32), n)
    for i in range(len(numbered)):
        all_back(i).wait_send()
    all_forth(0, link_len, 0).wait_send()

    @pl.when(me_l > 0)
    def _():
        down.wait_send()

    @pl.when(me_l < n_lev - 1)
    def _():
        up.wait_send()


def finish(left, turn, base, out_hbm, out, sem):
    tiles, _, fine = turn.shape
    copies = []
    for t in range(tiles):
        sums = base[t] + jnp.dot(left[...], turn[t], preferred_element_type=F32)
        columns = pl.ds(t * fine, fine)
        out[:, :, columns] = sums.reshape(out.shape[0], out.shape[1], fine)
        copy = pltpu.make_async_copy(out.at[:, :, columns], out_hbm.at[:, :, columns], sem.at[t])
        copy.start()
        copies.append(copy)
    for copy in copies:
        copy.wait()


def solution(mesh):
    n_patch, n_lev = mesh.shape["patch"], mesh.shape["lev"]

    def shards(fields, interp, conv_weight, vert_weight, send_tiles, tile_pattern):
        members, level_len, column_len = fields.shape
        tiles, tile_len, fine = interp.shape
        k_len = conv_weight.shape[1]
        link_len, most = send_tiles.shape[1:]
        wide = vert_weight.shape[1] - 1
        rows = members * level_len
        any_spec = pl.BlockSpec(memory_space=pl.ANY)
        entries = tiles + link_len * most
        weight, send = vert_weight.T, send_tiles.transpose(0, 2, 1)
        parts = split_rows(n_lev, level_len, members, wide)
        sizes = [count for part in chunks_of(parts) for _, count in part]

        def per_link(count, size=rows):
            return pltpu.VMEM((link_len, count, size, tile_len), BF16)

        vmem_spec = pl.BlockSpec(memory_space=pltpu.VMEM)
        wide_len = link_len * most * tile_len
        spare = VMEM_BYTES - 2 * (rows + tiles * fine) * wide_len - 4 * tiles * rows * fine
        spare -= 1 << 18
        left, turn, base = pl.pallas_call(
            functools.partial(kernel, n_patch, n_lev),
            name="localize",
            out_shape=[
                pltpu.VMEM((rows, wide_len), BF16),
                pltpu.VMEM((tiles, wide_len, fine), BF16),
                pltpu.VMEM((tiles, rows, fine), F32),
            ],
            in_specs=[any_spec] * 6,
            out_specs=[vmem_spec] * 3,
            scratch_shapes=[
                pltpu.SMEM(weight.shape, F32),
                pltpu.SMEM(send.shape, jnp.int32),
                pltpu.VMEM(tile_pattern.shape, jnp.int32),
                pltpu.VMEM(fields.shape, BF16),
                pltpu.VMEM(interp.shape, BF16),
                pltpu.VMEM((tiles, k_len + 1, tile_len, tile_len), BF16),
                pltpu.VMEM((tiles, k_len + 1, tile_len, tile_len), BF16),
                pltpu.VMEM((tiles, rows, tile_len), F32),
                pltpu.VMEM((level_len + 2 * wide, tiles, members, tile_len), F32),
                pltpu.VMEM((level_len + wide, tiles, members, tile_len), F32),
                pltpu.VMEM((2, wide // 2, tiles, 2 * members, tile_len), BF16),
                pltpu.VMEM((2, wide // 2, tiles, 2 * members, tile_len), BF16),
                pltpu.VMEM((tiles, rows, tile_len), F32),
                pltpu.VMEM((tiles, rows, tile_len), BF16),
                pltpu.VMEM((tiles + 1, rows, tile_len), BF16),
                pltpu.VMEM(send.shape, jnp.int32),
                pltpu.VMEM((tiles, entries), jnp.int32),
                pltpu.VMEM((tiles, link_len), jnp.int32),
                pltpu.SMEM((tiles, entries), jnp.int32),
                pltpu.SMEM((tiles, link_len), jnp.int32),
                pltpu.SemaphoreType.DMA((9,)),
                pltpu.SemaphoreType.DMA((4,)),
                pltpu.SemaphoreType.DMA((2,)),
                pltpu.SemaphoreType.DMA((len(sizes),)),
                pltpu.SemaphoreType.DMA((2,)),
                pltpu.SemaphoreType.REGULAR((2,)),
                pltpu.SemaphoreType.REGULAR,
            ]
            + [per_link(most)] * 3
            + [per_link(most + 1, size) for size in sizes],
            compiler_params=pltpu.CompilerParams(
                collective_id=0, has_side_effects=True, vmem_limit_bytes=spare
            ),
        )(fields, interp, conv_weight, weight, send, tile_pattern)
        return pl.pallas_call(
            finish,
            name="finish",
            out_shape=jax.ShapeDtypeStruct(fields.shape, F32),
            in_specs=[vmem_spec] * 3,
            out_specs=any_spec,
            scratch_shapes=[
                pltpu.VMEM(fields.shape, F32),
                pltpu.SemaphoreType.DMA((tiles,)),
            ],
            compiler_params=pltpu.CompilerParams(vmem_limit_bytes=8 << 20),
        )(left, turn, base)

    in_specs = (
        P(None, "lev", "patch"),
        P("patch", None, None),
        P("patch", None, None, None),
        P(),
        P("patch", None, None),
        P("patch", None),
    )
    out_specs = P(None, "lev", "patch")
    return jax.shard_map(shards, mesh=mesh, in_specs=in_specs, out_specs=out_specs, check_vma=False)
```

```python
import functools

import jax
import jax.numpy as jnp
from jax import lax
from jax.experimental import pallas as pl
from jax.experimental.pallas import tpu as pltpu
from jax.sharding import PartitionSpec as P

MESH = pl.DeviceIdType.MESH
F32 = jnp.float32
BF16 = jnp.bfloat16
VMEM_BYTES = 67043328


def link_offsets(reach_len):
    return [
        position - reach_len if position < reach_len else position - reach_len + 1
        for position in range(2 * reach_len)
    ]


def chunks_of(parts):
    chunks = []
    for low, count in parts:
        step = 32 if count % 32 == 0 else count
        chunks.append([(low + at, step) for at in range(0, count, step)])
    return chunks


def split_rows(n_lev, level_len, members, wide):
    early = level_len - wide if n_lev == 2 else level_len - 2 * wide
    return [(0, early * members), (early * members, (level_len - early) * members)]


def dot_t(left, right):
    return lax.dot_general(left, right, (((1,), (1,)), ((), ())), preferred_element_type=F32)


def kernel(
    n_patch,
    n_lev,
    fields_hbm,
    interp_hbm,
    conv_hbm,
    weight_hbm,
    send_hbm,
    pattern_hbm,
    left_out,
    turn_out,
    base_out,
    weight,
    send,
    pattern,
    fields,
    interp,
    conv,
    turned,
    coarse,
    levels,
    middle,
    halo_out,
    halo_in,
    own,
    smooth,
    ext,
    send_rows,
    which_made,
    slot_made,
    which,
    slot_of,
    load_sem,
    halo_sem,
    send_sem,
    back_sem,
    forth_sem,
    enter_sem,
    enter_lev,
    returning,
    sending,
    arrived,
    *arrived_back,
):
    members, level_len, _ = fields.shape
    tiles, tile_len, fine = interp.shape
    k_len = conv_hbm.shape[1]
    most, link_len = send.shape[1], send.shape[2]
    half = (weight.shape[0] - 1) // 2
    wide = 2 * half
    rows = members * level_len
    total_levels = weight.shape[1]
    offsets = link_offsets(link_len // 2)
    two = n_lev == 2
    parts = split_rows(n_lev, level_len, members, wide)
    chunks = chunks_of(parts)
    numbered = [(low, count) for part in chunks for low, count in part]
    me_p, me_l = lax.axis_index("patch"), lax.axis_index("lev")
    partner = [lax.rem(me_p + d + n_patch, n_patch) for d in offsets]
    source = [lax.rem(me_p - d + n_patch, n_patch) for d in offsets]

    order = list(range(wide, level_len - wide))
    order += list(range(wide)) + list(range(level_len - wide, level_len))

    def turned_level(index):
        return jnp.where(me_l == 0, index, level_len - 1 - index) if two else index

    def level_of(group):
        return turned_level(group) if two else order[group]

    def rank(index):
        return jnp.where(index < n_patch - 4, index, 2 * n_patch - 5 - index)

    me_rank = rank(me_p)
    ahead = [rank(other) < me_rank for other in partner]
    behind = [rank(other) > me_rank for other in partner]
    answers = [rank(other) > me_rank for other in source]
    upper = sorted((o for o in range(link_len) if offsets[o] < 0), key=lambda o: offsets[o])
    lower = sorted((o for o in range(link_len) if offsets[o] > 0), key=lambda o: -offsets[o])

    load_w = pltpu.make_async_copy(weight_hbm, weight, load_sem.at[3])
    load_s = pltpu.make_async_copy(send_hbm, send, load_sem.at[4])
    load_v = pltpu.make_async_copy(send_hbm, send_rows, load_sem.at[6])
    load_p = pltpu.make_async_copy(pattern_hbm, pattern, load_sem.at[5])
    load_f = pltpu.make_async_copy(fields_hbm, fields, load_sem.at[0])
    load_i = pltpu.make_async_copy(interp_hbm, interp, load_sem.at[1])
    load_c = pltpu.make_async_copy(conv_hbm, conv.at[:, pl.ds(0, k_len)], load_sem.at[2])
    load_p.start()
    load_v.start()
    load_s.start()
    load_w.start()
    load_f.start()
    load_i.start()
    load_c.start()

    barrier = pltpu.get_barrier_semaphore()
    for o in range(link_len):

        @pl.when(behind[o])
        def _(o=o):
            pl.semaphore_signal(
                barrier, inc=1, device_id={"patch": partner[o]}, device_id_type=MESH
            )

    @pl.when(me_l < n_lev - 1)
    def _():
        pl.semaphore_signal(barrier, inc=1, device_id={"lev": me_l + 1}, device_id_type=MESH)

    entries = tiles + link_len * most
    enter_first = jnp.logical_or(me_p < 4, me_p >= n_patch - 2)
    enter_last = jnp.logical_and(jnp.logical_not(enter_first), me_p >= n_patch - 4)
    enter_second = jnp.logical_not(jnp.logical_or(enter_first, enter_last))

    def enter():
        before = jnp.where(me_l > 0, 1, 0)
        for o in range(link_len):
            before = before + jnp.where(ahead[o], 1, 0)

        @pl.when(before > 0)
        def _():
            pl.semaphore_wait(barrier, before)

        for o in range(link_len):

            @pl.when(ahead[o])
            def _(o=o):
                wrapped = partner[o] < me_p if offsets[o] > 0 else partner[o] > me_p
                pl.semaphore_signal(
                    enter_sem.at[jnp.where(wrapped, 1, 0)],
                    inc=1,
                    device_id={"patch": partner[o]},
                    device_id_type=MESH,
                )

        @pl.when(me_l > 0)
        def _():
            pl.semaphore_signal(enter_lev, inc=1, device_id={"lev": me_l - 1}, device_id_type=MESH)

    pl.when(enter_first)(enter)
    for t in range(tiles):
        conv[t, k_len] = jnp.zeros((tile_len, tile_len), BF16)
    for i, (_, count) in enumerate(numbered):
        for o in range(link_len):
            arrived_back[i][o, most] = jnp.zeros((count, tile_len), BF16)
    ext[tiles] = jnp.zeros((rows, tile_len), BF16)
    load_p.wait()
    load_v.wait()
    lane = lax.broadcasted_iota(jnp.int32, (tiles, entries), 1)
    index = jnp.full((tiles, entries), k_len, jnp.int32)
    for k in range(k_len):
        index = jnp.where(pattern[:, k : k + 1] == lane, k, index)
    which_made[...] = index
    row = lax.broadcasted_iota(jnp.int32, (tiles, link_len), 0)
    index = jnp.full((tiles, link_len), most, jnp.int32)
    for s in range(most):
        index = jnp.where(send_rows[0, s : s + 1, :] == row, s, index)
    slot_made[...] = index
    pl.when(enter_second)(enter)
    load_f.wait()
    load_i.wait()
    make_which = pltpu.make_async_copy(which_made, which, load_sem.at[5])
    make_slot = pltpu.make_async_copy(slot_made, slot_of, load_sem.at[6])
    make_which.start()
    make_slot.start()
    split = tiles // 2
    below = {"lev": lax.rem(me_l + n_lev - 1, n_lev)}
    above = {"lev": lax.rem(me_l + 1, n_lev)}

    def exchange(side, place, to, some=slice(None)):
        return pltpu.make_async_remote_copy(
            halo_out.at[side, :, some],
            halo_in.at[place, :, some],
            halo_sem.at[2 * side],
            halo_sem.at[2 * side + 1],
            device_id=to,
            device_id_type=MESH,
        )

    down = exchange(0, 1, below)
    up = down if two else exchange(1, 0, above)
    for h in range(2):
        for t in range(h * split, (h + 1) * split):
            block = fields[:, :, t * fine : (t + 1) * fine].reshape(rows, fine)
            coarse[t] = dot_t(block, interp[t])
            for l in range(level_len):
                place = pl.ds(turned_level(l), members, stride=level_len)
                levels[wide + l, t] = coarse[t, place, :]
        some = pl.ds(h * split, split)
        for i in range(wide // 2):
            low = [level_len - 1 - 2 * i - n if two else 2 * i + n for n in range(2)]
            low = [levels[wide + l, some] for l in low]
            halo_out[0, i, some] = jnp.concatenate(low, axis=1).astype(BF16)
            if not two:
                high = [levels[level_len + 2 * i + n, some] for n in range(2)]
                halo_out[1, i, some] = jnp.concatenate(high, axis=1).astype(BF16)
        if h == 0:
            pl.when(enter_last)(enter)

        @pl.when(me_l > 0)
        def _(some=some):
            exchange(0, 1, below, some).start()

    start = me_l * level_len

    sign = jnp.where(me_l == 0, 1, -1) if two else 1
    load_w.wait()

    def coefficient(level, shift):
        return weight[half + sign * shift, jnp.clip(start + turned_level(level), 0, total_levels - 1)]

    def adjoint_level(level):
        value = coefficient(level - half, half) * levels[wide + level - half]
        for e in range(1 - half, half + 1):
            value = value + coefficient(level + e, -e) * levels[wide + level + e]
        if level < 0:
            value = jnp.where(start + level >= 0, value, 0.0)
        if level >= level_len:
            value = jnp.where(start + level < total_levels, value, 0.0) if not two else value
        middle[half + level] = value

    def forward_pair(level):
        both = []
        for l in (level, level + 1):
            value = coefficient(l, -half) * middle[l]
            for j in range(1, wide + 1):
                value = value + coefficient(l, j - half) * middle[l + j]
            both.append(value)
        pair = jnp.concatenate(both, axis=1).astype(BF16)
        place = (level if two else order.index(level)) * members
        smooth[:, pl.ds(place, 2 * members), :] = pair

    def clear(base):
        for i in range(wide):
            levels[base + i] = jnp.zeros(levels.shape[1:], F32)

    if two:
        clear(0)
        for i in range(half):
            middle[i] = jnp.zeros(middle.shape[1:], F32)
        early = [range(level_len - half), range(0, level_len - wide, 2)]
        late = [range(level_len - half, level_len + half), range(level_len - wide, level_len, 2)]
    else:
        early = [range(half, level_len - half), range(wide, level_len - wide, 2)]
        late = [list(range(-half, half)) + list(range(level_len - half, level_len + half))]
        late.append(list(range(0, wide, 2)) + list(range(level_len - wide, level_len, 2)))
    for level in early[0]:
        adjoint_level(level)
    for level in early[1]:
        forward_pair(level)

    load_c.wait()
    load_s.wait()
    make_which.wait()
    make_slot.wait()

    def gathered(left, first):
        right = jnp.concatenate(
            [
                jnp.concatenate([conv[t, which[t, first + s]] for t in range(tiles)], axis=1)
                for s in range(most)
            ],
            axis=0,
        )
        return dot_t(left, right)

    def gathered_turned(left, first):
        right = jnp.concatenate(
            [
                jnp.concatenate([turned[t, which[t, first + s]] for t in range(tiles)], axis=0)
                for s in range(most)
            ],
            axis=1,
        )
        return jnp.dot(left, right, preferred_element_type=F32)

    def side_by_side(ref, count, low, size):
        return jnp.concatenate([ref[i, pl.ds(low, size)] for i in range(count)], axis=1)

    def sum_back(c, o):
        low, count = parts[c]
        left = side_by_side(smooth, tiles, low, count)
        sums = (gathered_turned if c else gathered)(left, tiles + o * most).astype(BF16)
        for s in range(most):
            returning[o, s, pl.ds(low, count)] = sums[:, s * tile_len : (s + 1) * tile_len]

    def copy_back(o, i):
        low, count = numbered[i]
        return pltpu.make_async_remote_copy(
            returning.at[o, :, pl.ds(low, count)],
            arrived_back[i].at[o, pl.ds(0, most)],
            send_sem.at[0],
            back_sem.at[i],
            device_id={"patch": source[o]},
            device_id_type=MESH,
        )

    def copy_forth(o, i):
        low, count = numbered[i]
        return pltpu.make_async_remote_copy(
            sending.at[o, :, pl.ds(low, count)],
            arrived.at[o, :, pl.ds(low, count)],
            send_sem.at[1],
            forth_sem.at[0 if offsets[o] < 0 else 1],
            device_id={"patch": partner[o]},
            device_id_type=MESH,
        )

    def all_back(i):
        low, count = numbered[i]
        return pltpu.make_async_remote_copy(
            returning.at[:, :, pl.ds(low, count)],
            arrived_back[i].at[:, pl.ds(0, most)],
            send_sem.at[0],
            back_sem.at[i],
            device_id={"patch": source[0]},
            device_id_type=MESH,
        )

    def all_forth(first, count, sem):
        return pltpu.make_async_remote_copy(
            sending.at[pl.ds(first, count)],
            arrived.at[pl.ds(first, count)],
            send_sem.at[1],
            forth_sem.at[sem],
            device_id={"patch": partner[0]},
            device_id_type=MESH,
        )

    def indices(c):
        first = len(chunks[0]) if c else 0
        return range(first, first + len(chunks[c]))

    def sum_own():
        left = side_by_side(smooth, tiles, 0, rows)
        for first in range(0, tiles, most):
            sums = gathered_turned(left, first)
            for s in range(most):
                own[first + s] = sums[:, s * tile_len : (s + 1) * tile_len]

    def await_entry(group, wrapped):
        later = jnp.int32(0)
        for o in group:
            around = source[o] > me_p if offsets[o] > 0 else source[o] < me_p
            wanted = jnp.logical_and(answers[o], around == wrapped)
            later = later + jnp.where(wanted, 1, 0)

        @pl.when(later > 0)
        def _():
            pl.semaphore_wait(enter_sem.at[1 if wrapped else 0], later)

    def send_back(c, group):
        for o in group:
            sum_back(c, o)
        if c == 0:
            await_entry(group, False)
        for i in indices(c):
            for o in group:
                if c == 0 and group is lower:

                    @pl.when(source[o] < me_p)
                    def _(o=o, i=i):
                        copy_back(o, i).start()

                else:
                    copy_back(o, i).start()

    send_back(0, upper)

    @pl.when(me_l < n_lev - 1)
    def _():
        pl.semaphore_wait(enter_lev, 1)
        up.start()

    send_back(0, lower)
    for t in range(tiles):
        for k in range(k_len + 1):
            turned[t, k] = conv[t, k].T

    def unpack(side, base):
        for i in range(wide // 2):
            pair = halo_in[side, i].astype(F32)
            levels[base + 2 * i] = pair[:, :members]
            levels[base + 2 * i + 1] = pair[:, members:]

    await_entry(upper + lower, True)
    for i in indices(0):
        for o in lower:

            @pl.when(source[o] > me_p)
            def _(o=o, i=i):
                copy_back(o, i).start()

    if two:
        down.wait_recv()
        unpack(1, wide + level_len)
    else:

        @pl.when(me_l > 0)
        def _():
            up.wait_recv()
            unpack(0, 0)

        @pl.when(me_l == 0)
        def _():
            clear(0)

        @pl.when(me_l < n_lev - 1)
        def _():
            down.wait_recv()
            unpack(1, wide + level_len)

        @pl.when(me_l == n_lev - 1)
        def _():
            clear(wide + level_len)

    for level in late[0]:
        adjoint_level(level)
    for level in late[1]:
        forward_pair(level)

    @pl.when(me_p < 2)
    def _():
        send_back(1, lower)
        send_back(1, upper)

    @pl.when(me_p >= 2)
    def _():
        send_back(1, upper)
        send_back(1, lower)

    sum_own()

    last = len(numbered) - 1

    def places_of(group):
        return 0 if group is lower else len(lower) * most * tile_len

    def through_interp(group):
        named = [tiles + o * most + s for o in group for s in range(most)]
        rows_of = pl.ds(places_of(group), len(named) * tile_len)
        for t in range(tiles):
            stack = jnp.concatenate([conv[t, which[t, e]] for e in named], axis=0)
            product = jnp.dot(stack, interp[t], preferred_element_type=F32)
            turn_out[t, rows_of] = product.astype(BF16)

    def both_through_interp():
        through_interp(lower)
        through_interp(upper)

    for i, (low, count) in enumerate(numbered):
        if i == last:
            pl.when(me_p < 2)(both_through_interp)
        all_back(i).wait_recv()
        for t in range(tiles):
            value = own[t, pl.ds(low, count)]
            for o in range(link_len):
                value = value + arrived_back[i][o, slot_of[t, o]].astype(F32)
            ext[t, pl.ds(low, count)] = value.astype(BF16)
        for o in lower + upper:
            for s in range(most):
                sending[o, s, pl.ds(low, count)] = ext[send[0, s, o], pl.ds(low, count)]
        for o in lower:

            @pl.when(partner[o] < me_p)
            def _(o=o, i=i):
                copy_forth(o, i).start()

        for o in upper:
            copy_forth(o, i).start()
        for o in lower:

            @pl.when(partner[o] > me_p)
            def _(o=o, i=i):
                copy_forth(o, i).start()

    def spread(left, named, t):
        right = jnp.concatenate(
            [
                jnp.concatenate([conv[u, which[u, e]] for e in named], axis=0)
                for u in (t, t + 1)
            ],
            axis=1,
        )
        return jnp.dot(left, right, preferred_element_type=F32)

    def by_member(value, n):
        for g in range(level_len):
            place = pl.ds(pl.multiple_of(level_of(g) * members, members), members)
            coarse[n, place] = value[g * members : (g + 1) * members]
        lines = [coarse[n, pl.ds(m, level_len, stride=members), :] for m in range(members)]
        return jnp.concatenate(lines, axis=0).astype(BF16)

    def by_member(value, n):
        for g in range(level_len):
            place = pl.ds(pl.multiple_of(level_of(g) * members, members), members)
            coarse[n, place] = value[g * members : (g + 1) * members]
        lines = [coarse[n, pl.ds(m, level_len, stride=members), :] for m in range(members)]
        return jnp.concatenate(lines, axis=0).astype(BF16)

    def received(group):
        return jnp.concatenate(
            [side_by_side(arrived.at[o], most, 0, rows) for o in group], axis=1
        )

    def entries_of(group):
        return [tiles + o * most + s for o in group for s in range(most)]

    left = side_by_side(ext, tiles, 0, rows)
    for t in range(0, tiles, 2):
        sums = spread(left, range(tiles), t)
        for i in range(2):
            part = by_member(sums[:, i * tile_len : (i + 1) * tile_len], t + i)
            base_out[t + i] = jnp.dot(part, interp[t + i], preferred_element_type=F32)
    pl.when(me_p >= 2)(both_through_interp)
    for group in (upper, lower):
        for n, (o, s) in enumerate((o, s) for o in group for s in range(most)):
            if n == 0:
                first = 0 if group is upper else link_len // 2
                all_forth(first, link_len // 2, 0 if group is upper else 1).wait_recv()
            place = places_of(group) + n * tile_len
            left_out[:, place : place + tile_len] = by_member(arrived[o, s].astype(F32), n)
    for i in range(len(numbered)):
        all_back(i).wait_send()
    all_forth(0, link_len, 0).wait_send()

    @pl.when(me_l > 0)
    def _():
        down.wait_send()

    @pl.when(me_l < n_lev - 1)
    def _():
        up.wait_send()


def finish(left, turn, base, out_hbm, out, sem):
    tiles, _, fine = turn.shape
    copies = []
    for t in range(tiles):
        sums = base[t] + jnp.dot(left[...], turn[t], preferred_element_type=F32)
        columns = pl.ds(t * fine, fine)
        out[:, :, columns] = sums.reshape(out.shape[0], out.shape[1], fine)
        copy = pltpu.make_async_copy(out.at[:, :, columns], out_hbm.at[:, :, columns], sem.at[t])
        copy.start()
        copies.append(copy)
    for copy in copies:
        copy.wait()


def solution(mesh):
    n_patch, n_lev = mesh.shape["patch"], mesh.shape["lev"]

    def shards(fields, interp, conv_weight, vert_weight, send_tiles, tile_pattern):
        members, level_len, column_len = fields.shape
        tiles, tile_len, fine = interp.shape
        k_len = conv_weight.shape[1]
        link_len, most = send_tiles.shape[1:]
        wide = vert_weight.shape[1] - 1
        rows = members * level_len
        any_spec = pl.BlockSpec(memory_space=pl.ANY)
        entries = tiles + link_len * most
        weight, send = vert_weight.T, send_tiles.transpose(0, 2, 1)
        parts = split_rows(n_lev, level_len, members, wide)
        sizes = [count for part in chunks_of(parts) for _, count in part]

        def per_link(count, size=rows):
            return pltpu.VMEM((link_len, count, size, tile_len), BF16)

        vmem_spec = pl.BlockSpec(memory_space=pltpu.VMEM)
        wide_len = link_len * most * tile_len
        spare = VMEM_BYTES - 2 * (rows + tiles * fine) * wide_len - 4 * tiles * rows * fine
        spare -= 1 << 18
        left, turn, base = pl.pallas_call(
            functools.partial(kernel, n_patch, n_lev),
            name="localize",
            out_shape=[
                pltpu.VMEM((rows, wide_len), BF16),
                pltpu.VMEM((tiles, wide_len, fine), BF16),
                pltpu.VMEM((tiles, rows, fine), F32),
            ],
            in_specs=[any_spec] * 6,
            out_specs=[vmem_spec] * 3,
            scratch_shapes=[
                pltpu.SMEM(weight.shape, F32),
                pltpu.SMEM(send.shape, jnp.int32),
                pltpu.VMEM(tile_pattern.shape, jnp.int32),
                pltpu.VMEM(fields.shape, BF16),
                pltpu.VMEM(interp.shape, BF16),
                pltpu.VMEM((tiles, k_len + 1, tile_len, tile_len), BF16),
                pltpu.VMEM((tiles, k_len + 1, tile_len, tile_len), BF16),
                pltpu.VMEM((tiles, rows, tile_len), F32),
                pltpu.VMEM((level_len + 2 * wide, tiles, members, tile_len), F32),
                pltpu.VMEM((level_len + wide, tiles, members, tile_len), F32),
                pltpu.VMEM((2, wide // 2, tiles, 2 * members, tile_len), BF16),
                pltpu.VMEM((2, wide // 2, tiles, 2 * members, tile_len), BF16),
                pltpu.VMEM((tiles, rows, tile_len), F32),
                pltpu.VMEM((tiles, rows, tile_len), BF16),
                pltpu.VMEM((tiles + 1, rows, tile_len), BF16),
                pltpu.VMEM(send.shape, jnp.int32),
                pltpu.VMEM((tiles, entries), jnp.int32),
                pltpu.VMEM((tiles, link_len), jnp.int32),
                pltpu.SMEM((tiles, entries), jnp.int32),
                pltpu.SMEM((tiles, link_len), jnp.int32),
                pltpu.SemaphoreType.DMA((7,)),
                pltpu.SemaphoreType.DMA((2 if n_lev == 2 else 4,)),
                pltpu.SemaphoreType.DMA((2,)),
                pltpu.SemaphoreType.DMA((len(sizes),)),
                pltpu.SemaphoreType.DMA((2,)),
                pltpu.SemaphoreType.REGULAR((2,)),
                pltpu.SemaphoreType.REGULAR,
            ]
            + [per_link(most)] * 3
            + [per_link(most + 1, size) for size in sizes],
            compiler_params=pltpu.CompilerParams(
                collective_id=0, has_side_effects=True, vmem_limit_bytes=spare
            ),
        )(fields, interp, conv_weight, weight, send, tile_pattern)
        return pl.pallas_call(
            finish,
            name="finish",
            out_shape=jax.ShapeDtypeStruct(fields.shape, F32),
            in_specs=[vmem_spec] * 3,
            out_specs=any_spec,
            scratch_shapes=[
                pltpu.VMEM(fields.shape, F32),
                pltpu.SemaphoreType.DMA((tiles,)),
            ],
            compiler_params=pltpu.CompilerParams(vmem_limit_bytes=8 << 20),
        )(left, turn, base)

    in_specs = (
        P(None, "lev", "patch"),
        P("patch", None, None),
        P("patch", None, None, None),
        P(),
        P("patch", None, None),
        P("patch", None),
    )
    out_specs = P(None, "lev", "patch")
    return jax.shard_map(shards, mesh=mesh, in_specs=in_specs, out_specs=out_specs, check_vma=False)
```

```python
import functools

import jax
import jax.numpy as jnp
from jax import lax
from jax.experimental import pallas as pl
from jax.experimental.pallas import tpu as pltpu
from jax.sharding import PartitionSpec as P

MESH = pl.DeviceIdType.MESH
F32 = jnp.float32
BF16 = jnp.bfloat16
VMEM_BYTES = 67043328


def link_offsets(reach_len):
    return [
        position - reach_len if position < reach_len else position - reach_len + 1
        for position in range(2 * reach_len)
    ]


def chunks_of(parts):
    chunks = []
    for low, count in parts:
        step = next((n for n in (32, 16) if count % n == 0 and count > n), count)
        chunks.append([(low + at, step) for at in range(0, count, step)])
    return chunks


def split_rows(n_lev, level_len, members, wide):
    early = level_len - wide if n_lev == 2 else level_len - 2 * wide
    return [(0, early * members), (early * members, (level_len - early) * members)]


def dot_t(left, right):
    return lax.dot_general(left, right, (((1,), (1,)), ((), ())), preferred_element_type=F32)


def kernel(
    n_patch,
    n_lev,
    fields_hbm,
    interp_hbm,
    conv_hbm,
    weight_hbm,
    send_hbm,
    pattern_hbm,
    left_out,
    turn_out,
    base_out,
    weight,
    send,
    pattern,
    fields,
    interp,
    conv,
    turned,
    coarse,
    levels,
    middle,
    halo_out,
    halo_in,
    own,
    smooth,
    ext,
    send_rows,
    which_made,
    slot_made,
    which,
    slot_of,
    load_sem,
    halo_sem,
    send_sem,
    back_sem,
    forth_sem,
    enter_sem,
    enter_lev,
    returning,
    sending,
    arrived,
    *arrived_back,
):
    members, level_len, _ = fields.shape
    tiles, tile_len, fine = interp.shape
    k_len = conv_hbm.shape[1]
    most, link_len = send.shape[1], send.shape[2]
    half = (weight.shape[0] - 1) // 2
    wide = 2 * half
    rows = members * level_len
    total_levels = weight.shape[1]
    offsets = link_offsets(link_len // 2)
    two = n_lev == 2
    parts = split_rows(n_lev, level_len, members, wide)
    chunks = chunks_of(parts)
    numbered = [(low, count) for part in chunks for low, count in part]
    me_p, me_l = lax.axis_index("patch"), lax.axis_index("lev")
    partner = [lax.rem(me_p + d + n_patch, n_patch) for d in offsets]
    source = [lax.rem(me_p - d + n_patch, n_patch) for d in offsets]

    order = list(range(wide, level_len - wide))
    order += list(range(wide)) + list(range(level_len - wide, level_len))

    def turned_level(index):
        return jnp.where(me_l == 0, index, level_len - 1 - index) if two else index

    def level_of(group):
        return turned_level(group) if two else order[group]

    def rank(index):
        return jnp.where(index < n_patch - 4, index, 2 * n_patch - 5 - index)

    me_rank = rank(me_p)
    ahead = [rank(other) < me_rank for other in partner]
    behind = [rank(other) > me_rank for other in partner]
    answers = [rank(other) > me_rank for other in source]
    upper = sorted((o for o in range(link_len) if offsets[o] < 0), key=lambda o: offsets[o])
    lower = sorted((o for o in range(link_len) if offsets[o] > 0), key=lambda o: -offsets[o])

    load_w = pltpu.make_async_copy(weight_hbm, weight, load_sem.at[3])
    load_s = pltpu.make_async_copy(send_hbm, send, load_sem.at[4])
    load_v = pltpu.make_async_copy(send_hbm, send_rows, load_sem.at[6])
    load_p = pltpu.make_async_copy(pattern_hbm, pattern, load_sem.at[5])
    load_f = pltpu.make_async_copy(fields_hbm, fields, load_sem.at[0])
    load_i = pltpu.make_async_copy(interp_hbm, interp, load_sem.at[1])
    load_c = pltpu.make_async_copy(conv_hbm, conv.at[:, pl.ds(0, k_len)], load_sem.at[2])
    load_p.start()
    load_v.start()
    load_s.start()
    load_w.start()
    load_f.start()
    load_i.start()
    load_c.start()

    barrier = pltpu.get_barrier_semaphore()
    for o in range(link_len):

        @pl.when(behind[o])
        def _(o=o):
            pl.semaphore_signal(
                barrier, inc=1, device_id={"patch": partner[o]}, device_id_type=MESH
            )

    @pl.when(me_l < n_lev - 1)
    def _():
        pl.semaphore_signal(barrier, inc=1, device_id={"lev": me_l + 1}, device_id_type=MESH)

    entries = tiles + link_len * most
    enter_first = jnp.logical_or(me_p < 4, me_p >= n_patch - 2)
    enter_last = jnp.logical_and(jnp.logical_not(enter_first), me_p >= n_patch - 4)
    enter_second = jnp.logical_not(jnp.logical_or(enter_first, enter_last))

    def enter():
        before = jnp.where(me_l > 0, 1, 0)
        for o in range(link_len):
            before = before + jnp.where(ahead[o], 1, 0)

        @pl.when(before > 0)
        def _():
            pl.semaphore_wait(barrier, before)

        for o in range(link_len):

            @pl.when(ahead[o])
            def _(o=o):
                wrapped = partner[o] < me_p if offsets[o] > 0 else partner[o] > me_p
                pl.semaphore_signal(
                    enter_sem.at[jnp.where(wrapped, 1, 0)],
                    inc=1,
                    device_id={"patch": partner[o]},
                    device_id_type=MESH,
                )

        @pl.when(me_l > 0)
        def _():
            pl.semaphore_signal(enter_lev, inc=1, device_id={"lev": me_l - 1}, device_id_type=MESH)

    pl.when(enter_first)(enter)
    for t in range(tiles):
        conv[t, k_len] = jnp.zeros((tile_len, tile_len), BF16)
    for i, (_, count) in enumerate(numbered):
        for o in range(link_len):
            arrived_back[i][o, most] = jnp.zeros((count, tile_len), BF16)
    ext[tiles] = jnp.zeros((rows, tile_len), BF16)
    load_p.wait()
    load_v.wait()
    lane = lax.broadcasted_iota(jnp.int32, (tiles, entries), 1)
    index = jnp.full((tiles, entries), k_len, jnp.int32)
    for k in range(k_len):
        index = jnp.where(pattern[:, k : k + 1] == lane, k, index)
    which_made[...] = index
    row = lax.broadcasted_iota(jnp.int32, (tiles, link_len), 0)
    index = jnp.full((tiles, link_len), most, jnp.int32)
    for s in range(most):
        index = jnp.where(send_rows[0, s : s + 1, :] == row, s, index)
    slot_made[...] = index
    pl.when(enter_second)(enter)
    load_f.wait()
    load_i.wait()
    make_which = pltpu.make_async_copy(which_made, which, load_sem.at[5])
    make_slot = pltpu.make_async_copy(slot_made, slot_of, load_sem.at[6])
    make_which.start()
    make_slot.start()
    split = tiles // 2
    below = {"lev": lax.rem(me_l + n_lev - 1, n_lev)}
    above = {"lev": lax.rem(me_l + 1, n_lev)}

    def exchange(side, place, to, some=slice(None)):
        return pltpu.make_async_remote_copy(
            halo_out.at[side, :, some],
            halo_in.at[place, :, some],
            halo_sem.at[2 * side],
            halo_sem.at[2 * side + 1],
            device_id=to,
            device_id_type=MESH,
        )

    down = exchange(0, 1, below)
    up = down if two else exchange(1, 0, above)
    for h in range(2):
        for t in range(h * split, (h + 1) * split):
            block = fields[:, :, t * fine : (t + 1) * fine].reshape(rows, fine)
            coarse[t] = dot_t(block, interp[t])
            for l in range(level_len):
                place = pl.ds(turned_level(l), members, stride=level_len)
                levels[wide + l, t] = coarse[t, place, :]
        some = pl.ds(h * split, split)
        for i in range(wide // 2):
            low = [level_len - 1 - 2 * i - n if two else 2 * i + n for n in range(2)]
            low = [levels[wide + l, some] for l in low]
            halo_out[0, i, some] = jnp.concatenate(low, axis=1).astype(BF16)
            if not two:
                high = [levels[level_len + 2 * i + n, some] for n in range(2)]
                halo_out[1, i, some] = jnp.concatenate(high, axis=1).astype(BF16)
        if h == 0:
            pl.when(enter_last)(enter)

        @pl.when(me_l > 0)
        def _(some=some):
            exchange(0, 1, below, some).start()

    start = me_l * level_len

    sign = jnp.where(me_l == 0, 1, -1) if two else 1
    load_w.wait()

    def coefficient(level, shift):
        return weight[half + sign * shift, jnp.clip(start + turned_level(level), 0, total_levels - 1)]

    def adjoint_level(level):
        value = coefficient(level - half, half) * levels[wide + level - half]
        for e in range(1 - half, half + 1):
            value = value + coefficient(level + e, -e) * levels[wide + level + e]
        if level < 0:
            value = jnp.where(start + level >= 0, value, 0.0)
        if level >= level_len:
            value = jnp.where(start + level < total_levels, value, 0.0) if not two else value
        middle[half + level] = value

    def forward_pair(level):
        both = []
        for l in (level, level + 1):
            value = coefficient(l, -half) * middle[l]
            for j in range(1, wide + 1):
                value = value + coefficient(l, j - half) * middle[l + j]
            both.append(value)
        pair = jnp.concatenate(both, axis=1).astype(BF16)
        place = (level if two else order.index(level)) * members
        smooth[:, pl.ds(place, 2 * members), :] = pair

    def clear(base):
        for i in range(wide):
            levels[base + i] = jnp.zeros(levels.shape[1:], F32)

    if two:
        clear(0)
        for i in range(half):
            middle[i] = jnp.zeros(middle.shape[1:], F32)
        early = [range(level_len - half), range(0, level_len - wide, 2)]
        late = [range(level_len - half, level_len + half), range(level_len - wide, level_len, 2)]
    else:
        early = [range(half, level_len - half), range(wide, level_len - wide, 2)]
        late = [list(range(-half, half)) + list(range(level_len - half, level_len + half))]
        late.append(list(range(0, wide, 2)) + list(range(level_len - wide, level_len, 2)))
    for level in early[0]:
        adjoint_level(level)
    for level in early[1]:
        forward_pair(level)

    load_c.wait()
    load_s.wait()
    make_which.wait()
    make_slot.wait()

    def gathered(left, first):
        right = jnp.concatenate(
            [
                jnp.concatenate([conv[t, which[t, first + s]] for t in range(tiles)], axis=1)
                for s in range(most)
            ],
            axis=0,
        )
        return dot_t(left, right)

    def gathered_turned(left, first):
        right = jnp.concatenate(
            [
                jnp.concatenate([turned[t, which[t, first + s]] for t in range(tiles)], axis=0)
                for s in range(most)
            ],
            axis=1,
        )
        return jnp.dot(left, right, preferred_element_type=F32)

    def side_by_side(ref, count, low, size):
        return jnp.concatenate([ref[i, pl.ds(low, size)] for i in range(count)], axis=1)

    def sum_back(c, o):
        low, count = parts[c]
        left = side_by_side(smooth, tiles, low, count)
        sums = (gathered_turned if c else gathered)(left, tiles + o * most).astype(BF16)
        for s in range(most):
            returning[o, s, pl.ds(low, count)] = sums[:, s * tile_len : (s + 1) * tile_len]

    def copy_back(o, i):
        low, count = numbered[i]
        return pltpu.make_async_remote_copy(
            returning.at[o, :, pl.ds(low, count)],
            arrived_back[i].at[o, pl.ds(0, most)],
            send_sem.at[0],
            back_sem.at[i],
            device_id={"patch": source[o]},
            device_id_type=MESH,
        )

    def copy_forth(o, i):
        low, count = numbered[i]
        return pltpu.make_async_remote_copy(
            sending.at[o, :, pl.ds(low, count)],
            arrived.at[o, :, pl.ds(low, count)],
            send_sem.at[1],
            forth_sem.at[0 if offsets[o] < 0 else 1],
            device_id={"patch": partner[o]},
            device_id_type=MESH,
        )

    def all_back(i):
        low, count = numbered[i]
        return pltpu.make_async_remote_copy(
            returning.at[:, :, pl.ds(low, count)],
            arrived_back[i].at[:, pl.ds(0, most)],
            send_sem.at[0],
            back_sem.at[i],
            device_id={"patch": source[0]},
            device_id_type=MESH,
        )

    def all_forth(first, count, sem):
        return pltpu.make_async_remote_copy(
            sending.at[pl.ds(first, count)],
            arrived.at[pl.ds(first, count)],
            send_sem.at[1],
            forth_sem.at[sem],
            device_id={"patch": partner[0]},
            device_id_type=MESH,
        )

    def indices(c):
        first = len(chunks[0]) if c else 0
        return range(first, first + len(chunks[c]))

    def sum_own():
        left = side_by_side(smooth, tiles, 0, rows)
        for first in range(0, tiles, most):
            sums = gathered_turned(left, first)
            for s in range(most):
                own[first + s] = sums[:, s * tile_len : (s + 1) * tile_len]

    def await_entry(group, wrapped):
        later = jnp.int32(0)
        for o in group:
            around = source[o] > me_p if offsets[o] > 0 else source[o] < me_p
            wanted = jnp.logical_and(answers[o], around == wrapped)
            later = later + jnp.where(wanted, 1, 0)

        @pl.when(later > 0)
        def _():
            pl.semaphore_wait(enter_sem.at[1 if wrapped else 0], later)

    def send_back(c, group):
        for o in group:
            sum_back(c, o)
        if c == 0:
            await_entry(group, False)
        for i in indices(c):
            for o in group:
                if c == 0 and group is lower:

                    @pl.when(source[o] < me_p)
                    def _(o=o, i=i):
                        copy_back(o, i).start()

                else:
                    copy_back(o, i).start()

    send_back(0, upper)

    @pl.when(me_l < n_lev - 1)
    def _():
        pl.semaphore_wait(enter_lev, 1)
        up.start()

    send_back(0, lower)
    for t in range(tiles):
        for k in range(k_len + 1):
            turned[t, k] = conv[t, k].T

    def unpack(side, base):
        for i in range(wide // 2):
            pair = halo_in[side, i].astype(F32)
            levels[base + 2 * i] = pair[:, :members]
            levels[base + 2 * i + 1] = pair[:, members:]

    await_entry(upper + lower, True)
    for i in indices(0):
        for o in lower:

            @pl.when(source[o] > me_p)
            def _(o=o, i=i):
                copy_back(o, i).start()

    if two:
        down.wait_recv()
        unpack(1, wide + level_len)
    else:

        @pl.when(me_l > 0)
        def _():
            up.wait_recv()
            unpack(0, 0)

        @pl.when(me_l == 0)
        def _():
            clear(0)

        @pl.when(me_l < n_lev - 1)
        def _():
            down.wait_recv()
            unpack(1, wide + level_len)

        @pl.when(me_l == n_lev - 1)
        def _():
            clear(wide + level_len)

    for level in late[0]:
        adjoint_level(level)
    for level in late[1]:
        forward_pair(level)

    @pl.when(me_p < 2)
    def _():
        send_back(1, lower)
        send_back(1, upper)

    @pl.when(me_p >= 2)
    def _():
        send_back(1, upper)
        send_back(1, lower)

    sum_own()

    last = len(numbered) - 1

    def places_of(group):
        return 0 if group is lower else len(lower) * most * tile_len

    def through_interp(group):
        named = [tiles + o * most + s for o in group for s in range(most)]
        rows_of = pl.ds(places_of(group), len(named) * tile_len)
        for t in range(tiles):
            stack = jnp.concatenate([conv[t, which[t, e]] for e in named], axis=0)
            product = jnp.dot(stack, interp[t], preferred_element_type=F32)
            turn_out[t, rows_of] = product.astype(BF16)

    def both_through_interp():
        through_interp(lower)
        through_interp(upper)

    for i, (low, count) in enumerate(numbered):
        if i == last:
            pl.when(me_p < 2)(both_through_interp)
        all_back(i).wait_recv()
        for t in range(tiles):
            value = own[t, pl.ds(low, count)]
            for o in range(link_len):
                value = value + arrived_back[i][o, slot_of[t, o]].astype(F32)
            ext[t, pl.ds(low, count)] = value.astype(BF16)
        for o in lower + upper:
            for s in range(most):
                sending[o, s, pl.ds(low, count)] = ext[send[0, s, o], pl.ds(low, count)]
        for o in lower:

            @pl.when(partner[o] < me_p)
            def _(o=o, i=i):
                copy_forth(o, i).start()

        for o in upper:
            copy_forth(o, i).start()
        for o in lower:

            @pl.when(partner[o] > me_p)
            def _(o=o, i=i):
                copy_forth(o, i).start()

    def spread(left, named, t):
        right = jnp.concatenate(
            [
                jnp.concatenate([conv[u, which[u, e]] for e in named], axis=0)
                for u in (t, t + 1)
            ],
            axis=1,
        )
        return jnp.dot(left, right, preferred_element_type=F32)

    def by_member(value, n):
        for g in range(level_len):
            place = pl.ds(pl.multiple_of(level_of(g) * members, members), members)
            coarse[n, place] = value[g * members : (g + 1) * members]
        lines = [coarse[n, pl.ds(m, level_len, stride=members), :] for m in range(members)]
        return jnp.concatenate(lines, axis=0).astype(BF16)

    def by_member(value, n):
        for g in range(level_len):
            place = pl.ds(pl.multiple_of(level_of(g) * members, members), members)
            coarse[n, place] = value[g * members : (g + 1) * members]
        lines = [coarse[n, pl.ds(m, level_len, stride=members), :] for m in range(members)]
        return jnp.concatenate(lines, axis=0).astype(BF16)

    def received(group):
        return jnp.concatenate(
            [side_by_side(arrived.at[o], most, 0, rows) for o in group], axis=1
        )

    def entries_of(group):
        return [tiles + o * most + s for o in group for s in range(most)]

    left = side_by_side(ext, tiles, 0, rows)
    for t in range(0, tiles, 2):
        sums = spread(left, range(tiles), t)
        for i in range(2):
            part = by_member(sums[:, i * tile_len : (i + 1) * tile_len], t + i)
            base_out[t + i] = jnp.dot(part, interp[t + i], preferred_element_type=F32)
    pl.when(me_p >= 2)(both_through_interp)
    for group in (upper, lower):
        for n, (o, s) in enumerate((o, s) for o in group for s in range(most)):
            if n == 0:
                first = 0 if group is upper else link_len // 2
                all_forth(first, link_len // 2, 0 if group is upper else 1).wait_recv()
            place = places_of(group) + n * tile_len
            left_out[:, place : place + tile_len] = by_member(arrived[o, s].astype(F32), n)
    for i in range(len(numbered)):
        all_back(i).wait_send()
    all_forth(0, link_len, 0).wait_send()

    @pl.when(me_l > 0)
    def _():
        down.wait_send()

    @pl.when(me_l < n_lev - 1)
    def _():
        up.wait_send()


def finish(left, turn, base, out_hbm, out, sem):
    tiles, _, fine = turn.shape
    copies = []
    for t in range(tiles):
        sums = base[t] + jnp.dot(left[...], turn[t], preferred_element_type=F32)
        columns = pl.ds(t * fine, fine)
        out[:, :, columns] = sums.reshape(out.shape[0], out.shape[1], fine)
        copy = pltpu.make_async_copy(out.at[:, :, columns], out_hbm.at[:, :, columns], sem.at[t])
        copy.start()
        copies.append(copy)
    for copy in copies:
        copy.wait()


def solution(mesh):
    n_patch, n_lev = mesh.shape["patch"], mesh.shape["lev"]

    def shards(fields, interp, conv_weight, vert_weight, send_tiles, tile_pattern):
        members, level_len, column_len = fields.shape
        tiles, tile_len, fine = interp.shape
        k_len = conv_weight.shape[1]
        link_len, most = send_tiles.shape[1:]
        wide = vert_weight.shape[1] - 1
        rows = members * level_len
        any_spec = pl.BlockSpec(memory_space=pl.ANY)
        entries = tiles + link_len * most
        weight, send = vert_weight.T, send_tiles.transpose(0, 2, 1)
        parts = split_rows(n_lev, level_len, members, wide)
        sizes = [count for part in chunks_of(parts) for _, count in part]

        def per_link(count, size=rows):
            return pltpu.VMEM((link_len, count, size, tile_len), BF16)

        vmem_spec = pl.BlockSpec(memory_space=pltpu.VMEM)
        wide_len = link_len * most * tile_len
        spare = VMEM_BYTES - 2 * (rows + tiles * fine) * wide_len - 4 * tiles * rows * fine
        spare -= 1 << 18
        left, turn, base = pl.pallas_call(
            functools.partial(kernel, n_patch, n_lev),
            name="localize",
            out_shape=[
                pltpu.VMEM((rows, wide_len), BF16),
                pltpu.VMEM((tiles, wide_len, fine), BF16),
                pltpu.VMEM((tiles, rows, fine), F32),
            ],
            in_specs=[any_spec] * 6,
            out_specs=[vmem_spec] * 3,
            scratch_shapes=[
                pltpu.SMEM(weight.shape, F32),
                pltpu.SMEM(send.shape, jnp.int32),
                pltpu.VMEM(tile_pattern.shape, jnp.int32),
                pltpu.VMEM(fields.shape, BF16),
                pltpu.VMEM(interp.shape, BF16),
                pltpu.VMEM((tiles, k_len + 1, tile_len, tile_len), BF16),
                pltpu.VMEM((tiles, k_len + 1, tile_len, tile_len), BF16),
                pltpu.VMEM((tiles, rows, tile_len), F32),
                pltpu.VMEM((level_len + 2 * wide, tiles, members, tile_len), F32),
                pltpu.VMEM((level_len + wide, tiles, members, tile_len), F32),
                pltpu.VMEM((2, wide // 2, tiles, 2 * members, tile_len), BF16),
                pltpu.VMEM((2, wide // 2, tiles, 2 * members, tile_len), BF16),
                pltpu.VMEM((tiles, rows, tile_len), F32),
                pltpu.VMEM((tiles, rows, tile_len), BF16),
                pltpu.VMEM((tiles + 1, rows, tile_len), BF16),
                pltpu.VMEM(send.shape, jnp.int32),
                pltpu.VMEM((tiles, entries), jnp.int32),
                pltpu.VMEM((tiles, link_len), jnp.int32),
                pltpu.SMEM((tiles, entries), jnp.int32),
                pltpu.SMEM((tiles, link_len), jnp.int32),
                pltpu.SemaphoreType.DMA((7,)),
                pltpu.SemaphoreType.DMA((2 if n_lev == 2 else 4,)),
                pltpu.SemaphoreType.DMA((2,)),
                pltpu.SemaphoreType.DMA((len(sizes),)),
                pltpu.SemaphoreType.DMA((2,)),
                pltpu.SemaphoreType.REGULAR((2,)),
                pltpu.SemaphoreType.REGULAR,
            ]
            + [per_link(most)] * 3
            + [per_link(most + 1, size) for size in sizes],
            compiler_params=pltpu.CompilerParams(
                collective_id=0, has_side_effects=True, vmem_limit_bytes=spare
            ),
        )(fields, interp, conv_weight, weight, send, tile_pattern)
        return pl.pallas_call(
            finish,
            name="finish",
            out_shape=jax.ShapeDtypeStruct(fields.shape, F32),
            in_specs=[vmem_spec] * 3,
            out_specs=any_spec,
            scratch_shapes=[
                pltpu.VMEM(fields.shape, F32),
                pltpu.SemaphoreType.DMA((tiles,)),
            ],
            compiler_params=pltpu.CompilerParams(vmem_limit_bytes=8 << 20),
        )(left, turn, base)

    in_specs = (
        P(None, "lev", "patch"),
        P("patch", None, None),
        P("patch", None, None, None),
        P(),
        P("patch", None, None),
        P("patch", None),
    )
    out_specs = P(None, "lev", "patch")
    return jax.shard_map(shards, mesh=mesh, in_specs=in_specs, out_specs=out_specs, check_vma=False)
```
